32 devices in a mesh: outer: 4 (over z), middle: 2 (over y), inner: 4 (over x, core).
Axes of the slice: x: 2, y: 2, z: 4, core: 2. Of those that a mesh axis runs over, the one named last changes fastest.
Arguments:
- g_embed: float32 [32, 32768, 128], P(('outer', 'middle', 'inner'))
- g_attn: float32 [32, 16, 128, 512], P(('outer', 'middle', 'inner'))
- g_ffn_in: float32 [32, 16, 128, 512], P(('outer', 'middle', 'inner'))
- g_ffn_out: float32 [32, 16, 512, 128], P(('outer', 'middle', 'inner'))
- g_vec: float32 [32, 16, 1664], P(('outer', 'middle', 'inner'))
- m_flat: float32 [7366656], P(('outer', 'middle', 'inner'))
- v_flat: float32 [7366656], P(('outer', 'middle', 'inner'))
- w_flat: float32 [7366656], P(('outer', 'middle', 'inner'))
Outputs:
- output 1: float32 [7366656], P(('outer', 'middle', 'inner'))
- output 2: float32 [7366656], P(('outer', 'middle', 'inner'))
- output 3: float32 [7366656], P(('outer', 'middle', 'inner'))
- output 4: bfloat16 [32768, 128], replicated
- output 5: bfloat16 [16, 128, 512], replicated
- output 6: bfloat16 [16, 128, 512], replicated
- output 7: bfloat16 [16, 512, 128], replicated
- output 8: bfloat16 [16, 1664], replicated
- output 9: bfloat16 [32, 460416], P(('outer', 'middle', 'inner'))
All inputs are finite; a program needn't handle non-finite values.
Results may differ from the reference program's by a relative error of at most 0.001.
Values are sent between devices in bfloat16 or wider.
A program may use at most 1 GiB of HBM per device.

```python
import math
import jax
import jax.numpy as jnp

DEVICES = 32
VOCAB_ROWS = 32768
D = 128
FF = 512
LAYERS = 16
ADAM_STEP = 3

ADAM_BETA1 = 0.9
ADAM_BETA2 = 0.98
ADAM_EPS = 1e-9
LEARN_RATE = 0.05
NUM_CHIPS = DEVICES // 2
VEC_WIDTH = 9 * D + FF
TENSOR_SHAPES = ((VOCAB_ROWS, D), (LAYERS, D, 4 * D), (LAYERS, D, FF), (LAYERS, FF, D), (LAYERS, VEC_WIDTH))
PARAM_COUNT = sum(math.prod(shape) for shape in TENSOR_SHAPES)


def draw_gradient(gen_key, shape):
    common_key, chip_key, core_key = jax.random.split(gen_key, 3)
    common = jax.random.normal(common_key, shape, jnp.float32)
    per_chip = jax.random.normal(chip_key, (NUM_CHIPS,) + shape, jnp.float32)
    per_core = jax.random.normal(core_key, (DEVICES,) + shape, jnp.float32)
    return common[None] + jnp.repeat(per_chip, 2, axis=0) + 0.25 * per_core


def setup_inputs(seed: int = 0) -> dict:
    key_list = jax.random.split(jax.random.key(seed), 8)
    return {
        'g_embed': draw_gradient(key_list[0], TENSOR_SHAPES[0]),
        'g_attn': draw_gradient(key_list[1], TENSOR_SHAPES[1]),
        'g_ffn_in': draw_gradient(key_list[2], TENSOR_SHAPES[2]),
        'g_ffn_out': draw_gradient(key_list[3], TENSOR_SHAPES[3]),
        'g_vec': draw_gradient(key_list[4], TENSOR_SHAPES[4]),
        'm_flat': 0.3 * jax.random.normal(key_list[5], (PARAM_COUNT,), jnp.float32),
        'v_flat': 0.1 * (0.5 + jax.random.uniform(key_list[6], (PARAM_COUNT,), jnp.float32)),
        'w_flat': jax.random.normal(key_list[7], (PARAM_COUNT,), jnp.float32),
    }


def adam_update(grad_mean, m_old, v_old, w_old):
    m_new = ADAM_BETA1 * m_old + (1.0 - ADAM_BETA1) * grad_mean
    v_new = ADAM_BETA2 * v_old + (1.0 - ADAM_BETA2) * (grad_mean * grad_mean)
    m_hat = m_new / (1.0 - ADAM_BETA1 ** ADAM_STEP)
    v_hat = v_new / (1.0 - ADAM_BETA2 ** ADAM_STEP)
    w_new = w_old - LEARN_RATE * m_hat / (jnp.sqrt(v_hat) + ADAM_EPS)
    return m_new, v_new, w_new


def split_tensors(flat_values, shape_list):
    pieces = []
    offset = 0
    for shape in shape_list:
        count = math.prod(shape)
        pieces.append(flat_values[offset:offset + count].reshape(shape))
        offset += count
    return pieces


def chip_blocks(w_tensors, num_chips):
    blocks = [w_tensors[0].reshape(num_chips, -1)]
    for tensor in w_tensors[1:]:
        layer_count = tensor.shape[0]
        blocks.append(jnp.swapaxes(tensor.reshape(layer_count, num_chips, -1), 0, 1).reshape(num_chips, -1))
    return jnp.concatenate(blocks, axis=1)


def reference(g_embed, g_attn, g_ffn_in, g_ffn_out, g_vec, m_flat, v_flat, w_flat):
    grad_list = (g_embed, g_attn, g_ffn_in, g_ffn_out, g_vec)
    grad_mean = jnp.concatenate([jnp.sum(gradient, axis=0).reshape(-1) for gradient in grad_list]) / DEVICES
    m_new, v_new, w_new = adam_update(grad_mean, m_flat, v_flat, w_flat)
    w_tensors = split_tensors(w_new.astype(jnp.bfloat16), TENSOR_SHAPES)
    w_chip = jnp.repeat(chip_blocks(w_tensors, NUM_CHIPS), 2, axis=0)
    return (m_new, v_new, w_new, w_tensors[0], w_tensors[1], w_tensors[2], w_tensors[3], w_tensors[4], w_chip)
```

```python
import jax
import jax.numpy as jnp
from jax import lax
from jax.experimental import pallas as pl
from jax.experimental.pallas import tpu as pltpu
from jax.sharding import PartitionSpec as P

MESH_AXES = ('outer', 'middle', 'inner')
MESH = pl.DeviceIdType.MESH
BETA1, BETA2, EPS, RATE, STEP = 0.9, 0.98, 1e-9, 0.05, 3

NDEV = 32
ROWS = 1856
HALF = ROWS // 2
SLICE = 230208
SLICE_ROWS = 1800
PAD = SLICE_ROWS * 128 - SLICE
MARGIN = 64
COVER = ROWS + 8
TENSOR_ROWS = (32768, 8192, 8192, 8192, 208)
STARTS = (0, 32768, 40960, 49152, 57344, 57552)
PERM_LO, PERM_HI = 32768, 49152
PIECES = (32, 64, 128, 128, 128, 128, 128, 128, 64)
LOADS = (32, 64, 128, 256, 448)
E_SLOTS = 9


def bounds(sizes):
    out, at = [], 0
    for n in sizes:
        out.append((at, n))
        at += n
    return out


PIECE = bounds(PIECES)
LOAD = bounds(LOADS)
LOAD_OF = [next(i for i, (a, n) in enumerate(LOAD) if a <= p < a + n) for p, _ in PIECE]
SPLIT = ((0, 0), (1, 0))


def start_row(d):
    return 55696 if d == NDEV - 1 else 32 * (3597 * d // 64)


def merge_row(d):
    return 32 * (3597 * d // 64)


def segments(row, n):
    out = []
    for t in range(5):
        lo, hi = max(row, STARTS[t]), min(row + n, STARTS[t + 1])
        if lo < hi:
            out.append((t, lo - STARTS[t], lo - row, hi - lo))
    return out


def slot_of(color, k):
    x, y, z0, z1 = k % 2, k // 2 % 2, k // 4 % 2, k // 8
    return (x * 8 + z0 * 4 + y * 2 + z1) if color == 0 else (y * 8 + z0 * 4 + x * 2 + z1)


def event_order():
    unit = 128 * 4 / 46.6e3
    last = {0: 0.0}
    events, links = [], {'x': 0.0, 'y': 0.0, 'z': 0.0}
    heap = []
    loaded = 2.0
    load_done = []
    for a, n in LOAD:
        for color in (0, 1):
            loaded += n * 16 * 128 * 4 / 600e3
        load_done.append(loaded)
    for p in range(len(PIECE)):
        for color in (0, 1):
            heap.append((load_done[LOAD_OF[p]], 0, p, color))
    names = (('x', 'z', 'y', 'z'), ('y', 'z', 'x', 'z'))
    while heap:
        heap.sort()
        time, stage, p, color = heap.pop(0)
        events.append((stage, p, color))
        n = PIECE[p][1]
        if stage < 4:
            link, size = names[color][stage], n * (8 >> stage) * unit
        elif stage < 8:
            link, size = names[color][7 - stage], n * (1 << (stage - 4)) * unit / 2
        else:
            continue
        begin = max(time, links[link])
        links[link] = begin + size
        heap.append((begin + size + 3.0, stage + 1, p, color))
    return events


def big_kernel(ge, ga, gf1, gf2, gb, m_in, v_in, w_in, out_a, out_b, m_out, v_out, w_out, acc_a, acc_b, pair_a, pair_b, r1_a, r1_b, r2_a, r2_b, r3_a, r3_b, r4_a, r4_b, own_a, own_b, stage, cov, ld_sem, pr_recv, pr_send, rs_recv, rs_send, ag_recv, ag_send, loc_sem, dag_recv, dag_send, state_sem):
    grads = (ge, ga, gf1, gf2, gb)
    acc, pair, own, gat = (acc_a, acc_b), (pair_a, pair_b), (own_a, own_b), (out_a, out_b)
    rec = ((r1_a, r2_a, r3_a, r4_a), (r1_b, r2_b, r3_b, r4_b))
    z, y, inner = lax.axis_index('outer'), lax.axis_index('middle'), lax.axis_index('inner')
    x, c = inner // 2, inner % 2
    z0, z1 = z % 2, z // 2
    dev = (z * 2 + y) * 4 + inner
    to_pair = {'inner': inner + 1 - 2 * c}
    to_x = {'inner': inner + 2 - 4 * x}
    to_y = {'middle': 1 - y}
    to_z0 = {'outer': z + 1 - 2 * z0}
    to_z1 = {'outer': z + 2 - 4 * z1}
    routes = ((to_x, to_z0, to_y, to_z1), (to_y, to_z0, to_x, to_z1))
    bits = ((x, z0, y, z1), (y, z0, x, z1))

    barrier = pltpu.get_barrier_semaphore()
    for to in (to_pair, to_x, to_y, to_z0, to_z1):
        pl.semaphore_signal(barrier, inc=1, device_id=to, device_id_type=MESH)

    state_in = [pltpu.make_async_copy(src, stage.at[i, pl.ds(MARGIN, SLICE_ROWS)], state_sem.at[i]) for i, src in enumerate((m_in, v_in, w_in))]
    for copy in state_in:
        copy.start()
    pl.semaphore_wait(barrier, 5)

    def load_one(color, i, tensor, row, slot, at, n, mine):
        src = grads[tensor].at[pl.ds(row, n)]
        if mine:
            pltpu.make_async_copy(src, acc[color].at[slot, pl.ds(at, n)], ld_sem.at[color, i]).start()
        else:
            pltpu.make_async_remote_copy(src, pair[color].at[slot, pl.ds(at, n)], pr_send.at[color], pr_recv.at[color, i], device_id=to_pair, device_id_type=MESH).start()

    def load(i):
        at, n = LOAD[i]
        for color in (0, 1):
            @pl.loop(0, E_SLOTS)
            def _(k):
                slot = slot_of(color, k)
                for mine in (False, True):
                    d = 2 * k + (c if mine else 1 - c)
                    row = pl.multiple_of(32 * ((3597 * d) // 64), 32) + color * HALF + at
                    load_one(color, i, 0, row, slot, at, n, mine)
            for core in (0, 1):
                @pl.when(c == core)
                def _():
                    for k in range(E_SLOTS, NDEV // 2):
                        slot = slot_of(color, k)
                        for mine in (False, True):
                            d = 2 * k + (core if mine else 1 - core)
                            for tensor, row, off, rows in segments(start_row(d) + color * HALF + at, n):
                                load_one(color, i, tensor, row, slot, at + off, rows, mine)

    def wait_on(ref, sem):
        pltpu.make_async_copy(ref, ref, sem).wait()

    def add(color, into, slots, src, first, at, n):
        @pl.loop(0, slots)
        def _(i):
            acc[color][into + i, pl.ds(at, n), :] += src[first + i, pl.ds(at, n), :]

    def base(color, level):
        return sum((bits[color][i] * (8 >> i) for i in range(level)), 0 * c)

    def reduce_send(color, s, p):
        at, n = PIECE[p]
        size = 8 >> s
        first = base(color, s) + (1 - bits[color][s]) * size
        pltpu.make_async_remote_copy(acc[color].at[pl.ds(first, size), pl.ds(at, n)], rec[color][s].at[:, pl.ds(at, n)], rs_send.at[color, s], rs_recv.at[color, s, p], device_id=routes[color][s], device_id_type=MESH).start()

    def pair_out(color, slot, size, p):
        at, n = PIECE[p]
        block = gat[color].at[c, pl.ds(slot, size), pl.ds(at, n)]
        pltpu.make_async_remote_copy(block, block, dag_send.at[color], dag_recv.at[color], device_id=to_pair, device_id_type=MESH).start()

    def adam_block(g, load_state, store_state):
        g = g * (1.0 / NDEV)
        m = BETA1 * load_state(0) + (1.0 - BETA1) * g
        v = BETA2 * load_state(1) + (1.0 - BETA2) * (g * g)
        m_hat = m / (1.0 - BETA1 ** STEP)
        v_hat = v / (1.0 - BETA2 ** STEP)
        w = load_state(2) - RATE * m_hat / (jnp.sqrt(v_hat) + EPS)
        store_state(0, m)
        store_state(1, v)
        store_state(2, w)
        return w

    cover_start = jnp.where(dev == NDEV - 1, 55696, 32 * ((3597 * dev) // 64))

    def adam(color, p):
        at, n = PIECE[p]
        slot = base(color, 4)

        @pl.loop(0, n // 32)
        def _(j):
            r = pl.multiple_of(at + j * 32, 32)
            f = pl.multiple_of(color * HALF + r, 32)
            row = cover_start + f
            permuted = (row >= PERM_LO) & (row < PERM_HI)

            def group(index):
                for t in range(2):
                    parts = []
                    for q in (2 * t, 2 * t + 1):
                        where = index(f, q)

                        def keep(i, value, where=where):
                            cov[i, where, :] = value

                        parts.append(adam_block(acc[color][slot, pl.ds(r + 8 * q, 8), :], lambda i, where=where: cov[i, where, :], keep))
                    own[color][pl.ds(r + 16 * t, 16), :] = jnp.concatenate(parts, axis=0).astype(jnp.bfloat16)

            @pl.when(permuted)
            def _():
                group(lambda f, q: pl.ds(f + q, 8, stride=4))

            @pl.when(jnp.logical_not(permuted))
            def _():
                group(lambda f, q: pl.ds(f + 8 * q, 8))

    half_rows = jnp.where(dev == NDEV - 1, 115, (3597 * dev) % 64)
    shift = half_rows // 2
    lane = lax.broadcasted_iota(jnp.int32, (32, 128), 1)

    def moved(first, second):
        return jnp.where(lane < 64, pltpu.roll(first, 64, 1), pltpu.roll(second, 64, 1))

    def state_to_cover():
        for i, copy in enumerate(state_in):
            copy.wait()
            stage[i, 0:MARGIN, :] = jnp.zeros((MARGIN, 128), jnp.float32)
            stage[i, MARGIN + SLICE_ROWS:, :] = jnp.zeros((MARGIN, 128), jnp.float32)
            cov[i, ROWS:, :] = jnp.zeros((COVER - ROWS, 128), jnp.float32)

        @pl.loop(0, ROWS // 32)
        def _(j):
            f = pl.multiple_of(j * 32, 32)
            r = MARGIN + f - shift
            for i in range(3):
                here = stage[i, pl.ds(r, 32), :]
                before = stage[i, pl.ds(r - 1, 32), :]
                cov[i, pl.ds(f, 32), :] = jnp.where(c == 1, moved(before, here), here)

    def cover_to_state():
        @pl.loop(0, SLICE_ROWS // 8)
        def _(j):
            r = pl.multiple_of(j * 8, 8)
            for i in range(3):
                here = cov[i, pl.ds(r + shift, 8), :]
                after = cov[i, pl.ds(r + shift + 1, 8), :]
                both = jnp.where(lane[:8] < 64, pltpu.roll(here, 64, 1), pltpu.roll(after, 64, 1))
                stage[i, pl.ds(MARGIN + r, 8), :] = jnp.where(c == 1, both, here)

    load(0)
    load(1)
    events = event_order()
    loads_started = 2
    waited = set()
    state_ready = False
    for stage_no, p, color in events:
        at, n = PIECE[p]
        if stage_no == 0:
            i = LOAD_OF[p]
            while loads_started < min(i + 2, len(LOAD)):
                load(loads_started)
                loads_started += 1
            if (color, i) not in waited:
                waited.add((color, i))
                la, ln = LOAD[i]
                wait_on(acc[color].at[:, pl.ds(la, ln)], ld_sem.at[color, i])
                wait_on(pair[color].at[:, pl.ds(la, ln)], pr_recv.at[color, i])
            away, home = (1 - bits[color][0]) * 8, bits[color][0] * 8
            add(color, away, 8, pair[color], away, at, n)
            add(color, home, 8, pair[color], home, at, n)
            reduce_send(color, 0, p)
            if p == 2 and color == 1 and not state_ready:
                state_ready = True
                state_to_cover()
        elif stage_no < 4:
            s = stage_no - 1
            size = 4 >> s
            wait_on(rec[color][s].at[:, pl.ds(at, n)], rs_recv.at[color, s, p])
            first = base(color, stage_no)
            bit = bits[color][stage_no]
            add(color, first + (1 - bit) * size, size, rec[color][s], (1 - bit) * size, at, n)
            add(color, first + bit * size, size, rec[color][s], bit * size, at, n)
            reduce_send(color, stage_no, p)
        elif stage_no == 4:
            wait_on(rec[color][3].at[:, pl.ds(at, n)], rs_recv.at[color, 3, p])
            slot = base(color, 4)
            add(color, slot, 1, rec[color][3], 0, at, n)
            adam(color, p)
            src = own[color].at[pl.ds(at, n)]
            dst = gat[color].at[c, slot, pl.ds(at, n)]
            pltpu.make_async_remote_copy(src, dst, ag_send.at[color, 0], ag_recv.at[color, 0, p], device_id=to_z1, device_id_type=MESH).start()
            pltpu.make_async_copy(src, dst, loc_sem.at[color, p]).start()
            pltpu.make_async_remote_copy(src, dst, dag_send.at[color], dag_recv.at[color], device_id=to_pair, device_id_type=MESH).start()
        else:
            s = stage_no - 5
            level = 4 - s
            size = 1 << s
            bit = bits[color][level - 1]
            arrived = base(color, level - 1) + (1 - bit) * size
            wait_on(gat[color].at[c, pl.ds(arrived, size), pl.ds(at, n)], ag_recv.at[color, s, p])
            if s == 0:
                wait_on(gat[color].at[c, base(color, 4), pl.ds(at, n)], loc_sem.at[color, p])
            if s < 3:
                block = gat[color].at[c, pl.ds(base(color, level - 1), 2 * size), pl.ds(at, n)]
                pltpu.make_async_remote_copy(block, block, ag_send.at[color, s + 1], ag_recv.at[color, s + 1, p], device_id=routes[color][level - 2], device_id_type=MESH).start()
            pair_out(color, arrived, size, p)
        if stage_no == 4:
            waited.add((color, p, 4))
            if sum(len(w) == 3 for w in waited) == 2 * len(PIECE):
                cover_to_state()
                for i, dst in enumerate((m_out, v_out, w_out)):
                    pltpu.make_async_copy(stage.at[i, pl.ds(MARGIN, SLICE_ROWS)], dst, state_sem.at[i]).start()

    for i, dst in enumerate((m_out, v_out, w_out)):
        wait_on(dst, state_sem.at[i])
    for color in (0, 1):
        wait_on(gat[color].at[1 - c], dag_recv.at[color])
        wait_on(gat[color].at[c], dag_send.at[color])
        wait_on(acc[color], pr_send.at[color])
        for s in range(4):
            wait_on(rec[color][s], rs_send.at[color, s])
        wait_on(own[color], ag_send.at[color, 0])
        for s in range(1, 4):
            wait_on(gat[color].at[0, pl.ds(0, 1 << s)], ag_send.at[color, s])


def place_kernel(in_a, in_b, e_out, a_out, f1_out, f2_out, b_out, buf_a, buf_b, in_sem, out_sem):
    outs = (e_out, a_out, f1_out, f2_out, b_out)
    ins, buf = (in_a, in_b), (buf_a, buf_b)
    places = [(color, d) for d in range(NDEV) for color in (0, 1)]
    for color, d in places:
        slot = slot_of(color, d // 2)
        pltpu.make_async_copy(ins[color].at[d % 2, slot], buf[color].at[d], in_sem.at[color, d]).start()
    row = lax.broadcasted_iota(jnp.int32, (32, 128), 0)
    lane = lax.broadcasted_iota(jnp.int32, (32, 128), 1)
    tile_order = (row % 8) * 4 + row // 8
    started = []
    for d in range(NDEV):
        for color in (0, 1):
            pltpu.make_async_copy(ins[color].at[d % 2, slot_of(color, d // 2)], buf[color].at[d], in_sem.at[color, d]).wait()
        first = merge_row(d)
        last = merge_row(d + 1) if d + 1 < NDEV else STARTS[-1]
        if d > 0:
            mine = first - start_row(d)
            his = first - start_row(d - 1) - HALF
            flat = tile_order if PERM_LO <= first < PERM_HI else row
            keep = 2 * flat + lane // 64 >= 3597 * d - 2 * first
            new = buf_a[d, pl.ds(mine, 32), :].astype(jnp.float32)
            old = buf_b[d - 1, pl.ds(his, 32), :].astype(jnp.float32)
            buf_a[d, pl.ds(mine, 32), :] = jnp.where(keep, new, old).astype(jnp.bfloat16)
        for color in (0, 1):
            lo = max(first, start_row(d) + color * HALF)
            hi = min(last, start_row(d) + (color + 1) * HALF)
            for tensor, at, off, n in segments(lo, hi - lo):
                copy = pltpu.make_async_copy(buf[color].at[d, pl.ds(lo + off - start_row(d) - color * HALF, n)], outs[tensor].at[pl.ds(at, n)], out_sem.at[len(started)])
                copy.start()
                started.append(copy)
    for copy in started:
        copy.wait()


def tile_rows(tensor):
    return tensor.reshape(-1, 8, 4, 128).transpose(0, 2, 1, 3).reshape(-1, 128)


def untile(rows, shape):
    return rows.reshape(-1, 4, 8, 128).transpose(0, 2, 1, 3).reshape(shape)


def solution(mesh):
    def local_step(g_embed, g_attn, g_ffn_in, g_ffn_out, g_vec, m_shard, v_shard, w_shard):
        grads = (g_embed[0], tile_rows(g_attn[0]), tile_rows(g_ffn_in[0]), g_ffn_out[0].reshape(-1, 128), g_vec[0].reshape(-1, 128))
        state = [jnp.pad(s, (0, PAD)).reshape(SLICE_ROWS, 128) for s in (m_shard, v_shard, w_shard)]
        any_spec = pl.BlockSpec(memory_space=pl.ANY)
        f32, bf16 = jnp.float32, jnp.bfloat16
        np_ = len(PIECE)
        gathered = jax.ShapeDtypeStruct((2, 16, HALF, 128), bf16)
        flat = jax.ShapeDtypeStruct((SLICE_ROWS, 128), f32)
        both = lambda *shape: [pltpu.VMEM(shape, f32)] * 2
        dma = pltpu.SemaphoreType.DMA
        out_a, out_b, m_new, v_new, w_new = pl.pallas_call(
            big_kernel,
            out_shape=(gathered, gathered, flat, flat, flat),
            in_specs=[any_spec] * 8,
            out_specs=[any_spec] * 5,
            scratch_shapes=both(16, HALF, 128) + both(16, HALF, 128) + both(8, HALF, 128) + both(4, HALF, 128) + both(2, HALF, 128) + both(1, HALF, 128)
            + [pltpu.VMEM((HALF, 128), bf16)] * 2
            + [pltpu.VMEM((3, SLICE_ROWS + 2 * MARGIN, 128), f32), pltpu.VMEM((3, COVER, 128), f32)]
            + [dma((2, len(LOAD))), dma((2, len(LOAD))), dma((2,)), dma((2, 4, np_)), dma((2, 4)), dma((2, 4, np_)), dma((2, 4)), dma((2, np_)), dma((2,)), dma((2,)), dma((3,))],
            compiler_params=pltpu.CompilerParams(collective_id=0, has_side_effects=True, vmem_limit_bytes=62 * 1024 * 1024),
            name='reduce_adam_gather',
        )(*grads, *state)
        placed = pl.pallas_call(
            place_kernel,
            out_shape=[jax.ShapeDtypeStruct((n, 128), bf16) for n in TENSOR_ROWS],
            in_specs=[any_spec] * 2,
            out_specs=[any_spec] * 5,
            scratch_shapes=[pltpu.VMEM((NDEV, HALF, 128), bf16)] * 2 + [dma((2, NDEV)), dma((2 * NDEV + 8,))],
            compiler_params=pltpu.CompilerParams(vmem_limit_bytes=40 * 1024 * 1024),
            name='place',
        )(out_a, out_b)
        e, a, f1, f2, b = placed
        tensors = (e, untile(a, (16, 128, 512)), untile(f1, (16, 128, 512)), f2.reshape(16, 512, 128), b.reshape(16, 1664))
        chip = ((lax.axis_index('outer') * 2 + lax.axis_index('middle')) * 4 + lax.axis_index('inner')) // 2
        blocks = [lax.dynamic_slice_in_dim(e, chip * 2048, 2048, axis=0)]
        for t in (a, f1):
            rows = lax.dynamic_slice_in_dim(t.reshape(16, 16, 32, 128), chip, 1, axis=1)
            blocks.append(untile(rows, (512, 128)))
        blocks.append(lax.dynamic_slice_in_dim(f2.reshape(16, 512, 128), chip * 32, 32, axis=1).reshape(512, 128))
        blocks.append(lax.dynamic_slice_in_dim(tensors[4], chip * 104, 104, axis=1).reshape(13, 128))
        wide = jnp.concatenate([t.astype(f32) for t in blocks], axis=0)
        w_chip = lax.optimization_barrier(wide).reshape(1, -1).astype(bf16)
        state = tuple(s.reshape(-1)[:SLICE] for s in (m_new, v_new, w_new))
        return state + tensors + (w_chip,)

    return jax.shard_map(local_step, mesh=mesh, in_specs=(P(MESH_AXES),) * 8, out_specs=(P(MESH_AXES),) * 3 + (P(),) * 5 + (P(MESH_AXES),), check_vma=False)
```

```python
import functools

import jax
import jax.numpy as jnp
from jax import lax
from jax.experimental import pallas as pl
from jax.experimental.pallas import tpu as pltpu
from jax.sharding import PartitionSpec as P

MESH_AXES = ('outer', 'middle', 'inner')
MESH = pl.DeviceIdType.MESH
BETA1, BETA2, EPS, RATE, STEP = 0.9, 0.98, 1e-9, 0.05, 3

NDEV = 32
GROUP = 32
LANES = 128
TILE = 8
BLOCK = 1024
LAST = NDEV - 1
LAST_START = 55696
SPAN = 3597
COLORS = (0, 1)
REST = 1792
ROWS = 1856
HALF = ROWS // 2
SLICE = 230208
SLICE_ROWS = 1800
MARGIN = 64
VMEM = 62 << 20
COVER = ROWS + 8
TENSOR_ROWS = (32768, 8192, 8192, 8192, 208)
STARTS = (0, 32768, 40960, 49152, 57344, 57552)
PERM_LO, PERM_HI = 32768, 49152
PIECES = (32, 64) + (128,) * 6 + (64,)
LOADS = (32, 64, 128, 256, 448)
E_SLOTS = 9


def bounds(sizes):
    out, at = [], 0
    for n in sizes:
        out.append((at, n))
        at += n
    return out


PIECE = bounds(PIECES)
LOAD = bounds(LOADS)
LOAD_OF = [next(i for i, (a, n) in enumerate(LOAD) if a <= p < a + n) for p, _ in PIECE]
LOAD_MODEL = (2, 0.0136, 3, 40, 0.25)
LINK_RATE = 46600


def start_row(d):
    return LAST_START if d == LAST else 32 * (SPAN * d // 64)


def merge_row(d):
    return 32 * (SPAN * d // 64)


def segments(row, n):
    out = []
    for t in range(5):
        lo, hi = max(row, STARTS[t]), min(row + n, STARTS[t + 1])
        if lo < hi:
            out.append((t, lo - STARTS[t], lo - row, hi - lo))
    return out


def slot_of(color, k):
    x, y, z0, z1 = k % 2, k // 2 % 2, k // 4 % 2, k // 8
    return (x * 8 + z0 * 4 + y * 2 + z1) if color == 0 else (y * 8 + z0 * 4 + x * 2 + z1)


def event_order():
    loaded, rate, hop, ahead, step = LOAD_MODEL
    ready = []
    for at, n in LOAD:
        for color in COLORS:
            loaded += n * rate
        ready.append(loaded)
    waiting = [(ready[LOAD_OF[p]], 0, p, color) for p in range(len(PIECE)) for color in COLORS]
    free = dict.fromkeys('xyz', 0)
    names = ('xzyz', 'yzxz')
    now, events = 0, []
    while waiting:
        def begin(e):
            return max(now, e[0], 0 if e[1] else free[names[e[3]][0]] - ahead)

        at = min(map(begin, waiting))
        time, stage, p, color = e = max((e for e in waiting if begin(e) <= at), key=lambda e: (e[1], -e[2], -e[3]))
        waiting.remove(e)
        events.append(e[1:])
        now = at + step * (1 if stage else 3)
        if stage < 8:
            link = names[color][min(stage, 7 - stage)]
            rows = PIECE[p][1] * (8 >> stage if stage < 4 else (1 << stage) / GROUP)
            free[link] = max(now, free[link]) + rows * LANES * 4 / LINK_RATE
            waiting.append((free[link] + hop, stage + 1, p, color))
    return events


def big_kernel(ge, ga, gf1, gf2, gb, m_in, v_in, w_in, out_a, out_b, m_out, v_out, w_out, acc_a, acc_b, pair_a, pair_b, r1_a, r1_b, r2_a, r2_b, r3_a, r3_b, r4_a, r4_b, own_a, own_b, line_m, line_v, line_w, stage, cov, ld_sem, pr_recv, pr_send, rs_recv, rs_send, ag_recv, ag_send, loc_sem, dag_recv, dag_send, state_sem):
    grads = (ge, ga, gf1, gf2, gb)
    acc, pair, own, gat = (acc_a, acc_b), (pair_a, pair_b), (own_a, own_b), (out_a, out_b)
    rec = ((r1_a, r2_a, r3_a, r4_a), (r1_b, r2_b, r3_b, r4_b))
    z, y, inner = lax.axis_index('outer'), lax.axis_index('middle'), lax.axis_index('inner')
    x, c = inner // 2, inner % 2
    z0, z1 = z % 2, z // 2
    dev = (z * 2 + y) * 4 + inner
    to_pair = {'inner': inner + 1 - 2 * c}
    to_x = {'inner': inner + 2 - 4 * x}
    to_y = {'middle': 1 - y}
    to_z0 = {'outer': z + 1 - 2 * z0}
    to_z1 = {'outer': z + 2 - 4 * z1}
    routes = ((to_x, to_z0, to_y, to_z1), (to_y, to_z0, to_x, to_z1))
    bits = ((x, z0, y, z1), (y, z0, x, z1))

    barrier = pltpu.get_barrier_semaphore()
    for to in (to_pair, to_x, to_y, to_z0, to_z1):
        pl.semaphore_signal(barrier, inc=1, device_id=to, device_id_type=MESH)

    lines = (line_m, line_v, line_w)
    state_in = [pltpu.make_async_copy(src, lines[i], state_sem.at[i]) for i, src in enumerate((m_in, v_in, w_in))]
    for copy in state_in:
        copy.start()
    pl.semaphore_wait(barrier, 5)

    def load_one(color, i, tensor, row, slot, at, n, mine):
        src = grads[tensor].at[pl.ds(row, n)]
        if mine:
            pltpu.make_async_copy(src, acc[color].at[slot, pl.ds(at, n)], ld_sem.at[color, i]).start()
        else:
            pltpu.make_async_remote_copy(src, pair[color].at[slot, pl.ds(at, n)], pr_send.at[color], pr_recv.at[color, i], device_id=to_pair, device_id_type=MESH).start()

    def load(i):
        at, n = LOAD[i]
        for color in COLORS:
            @pl.loop(0, E_SLOTS)
            def _(k):
                slot = slot_of(color, k)
                for mine in (False, True):
                    d = 2 * k + (c if mine else 1 - c)
                    row = pl.multiple_of(GROUP * ((SPAN * d) // 64), GROUP) + color * HALF + at
                    load_one(color, i, 0, row, slot, at, n, mine)
            for core in COLORS:
                @pl.when(c == core)
                def _():
                    for k in range(E_SLOTS, NDEV // 2):
                        slot = slot_of(color, k)
                        for mine in (False, True):
                            d = 2 * k + (core if mine else 1 - core)
                            for tensor, row, off, rows in segments(start_row(d) + color * HALF + at, n):
                                load_one(color, i, tensor, row, slot, at + off, rows, mine)

    def wait_on(ref, sem):
        pltpu.make_async_copy(ref, ref, sem).wait()

    def add(color, into, slots, src, first, at, n):
        @pl.loop(0, slots)
        def _(i):
            acc[color][into + i, pl.ds(at, n), :] += src[first + i, pl.ds(at, n), :]

    def base(color, level):
        return sum((bits[color][i] * (TILE >> i) for i in range(level)), 0 * c)

    def reduce_send(color, s, p):
        at, n = PIECE[p]
        size = TILE >> s
        first = base(color, s) + (1 - bits[color][s]) * size
        pltpu.make_async_remote_copy(acc[color].at[pl.ds(first, size), pl.ds(at, n)], rec[color][s].at[:, pl.ds(at, n)], rs_send.at[color, s], rs_recv.at[color, s, p], device_id=routes[color][s], device_id_type=MESH).start()

    def pair_out(color, slot, size, p):
        at, n = PIECE[p]
        block = gat[color].at[c, pl.ds(slot, size), pl.ds(at, n)]
        pltpu.make_async_remote_copy(block, block, dag_send.at[color], dag_recv.at[color], device_id=to_pair, device_id_type=MESH).start()

    def adam_block(g, load_state, store_state):
        g = g * (1.0 / NDEV)
        m = BETA1 * load_state(0) + (1.0 - BETA1) * g
        v = BETA2 * load_state(1) + (1.0 - BETA2) * (g * g)
        m_hat = m / (1.0 - BETA1 ** STEP)
        v_hat = v / (1.0 - BETA2 ** STEP)
        w = load_state(2) - RATE * m_hat / (jnp.sqrt(v_hat) + EPS)
        store_state(0, m)
        store_state(1, v)
        store_state(2, w)
        return w

    cover_start = jnp.where(dev == LAST, LAST_START, GROUP * ((SPAN * dev) // 64))

    def adam(color, p):
        at, n = PIECE[p]
        slot = base(color, 4)

        @pl.loop(0, n // GROUP)
        def _(j):
            r = pl.multiple_of(at + j * GROUP, GROUP)
            f = pl.multiple_of(color * HALF + r, GROUP)
            row = cover_start + f
            permuted = (row >= PERM_LO) & (row < PERM_HI)

            def group(index):
                for t in range(2):
                    parts = []
                    for q in (2 * t, 2 * t + 1):
                        where = index(f, q)

                        def keep(i, value, where=where):
                            cov[i, where, :] = value

                        parts.append(adam_block(acc[color][slot, pl.ds(r + TILE * q, TILE), :], lambda i, where=where: cov[i, where, :], keep))
                    own[color][pl.ds(r + 16 * t, 16), :] = jnp.concatenate(parts, axis=0).astype(jnp.bfloat16)

            @pl.when(permuted)
            def _():
                group(lambda f, q: pl.ds(f + q, TILE, stride=4))

            @pl.when(jnp.logical_not(permuted))
            def _():
                group(lambda f, q: pl.ds(f + TILE * q, TILE))

    half_rows = jnp.where(dev == LAST, 115, (SPAN * dev) % 64)
    shift = half_rows // 2
    lane = lax.broadcasted_iota(jnp.int32, (GROUP, LANES), 1)

    def moved(first, second):
        return jnp.where(lane < 64, pltpu.roll(first, 64, 1), pltpu.roll(second, 64, 1))

    def state_rows():
        for i, copy in enumerate(state_in):
            copy.wait()
            stage[i, 0:MARGIN, :] = jnp.zeros((MARGIN, LANES), jnp.float32)
            stage[i, MARGIN + SLICE_ROWS - TILE:, :] = jnp.zeros((MARGIN + TILE, LANES), jnp.float32)
            cov[i, ROWS:, :] = jnp.zeros((COVER - ROWS, LANES), jnp.float32)
            for r in range(REST, 1798):
                stage[i, MARGIN + r:MARGIN + r + 1, :] = lines[i][LANES * r:LANES * r + LANES].reshape(1, LANES)
            stage[i, MARGIN + 1798:MARGIN + 1799, 0:64] = lines[i][SLICE - 64:].reshape(1, 64)

    def state_rows_part(t):
        @pl.loop(GROUP * t, GROUP * t + GROUP)
        def _(j):
            for i in range(3):
                stage[i, pl.ds(pl.multiple_of(MARGIN + j * TILE, TILE), TILE), :] = lines[i][pl.ds(pl.multiple_of(j * BLOCK, BLOCK), BLOCK)].reshape(TILE, LANES)

    def state_to_cover(t):
        @pl.loop(6 * t, min(6 * t + 6, ROWS // GROUP))
        def _(j):
            f = pl.multiple_of(j * GROUP, GROUP)
            r = MARGIN + f - shift
            for i in range(3):
                here = stage[i, pl.ds(r, GROUP), :]
                before = stage[i, pl.ds(r - 1, GROUP), :]
                cov[i, pl.ds(f, GROUP), :] = jnp.where(c == 1, moved(before, here), here)

    def cover_to_state(t):
        @pl.loop(15 * t, 15 * t + 15)
        def _(j):
            r = pl.multiple_of(j * TILE, TILE)
            for i in range(3):
                here = cov[i, pl.ds(r + shift, TILE), :]
                after = cov[i, pl.ds(r + shift + 1, TILE), :]
                both = jnp.where(lane[:TILE] < 64, pltpu.roll(here, 64, 1), pltpu.roll(after, 64, 1))
                stage[i, pl.ds(pl.multiple_of(MARGIN + r, TILE), TILE), :] = jnp.where(c == 1, both, here)

    def state_out():
        for i, dst in enumerate((m_out, v_out, w_out)):
            pltpu.make_async_copy(stage.at[i, pl.ds(MARGIN, SLICE_ROWS)], dst, state_sem.at[i]).start()

    before_adam = [state_rows] + [functools.partial(state_rows_part, t) for t in range(7)] + [functools.partial(state_to_cover, t) for t in range(10)]
    after_adam = [functools.partial(cover_to_state, t) for t in range(15)] + [state_out]
    adams_left = 2 * len(PIECE)
    load(0)
    load(1)
    events = event_order()
    loads_started = 2
    waited = set()
    for place, (stage_no, p, color) in enumerate(events):
        at, n = PIECE[p]
        if stage_no == 0:
            i = LOAD_OF[p]
            while loads_started < min(i + 2, len(LOAD)):
                load(loads_started)
                loads_started += 1
            if (color, i) not in waited:
                waited.add((color, i))
                la, ln = LOAD[i]
                wait_on(acc[color].at[:, pl.ds(la, ln)], ld_sem.at[color, i])
                wait_on(pair[color].at[:, pl.ds(la, ln)], pr_recv.at[color, i])
            away, home = (1 - bits[color][0]) * TILE, bits[color][0] * TILE
            add(color, away, TILE, pair[color], away, at, n)
            add(color, home, TILE, pair[color], home, at, n)
            reduce_send(color, 0, p)
        elif stage_no < 4:
            s = stage_no - 1
            size = 4 >> s
            wait_on(rec[color][s].at[:, pl.ds(at, n)], rs_recv.at[color, s, p])
            first = base(color, stage_no)
            bit = bits[color][stage_no]
            add(color, first + (1 - bit) * size, size, rec[color][s], (1 - bit) * size, at, n)
            add(color, first + bit * size, size, rec[color][s], bit * size, at, n)
            reduce_send(color, stage_no, p)
        elif stage_no == 4:
            while before_adam:
                before_adam.pop(0)()
            adams_left -= 1
            wait_on(rec[color][3].at[:, pl.ds(at, n)], rs_recv.at[color, 3, p])
            slot = base(color, 4)
            add(color, slot, 1, rec[color][3], 0, at, n)
            adam(color, p)
            src = own[color].at[pl.ds(at, n)]
            dst = gat[color].at[c, slot, pl.ds(at, n)]
            pltpu.make_async_remote_copy(src, dst, ag_send.at[color, 0], ag_recv.at[color, 0, p], device_id=to_z1, device_id_type=MESH).start()
            pltpu.make_async_copy(src, dst, loc_sem.at[color, p]).start()
            pltpu.make_async_remote_copy(src, dst, dag_send.at[color], dag_recv.at[color], device_id=to_pair, device_id_type=MESH).start()
        else:
            s = stage_no - 5
            level = 4 - s
            size = 1 << s
            bit = bits[color][level - 1]
            arrived = base(color, level - 1) + (1 - bit) * size
            wait_on(gat[color].at[c, pl.ds(arrived, size), pl.ds(at, n)], ag_recv.at[color, s, p])
            if s == 0:
                wait_on(gat[color].at[c, base(color, 4), pl.ds(at, n)], loc_sem.at[color, p])
            if s < 3:
                block = gat[color].at[c, pl.ds(base(color, level - 1), 2 * size), pl.ds(at, n)]
                pltpu.make_async_remote_copy(block, block, ag_send.at[color, s + 1], ag_recv.at[color, s + 1, p], device_id=routes[color][level - 2], device_id_type=MESH).start()
            pair_out(color, arrived, size, p)
        if place >= 4 and before_adam:
            before_adam.pop(0)()
        if adams_left == 0 and after_adam:
            after_adam.pop(0)()
    for job in after_adam:
        job()

    for i, dst in enumerate((m_out, v_out, w_out)):
        wait_on(dst, state_sem.at[i])
    for color in COLORS:
        wait_on(gat[color].at[1 - c], dag_recv.at[color])
        wait_on(gat[color].at[c], dag_send.at[color])
        wait_on(acc[color], pr_send.at[color])
        for s in range(4):
            wait_on(rec[color][s], rs_send.at[color, s])
        wait_on(own[color], ag_send.at[color, 0])
        for s in range(1, 4):
            wait_on(gat[color].at[0, pl.ds(0, 1 << s)], ag_send.at[color, s])


def place_kernel(in_a, in_b, m_in, v_in, w_in, e_out, a_out, f1_out, f2_out, b_out, m_out, v_out, w_out, chip_out, buf, state, loose, vec, tail, block, in_sem, out_sem, state_sem, chip_sem):
    outs = (e_out, a_out, f1_out, f2_out, b_out)
    ins = (in_a, in_b)
    chip = (lax.axis_index('outer') * 2 + lax.axis_index('middle')) * 2 + lax.axis_index('inner') // 2

    def arriving(color, d):
        return pltpu.make_async_copy(ins[color].at[d % 2, slot_of(color, d // 2)], buf.at[d, pl.ds(color * HALF, HALF)], in_sem.at[color, d])

    for d in range(NDEV):
        for color in COLORS:
            arriving(color, d).start()
    kept = [(pltpu.make_async_copy(src, state.at[i], state_sem.at[i]), pltpu.make_async_copy(state.at[i], dst, state_sem.at[i])) for i, (src, dst) in enumerate(((m_in, m_out), (v_in, v_out), (w_in, w_out)))]
    for first, _ in kept:
        first.start()
    row = lax.broadcasted_iota(jnp.int32, (GROUP, LANES), 0)
    lane = lax.broadcasted_iota(jnp.int32, (GROUP, LANES), 1)
    tile_order = (row % TILE) * 4 + row // TILE
    started = []
    for d in range(NDEV):
        for color in COLORS:
            arriving(color, d).wait()
        first = merge_row(d)
        last = merge_row(d + 1) if d + 1 < NDEV else STARTS[-1]
        mine = first - start_row(d)
        if d > 0:
            his = first - start_row(d - 1)
            flat = tile_order if PERM_LO <= first < PERM_HI else row
            keep = 2 * flat + lane // 64 >= SPAN * d - 2 * first
            new = buf[d, mine:mine + GROUP, :].astype(jnp.float32)
            old = buf[d - 1, his:his + GROUP, :].astype(jnp.float32)
            buf[d, mine:mine + GROUP, :] = jnp.where(keep, new, old).astype(jnp.bfloat16)
        for tensor, at, off, n in segments(first, last - first):
            copy = pltpu.make_async_copy(buf.at[d, pl.ds(mine + off, n)], outs[tensor].at[pl.ds(at, n)], out_sem.at[len(started)])
            copy.start()
            started.append(copy)
    for first, second in kept:
        first.wait()
        second.start()

    def rows_of(group):
        d = (64 * group + 63) // SPAN
        begin = jnp.where(d == LAST, LAST_START, GROUP * ((SPAN * d) // 64))
        return buf[d, pl.ds(pl.multiple_of(GROUP * group - begin, 16), GROUP), :].astype(jnp.float32)

    def put(at, rows):
        block[0:1, pl.ds(pl.multiple_of(at * LANES, BLOCK), BLOCK)] = rows.reshape(1, BLOCK).astype(jnp.bfloat16)

    @pl.loop(0, 64)
    def _(j):
        rows = rows_of(chip * 64 + j)
        for q in range(4):
            put(GROUP * j + TILE * q, rows[TILE * q:TILE * q + TILE])

    @pl.loop(0, 16)
    def _(layer):
        for t in (1, 2):
            rows = rows_of(STARTS[t] // GROUP + layer * 16 + chip)
            for q in range(4):
                loose[t - 1, pl.ds(q, TILE, stride=4), :] = rows[TILE * q:TILE * q + TILE]
            for q in range(4):
                put(1536 + 512 * t + GROUP * layer + TILE * q, loose[t - 1, TILE * q:TILE * q + TILE, :])
        rows = rows_of(STARTS[3] // GROUP + layer * 16 + chip)
        for q in range(4):
            put(3072 + GROUP * layer + TILE * q, rows[TILE * q:TILE * q + TILE])

    at = STARTS[4] - start_row(LAST)
    vec[0:208, :] = buf[LAST, at:at + 208, :].astype(jnp.float32)
    vec[208:, :] = jnp.zeros((16, LANES), jnp.float32)
    tail[...] = jnp.zeros_like(tail)
    begin = (104 * chip) % LANES
    line = lax.broadcasted_iota(jnp.int32, (TILE, LANES), 1)
    for layer in range(16):
        source = layer * 13 + (104 * chip) // LANES
        to = layer * 104 // LANES
        off = layer * 104 % LANES
        turn = (off - begin + LANES) % LANES
        one = pltpu.roll(vec[pl.ds(source, TILE), :], turn, 1)
        two = pltpu.roll(vec[pl.ds(source + 1, TILE), :], turn, 1)
        t = (line - off + LANES) % LANES
        got = jnp.where(begin + t < LANES, one, two)
        here = (t < 104) & (line >= off)
        tail[to:to + 1, :] = jnp.where(here, got, tail[pl.ds(to, TILE), :])[0:1]
        if off + 104 > LANES:
            there = (t < 104) & (line < off)
            tail[to + 1:to + 2, :] = jnp.where(there, got, tail[pl.ds(to + 1, TILE), :])[0:1]
    put(3584, tail[0:TILE, :])
    block[0:1, 3592 * LANES:] = tail[TILE:16, :].reshape(1, BLOCK)[:, 0:640].astype(jnp.bfloat16)
    send = pltpu.make_async_copy(block, chip_out, chip_sem)
    send.start()
    for copy in started:
        copy.wait()
    for _, second in kept:
        second.wait()
    send.wait()


def tile_rows(tensor):
    return tensor.reshape(-1, TILE, 4, LANES).transpose(0, 2, 1, 3).reshape(-1, LANES)


def untile(rows, shape):
    return rows.reshape(-1, 4, TILE, LANES).transpose(0, 2, 1, 3).reshape(shape)


def solution(mesh):
    def local_step(g_embed, g_attn, g_ffn_in, g_ffn_out, g_vec, m_shard, v_shard, w_shard):
        grads = (g_embed[0], tile_rows(g_attn[0]), tile_rows(g_ffn_in[0]), g_ffn_out[0].reshape(-1, LANES), g_vec[0].reshape(-1, LANES))
        state = (m_shard, v_shard, w_shard)
        any_spec = pl.BlockSpec(memory_space=pl.ANY)
        f32, bf16 = jnp.float32, jnp.bfloat16
        np_ = len(PIECE)
        gathered = jax.ShapeDtypeStruct((2, 16, HALF, LANES), bf16)
        flat = jax.ShapeDtypeStruct((SLICE_ROWS, LANES), f32)
        both = lambda *shape: [pltpu.VMEM(shape, f32)] * 2
        dma = pltpu.SemaphoreType.DMA
        out_a, out_b, m_new, v_new, w_new = pl.pallas_call(
            big_kernel,
            out_shape=(gathered, gathered, flat, flat, flat),
            in_specs=[any_spec] * TILE,
            out_specs=[any_spec] * 5,
            scratch_shapes=both(16, HALF, LANES) + both(16, HALF, LANES) + both(TILE, HALF, LANES) + both(4, HALF, LANES) + both(2, HALF, LANES) + both(1, HALF, LANES)
            + [pltpu.VMEM((HALF, LANES), bf16)] * 2
            + [pltpu.VMEM((SLICE,), f32)] * 3 + [pltpu.VMEM((3, SLICE_ROWS + 2 * MARGIN, LANES), f32), pltpu.VMEM((3, COVER, LANES), f32)]
            + [dma((2, len(LOAD))), dma((2, len(LOAD))), dma((2,)), dma((2, 4, np_)), dma((2, 4)), dma((2, 4, np_)), dma((2, 4)), dma((2, np_)), dma((2,)), dma((2,)), dma((3,))],
            compiler_params=pltpu.CompilerParams(collective_id=0, has_side_effects=True, vmem_limit_bytes=VMEM),
            name='reduce_adam_gather',
        )(*grads, *state)
        placed = pl.pallas_call(
            place_kernel,
            out_shape=[jax.ShapeDtypeStruct((n, LANES), bf16) for n in TENSOR_ROWS] + [flat] * 3 + [jax.ShapeDtypeStruct((1, 2 * SLICE), bf16)],
            in_specs=[any_spec] * 5,
            out_specs=[any_spec] * 9,
            scratch_shapes=[pltpu.VMEM((NDEV, ROWS, LANES), bf16), pltpu.VMEM((3, SLICE_ROWS, LANES), f32), pltpu.VMEM((2, GROUP, LANES), f32), pltpu.VMEM((224, LANES), f32), pltpu.VMEM((24, LANES), f32), pltpu.VMEM((1, 2 * SLICE), bf16)]
            + [dma((2, NDEV)), dma((2 * NDEV,)), dma((3,)), dma(())],
            compiler_params=pltpu.CompilerParams(vmem_limit_bytes=VMEM),
            name='place',
        )(out_a, out_b, m_new, v_new, w_new)
        e, a, f1, f2, b, *state, w_chip = placed
        tensors = (e, untile(a, (16, LANES, 512)), untile(f1, (16, LANES, 512)), f2.reshape(16, 512, LANES), b.reshape(16, 1664))
        return tuple(t.reshape(-1)[:SLICE] for t in state) + tensors + (w_chip,)

    return jax.shard_map(local_step, mesh=mesh, in_specs=(P(MESH_AXES),) * TILE, out_specs=(P(MESH_AXES),) * 3 + (P(),) * 5 + (P(MESH_AXES),), check_vma=False)
```

```python
import functools

import jax
import jax.numpy as jnp
from jax import lax
from jax.experimental import pallas as pl
from jax.experimental.pallas import tpu as pltpu
from jax.sharding import PartitionSpec as P

MESH_AXES = ('outer', 'middle', 'inner')
MESH = pl.DeviceIdType.MESH
BETA1, BETA2, EPS, RATE, STEP = 0.9, 0.98, 1e-9, 0.05, 3

NDEV = 32
GROUP = 32
LANES = 128
TILE = 8
BLOCK = 1024
LAST = NDEV - 1
LAST_START = 55696
SPAN = 3597
COLORS = (0, 1)
REST = 1792
ROWS = 1856
HALF = ROWS // 2
SLICE = 230208
SLICE_ROWS = 1800
MARGIN = 64
VMEM = 62 << 20
COVER = ROWS + 8
TENSOR_ROWS = (32768, 8192, 8192, 8192, 208)
STARTS = (0, 32768, 40960, 49152, 57344, 57552)
PERM_LO, PERM_HI = 32768, 49152
LOADS = (32, 64, 128, 256, 448)
E_SLOTS = 9


def bounds(sizes):
    out, at = [], 0
    for n in sizes:
        out.append((at, n))
        at += n
    return out


LOAD = bounds(LOADS)
PIECES = HALF // GROUP
LAGS = ((0, 3, 6, 8, 12, 19, 32, 36, 53), (0, 3, 6, 10, 16, 20, 31, 35, 52))
SEQUENCE = ((8, 0), (6, 0), (8, 1), (7, 0), (2, 0), (3, 1), (1, 0), (0, 0), (5, 1), (5, 0), (4, 1), (6, 1), (4, 0), (2, 1), (1, 1), (0, 1), (3, 0), (7, 1))
STEPS = PIECES + max(map(max, LAGS))
FIRST_ADAM = min(lags[4] for lags in LAGS)
LAST_ADAM = max(lags[4] for lags in LAGS) + PIECES - 1
MOVES = FIRST_ADAM - 6


def start_row(d):
    return LAST_START if d == LAST else 32 * (SPAN * d // 64)


def merge_row(d):
    return 32 * (SPAN * d // 64)


def segments(row, n):
    out = []
    for t in range(5):
        lo, hi = max(row, STARTS[t]), min(row + n, STARTS[t + 1])
        if lo < hi:
            out.append((t, lo - STARTS[t], lo - row, hi - lo))
    return out


def slot_of(color, k):
    x, y, z0, z1 = k % 2, k // 2 % 2, k // 4 % 2, k // 8
    return (x * 8 + z0 * 4 + y * 2 + z1) if color == 0 else (y * 8 + z0 * 4 + x * 2 + z1)


def big_kernel(ge, ga, gf1, gf2, gb, m_in, v_in, w_in, out_a, out_b, m_out, v_out, w_out, acc_a, acc_b, pair_a, pair_b, r1_a, r1_b, r2_a, r2_b, r3_a, r3_b, r4_a, r4_b, own_a, own_b, line_m, line_v, line_w, stage, cov, ld_sem, pr_recv, pr_send, rs_recv, rs_send, ag_recv, ag_send, loc_sem, dag_recv, dag_send, state_sem):
    grads = (ge, ga, gf1, gf2, gb)
    acc, pair, own, gat = (acc_a, acc_b), (pair_a, pair_b), (own_a, own_b), (out_a, out_b)
    rec = ((r1_a, r2_a, r3_a, r4_a), (r1_b, r2_b, r3_b, r4_b))
    z, y, inner = lax.axis_index('outer'), lax.axis_index('middle'), lax.axis_index('inner')
    x, c = inner // 2, inner % 2
    z0, z1 = z % 2, z // 2
    dev = (z * 2 + y) * 4 + inner
    to_pair = {'inner': inner + 1 - 2 * c}
    to_x = {'inner': inner + 2 - 4 * x}
    to_y = {'middle': 1 - y}
    to_z0 = {'outer': z + 1 - 2 * z0}
    to_z1 = {'outer': z + 2 - 4 * z1}
    routes = ((to_x, to_z0, to_y, to_z1), (to_y, to_z0, to_x, to_z1))
    bits = ((x, z0, y, z1), (y, z0, x, z1))

    barrier = pltpu.get_barrier_semaphore()
    for to in (to_pair, to_x, to_y, to_z0, to_z1):
        pl.semaphore_signal(barrier, inc=1, device_id=to, device_id_type=MESH)

    lines = (line_m, line_v, line_w)
    state_in = [pltpu.make_async_copy(src, lines[i], state_sem.at[i]) for i, src in enumerate((m_in, v_in, w_in))]
    for copy in state_in:
        copy.start()
    pl.semaphore_wait(barrier, 5)

    def load_one(color, i, tensor, row, slot, at, n, mine):
        src = grads[tensor].at[pl.ds(row, n)]
        if mine:
            pltpu.make_async_copy(src, acc[color].at[slot, pl.ds(at, n)], ld_sem.at[color, i]).start()
        else:
            pltpu.make_async_remote_copy(src, pair[color].at[slot, pl.ds(at, n)], pr_send.at[color], pr_recv.at[color, i], device_id=to_pair, device_id_type=MESH).start()

    def load(i):
        at, n = LOAD[i]
        for color in COLORS:
            @pl.loop(0, E_SLOTS)
            def _(k):
                slot = slot_of(color, k)
                for mine in (False, True):
                    d = 2 * k + (c if mine else 1 - c)
                    row = pl.multiple_of(GROUP * ((SPAN * d) // 64), GROUP) + color * HALF + at
                    load_one(color, i, 0, row, slot, at, n, mine)
            for core in COLORS:
                @pl.when(c == core)
                def _():
                    for k in range(E_SLOTS, NDEV // 2):
                        slot = slot_of(color, k)
                        for mine in (False, True):
                            d = 2 * k + (core if mine else 1 - core)
                            for tensor, row, off, rows in segments(start_row(d) + color * HALF + at, n):
                                load_one(color, i, tensor, row, slot, at + off, rows, mine)

    def wait_on(ref, sem):
        pltpu.make_async_copy(ref, ref, sem).wait()

    def rows_at(p):
        return pl.ds(pl.multiple_of(p * GROUP, GROUP), GROUP)

    def add(color, into, slots, src, first, p):
        acc[color][pl.ds(into, slots), rows_at(p), :] += src[pl.ds(first, slots), rows_at(p), :]

    def base(color, level):
        return sum((bits[color][i] * (TILE >> i) for i in range(level)), 0 * c)

    def reduce_send(color, s, p):
        size = TILE >> s
        first = base(color, s) + (1 - bits[color][s]) * size
        pltpu.make_async_remote_copy(acc[color].at[pl.ds(first, size), rows_at(p)], rec[color][s].at[:, rows_at(p)], rs_send.at[color, s], rs_recv.at[color, s, p], device_id=routes[color][s], device_id_type=MESH).start()

    def pair_out(color, slot, size, p):
        block = gat[color].at[c, pl.ds(slot, size), rows_at(p)]
        pltpu.make_async_remote_copy(block, block, dag_send.at[color], dag_recv.at[color], device_id=to_pair, device_id_type=MESH).start()

    def adam_block(g, load_state, store_state):
        g = g * (1.0 / NDEV)
        m = BETA1 * load_state(0) + (1.0 - BETA1) * g
        v = BETA2 * load_state(1) + (1.0 - BETA2) * (g * g)
        m_hat = m / (1.0 - BETA1 ** STEP)
        v_hat = v / (1.0 - BETA2 ** STEP)
        w = load_state(2) - RATE * m_hat / (jnp.sqrt(v_hat) + EPS)
        store_state(0, m)
        store_state(1, v)
        store_state(2, w)
        return w

    cover_start = jnp.where(dev == LAST, LAST_START, GROUP * ((SPAN * dev) // 64))

    def adam(color, p):
        slot = base(color, 4)
        r = pl.multiple_of(p * GROUP, GROUP)
        f = pl.multiple_of(color * HALF + r, GROUP)
        row = cover_start + f
        permuted = (row >= PERM_LO) & (row < PERM_HI)

        def group(index):
            for t in range(2):
                parts = []
                for q in (2 * t, 2 * t + 1):
                    where = index(f, q)

                    def keep(i, value, where=where):
                        cov[i, where, :] = value

                    parts.append(adam_block(acc[color][slot, pl.ds(r + TILE * q, TILE), :], lambda i, where=where: cov[i, where, :], keep))
                own[color][pl.ds(r + 16 * t, 16), :] = jnp.concatenate(parts, axis=0).astype(jnp.bfloat16)

        @pl.when(permuted)
        def _():
            group(lambda f, q: pl.ds(f + q, TILE, stride=4))

        @pl.when(jnp.logical_not(permuted))
        def _():
            group(lambda f, q: pl.ds(f + TILE * q, TILE))

    half_rows = jnp.where(dev == LAST, 115, (SPAN * dev) % 64)
    shift = half_rows // 2
    lane = lax.broadcasted_iota(jnp.int32, (GROUP, LANES), 1)

    def moved(first, second):
        return jnp.where(lane < 64, pltpu.roll(first, 64, 1), pltpu.roll(second, 64, 1))

    def state_rows():
        for i, copy in enumerate(state_in):
            copy.wait()
            stage[i, 0:MARGIN, :] = jnp.zeros((MARGIN, LANES), jnp.float32)
            stage[i, MARGIN + SLICE_ROWS - TILE:, :] = jnp.zeros((MARGIN + TILE, LANES), jnp.float32)
            cov[i, ROWS:, :] = jnp.zeros((COVER - ROWS, LANES), jnp.float32)
            for r in range(REST, 1798):
                stage[i, MARGIN + r:MARGIN + r + 1, :] = lines[i][LANES * r:LANES * r + LANES].reshape(1, LANES)
            stage[i, MARGIN + 1798:MARGIN + 1799, 0:64] = lines[i][SLICE - 64:].reshape(1, 64)

    def state_rows_part(t):
        @pl.loop(0, 56)
        def _(k):
            j = t * 56 + k
            for i in range(3):
                stage[i, pl.ds(pl.multiple_of(MARGIN + j * TILE, TILE), TILE), :] = lines[i][pl.ds(pl.multiple_of(j * BLOCK, BLOCK), BLOCK)].reshape(TILE, LANES)

    def state_to_cover(t):
        @pl.loop(0, -(-ROWS // GROUP // MOVES))
        def _(k):
            f = pl.multiple_of(jnp.minimum((t + k * MOVES) * GROUP, ROWS - GROUP), GROUP)
            r = MARGIN + f - shift
            for i in range(3):
                here = stage[i, pl.ds(r, GROUP), :]
                before = stage[i, pl.ds(r - 1, GROUP), :]
                cov[i, pl.ds(f, GROUP), :] = jnp.where(c == 1, moved(before, here), here)

    def cover_to_state(t):
        @pl.loop(0, 15)
        def _(k):
            r = pl.multiple_of((t * 15 + k) * TILE, TILE)
            for i in range(3):
                here = cov[i, pl.ds(r + shift, TILE), :]
                after = cov[i, pl.ds(r + shift + 1, TILE), :]
                both = jnp.where(lane[:TILE] < 64, pltpu.roll(here, 64, 1), pltpu.roll(after, 64, 1))
                stage[i, pl.ds(pl.multiple_of(MARGIN + r, TILE), TILE), :] = jnp.where(c == 1, both, here)

    def state_out():
        for i, dst in enumerate((m_out, v_out, w_out)):
            pltpu.make_async_copy(stage.at[i, pl.ds(MARGIN, SLICE_ROWS)], dst, state_sem.at[i]).start()

    def start_pieces(color, p):
        for i, (first, n) in enumerate(LOAD):
            @pl.when(p == first // GROUP)
            def _():
                wait_on(acc[color].at[:, pl.ds(first, n)], ld_sem.at[color, i])
                wait_on(pair[color].at[:, pl.ds(first, n)], pr_recv.at[color, i])
        bit = bits[color][0]
        for slot in ((1 - bit) * TILE, bit * TILE):
            add(color, slot, TILE, pair[color], slot, p)
        reduce_send(color, 0, p)

    def reduce_piece(color, stage_no, p):
        s = stage_no - 1
        wait_on(rec[color][s].at[:, rows_at(p)], rs_recv.at[color, s, p])
        first, size, bit = base(color, stage_no), 4 >> s, bits[color][stage_no]
        for half in (1 - bit, bit):
            add(color, first + half * size, size, rec[color][s], half * size, p)
        reduce_send(color, stage_no, p)

    def adam_piece(color, p):
        wait_on(rec[color][3].at[:, rows_at(p)], rs_recv.at[color, 3, p])
        slot = base(color, 4)
        add(color, slot, 1, rec[color][3], 0, p)
        adam(color, p)
        src = own[color].at[rows_at(p)]
        dst = gat[color].at[c, slot, rows_at(p)]
        pltpu.make_async_remote_copy(src, dst, ag_send.at[color, 0], ag_recv.at[color, 0, p], device_id=to_z1, device_id_type=MESH).start()
        pltpu.make_async_copy(src, dst, loc_sem.at[color, p]).start()
        pltpu.make_async_remote_copy(src, dst, dag_send.at[color], dag_recv.at[color], device_id=to_pair, device_id_type=MESH).start()

    def gather_piece(color, s, p):
        level, size = 4 - s, 1 << s
        bit = bits[color][level - 1]
        arrived = base(color, level - 1) + (1 - bit) * size
        wait_on(gat[color].at[c, pl.ds(arrived, size), rows_at(p)], ag_recv.at[color, s, p])
        if s == 0:
            wait_on(gat[color].at[c, base(color, 4), rows_at(p)], loc_sem.at[color, p])
        if s < 3:
            block = gat[color].at[c, pl.ds(base(color, level - 1), 2 * size), rows_at(p)]
            pltpu.make_async_remote_copy(block, block, ag_send.at[color, s + 1], ag_recv.at[color, s + 1, p], device_id=routes[color][level - 2], device_id_type=MESH).start()
        pair_out(color, arrived, size, p)

    load(0)
    load(1)

    @pl.loop(0, STEPS)
    def _(t):
        for i in range(2, len(LOAD)):
            pl.when(t == LOAD[i - 1][0] // GROUP)(functools.partial(load, i))
        for stage_no, color in SEQUENCE:
            p = t - LAGS[color][stage_no]

            @pl.when((p >= 0) & (p < PIECES))
            def _():
                if stage_no == 0:
                    start_pieces(color, p)
                elif stage_no < 4:
                    reduce_piece(color, stage_no, p)
                elif stage_no == 4:
                    adam_piece(color, p)
                else:
                    gather_piece(color, stage_no - 5, p)

        @pl.when(t == 1)
        def _():
            state_rows()

        @pl.when((t >= 2) & (t < 6))
        def _():
            state_rows_part(t - 2)

        @pl.when((t >= 6) & (t < FIRST_ADAM))
        def _():
            state_to_cover(t - 6)

        @pl.when((t > LAST_ADAM) & (t <= LAST_ADAM + 15))
        def _():
            cover_to_state(t - LAST_ADAM - 1)

    for i, dst in enumerate((m_out, v_out, w_out)):
        pltpu.make_async_copy(stage.at[i, pl.ds(MARGIN, SLICE_ROWS)], dst, state_sem.at[i]).start()
    for i, dst in enumerate((m_out, v_out, w_out)):
        wait_on(dst, state_sem.at[i])
    for color in COLORS:
        wait_on(gat[color].at[1 - c], dag_recv.at[color])
        wait_on(gat[color].at[c], dag_send.at[color])
        wait_on(acc[color], pr_send.at[color])
        for s in range(4):
            wait_on(rec[color][s], rs_send.at[color, s])
        wait_on(own[color], ag_send.at[color, 0])
        for s in range(1, 4):
            wait_on(gat[color].at[0, pl.ds(0, 1 << s)], ag_send.at[color, s])


def place_kernel(in_a, in_b, m_in, v_in, w_in, e_out, a_out, f1_out, f2_out, b_out, m_out, v_out, w_out, chip_out, buf, state, loose, vec, tail, block, in_sem, out_sem, state_sem, chip_sem):
    outs = (e_out, a_out, f1_out, f2_out, b_out)
    ins = (in_a, in_b)
    chip = (lax.axis_index('outer') * 2 + lax.axis_index('middle')) * 2 + lax.axis_index('inner') // 2

    def arriving(color, d):
        return pltpu.make_async_copy(ins[color].at[d % 2, slot_of(color, d // 2)], buf.at[d, pl.ds(color * HALF, HALF)], in_sem.at[color, d])

    for d in range(NDEV):
        for color in COLORS:
            arriving(color, d).start()
    kept = [(pltpu.make_async_copy(src, state.at[i], state_sem.at[i]), pltpu.make_async_copy(state.at[i], dst, state_sem.at[i])) for i, (src, dst) in enumerate(((m_in, m_out), (v_in, v_out), (w_in, w_out)))]
    for first, _ in kept:
        first.start()
    row = lax.broadcasted_iota(jnp.int32, (GROUP, LANES), 0)
    lane = lax.broadcasted_iota(jnp.int32, (GROUP, LANES), 1)
    tile_order = (row % TILE) * 4 + row // TILE
    started = []
    for d in range(NDEV):
        for color in COLORS:
            arriving(color, d).wait()
        first = merge_row(d)
        last = merge_row(d + 1) if d + 1 < NDEV else STARTS[-1]
        mine = first - start_row(d)
        if d > 0:
            his = first - start_row(d - 1)
            flat = tile_order if PERM_LO <= first < PERM_HI else row
            keep = 2 * flat + lane // 64 >= SPAN * d - 2 * first
            new = buf[d, mine:mine + GROUP, :].astype(jnp.float32)
            old = buf[d - 1, his:his + GROUP, :].astype(jnp.float32)
            buf[d, mine:mine + GROUP, :] = jnp.where(keep, new, old).astype(jnp.bfloat16)
        for tensor, at, off, n in segments(first, last - first):
            copy = pltpu.make_async_copy(buf.at[d, pl.ds(mine + off, n)], outs[tensor].at[pl.ds(at, n)], out_sem.at[len(started)])
            copy.start()
            started.append(copy)
    for first, second in kept:
        first.wait()
        second.start()

    def rows_of(group):
        d = (64 * group + 63) // SPAN
        begin = jnp.where(d == LAST, LAST_START, GROUP * ((SPAN * d) // 64))
        return buf[d, pl.ds(pl.multiple_of(GROUP * group - begin, 16), GROUP), :].astype(jnp.float32)

    def put(at, rows):
        block[0:1, pl.ds(pl.multiple_of(at * LANES, BLOCK), BLOCK)] = rows.reshape(1, BLOCK).astype(jnp.bfloat16)

    @pl.loop(0, 64)
    def _(j):
        rows = rows_of(chip * 64 + j)
        for q in range(4):
            put(GROUP * j + TILE * q, rows[TILE * q:TILE * q + TILE])

    @pl.loop(0, 16)
    def _(layer):
        for t in (1, 2):
            rows = rows_of(STARTS[t] // GROUP + layer * 16 + chip)
            for q in range(4):
                loose[t - 1, pl.ds(q, TILE, stride=4), :] = rows[TILE * q:TILE * q + TILE]
            for q in range(4):
                put(1536 + 512 * t + GROUP * layer + TILE * q, loose[t - 1, TILE * q:TILE * q + TILE, :])
        rows = rows_of(STARTS[3] // GROUP + layer * 16 + chip)
        for q in range(4):
            put(3072 + GROUP * layer + TILE * q, rows[TILE * q:TILE * q + TILE])

    at = STARTS[4] - start_row(LAST)
    vec[0:208, :] = buf[LAST, at:at + 208, :].astype(jnp.float32)
    vec[208:, :] = jnp.zeros((16, LANES), jnp.float32)
    tail[...] = jnp.zeros_like(tail)
    begin = (104 * chip) % LANES
    line = lax.broadcasted_iota(jnp.int32, (TILE, LANES), 1)
    for layer in range(16):
        source = layer * 13 + (104 * chip) // LANES
        to = layer * 104 // LANES
        off = layer * 104 % LANES
        turn = (off - begin + LANES) % LANES
        one = pltpu.roll(vec[pl.ds(source, TILE), :], turn, 1)
        two = pltpu.roll(vec[pl.ds(source + 1, TILE), :], turn, 1)
        t = (line - off + LANES) % LANES
        got = jnp.where(begin + t < LANES, one, two)
        here = (t < 104) & (line >= off)
        tail[to:to + 1, :] = jnp.where(here, got, tail[pl.ds(to, TILE), :])[0:1]
        if off + 104 > LANES:
            there = (t < 104) & (line < off)
            tail[to + 1:to + 2, :] = jnp.where(there, got, tail[pl.ds(to + 1, TILE), :])[0:1]
    put(3584, tail[0:TILE, :])
    block[0:1, 3592 * LANES:] = tail[TILE:16, :].reshape(1, BLOCK)[:, 0:640].astype(jnp.bfloat16)
    send = pltpu.make_async_copy(block, chip_out, chip_sem)
    send.start()
    for copy in started:
        copy.wait()
    for _, second in kept:
        second.wait()
    send.wait()


def tile_rows(tensor):
    return tensor.reshape(-1, TILE, 4, LANES).transpose(0, 2, 1, 3).reshape(-1, LANES)


def untile(rows, shape):
    return rows.reshape(-1, 4, TILE, LANES).transpose(0, 2, 1, 3).reshape(shape)


def solution(mesh):
    def local_step(g_embed, g_attn, g_ffn_in, g_ffn_out, g_vec, m_shard, v_shard, w_shard):
        grads = (g_embed[0], tile_rows(g_attn[0]), tile_rows(g_ffn_in[0]), g_ffn_out[0].reshape(-1, LANES), g_vec[0].reshape(-1, LANES))
        state = (m_shard, v_shard, w_shard)
        any_spec = pl.BlockSpec(memory_space=pl.ANY)
        f32, bf16 = jnp.float32, jnp.bfloat16
        gathered = jax.ShapeDtypeStruct((2, 16, HALF, LANES), bf16)
        flat = jax.ShapeDtypeStruct((SLICE_ROWS, LANES), f32)
        both = lambda *shape: [pltpu.VMEM(shape, f32)] * 2
        dma = pltpu.SemaphoreType.DMA
        out_a, out_b, m_new, v_new, w_new = pl.pallas_call(
            big_kernel,
            out_shape=(gathered, gathered, flat, flat, flat),
            in_specs=[any_spec] * TILE,
            out_specs=[any_spec] * 5,
            scratch_shapes=both(16, HALF, LANES) + both(16, HALF, LANES) + both(TILE, HALF, LANES) + both(4, HALF, LANES) + both(2, HALF, LANES) + both(1, HALF, LANES)
            + [pltpu.VMEM((HALF, LANES), bf16)] * 2
            + [pltpu.VMEM((SLICE,), f32)] * 3 + [pltpu.VMEM((3, SLICE_ROWS + 2 * MARGIN, LANES), f32), pltpu.VMEM((3, COVER, LANES), f32)]
            + [dma((2, len(LOAD))), dma((2, len(LOAD))), dma((2,)), dma((2, 4, PIECES)), dma((2, 4)), dma((2, 4, PIECES)), dma((2, 4)), dma((2, PIECES)), dma((2,)), dma((2,)), dma((3,))],
            compiler_params=pltpu.CompilerParams(collective_id=0, has_side_effects=True, vmem_limit_bytes=VMEM),
            name='reduce_adam_gather',
        )(*grads, *state)
        placed = pl.pallas_call(
            place_kernel,
            out_shape=[jax.ShapeDtypeStruct((n, LANES), bf16) for n in TENSOR_ROWS] + [flat] * 3 + [jax.ShapeDtypeStruct((1, 2 * SLICE), bf16)],
            in_specs=[any_spec] * 5,
            out_specs=[any_spec] * 9,
            scratch_shapes=[pltpu.VMEM((NDEV, ROWS, LANES), bf16), pltpu.VMEM((3, SLICE_ROWS, LANES), f32), pltpu.VMEM((2, GROUP, LANES), f32), pltpu.VMEM((224, LANES), f32), pltpu.VMEM((24, LANES), f32), pltpu.VMEM((1, 2 * SLICE), bf16)]
            + [dma((2, NDEV)), dma((2 * NDEV,)), dma((3,)), dma(())],
            compiler_params=pltpu.CompilerParams(vmem_limit_bytes=VMEM),
            name='place',
        )(out_a, out_b, m_new, v_new, w_new)
        e, a, f1, f2, b, *state, w_chip = placed
        tensors = (e, untile(a, (16, LANES, 512)), untile(f1, (16, LANES, 512)), f2.reshape(16, 512, LANES), b.reshape(16, 1664))
        return tuple(t.reshape(-1)[:SLICE] for t in state) + tensors + (w_chip,)

    return jax.shard_map(local_step, mesh=mesh, in_specs=(P(MESH_AXES),) * TILE, out_specs=(P(MESH_AXES),) * 3 + (P(),) * 5 + (P(MESH_AXES),), check_vma=False)
```

```python
import functools

import jax
import jax.numpy as jnp
from jax import lax
from jax.experimental import pallas as pl
from jax.experimental.pallas import tpu as pltpu
from jax.sharding import PartitionSpec as P

MESH_AXES = ('outer', 'middle', 'inner')
MESH = pl.DeviceIdType.MESH
BETA1, BETA2, EPS, RATE, STEP = 0.9, 0.98, 1e-9, 0.05, 3

NDEV = 32
GROUP = 32
LANES = 128
TILE = 8
BLOCK = 1024
LAST = NDEV - 1
LAST_START = 55696
SPAN = 3597
COLORS = (0, 1)
REST = 1792
ROWS = 1856
HALF = ROWS // 2
SLICE = 230208
SLICE_ROWS = 1800
MARGIN = 64
BIG_VMEM, PLACE_VMEM = 43 << 20, 8 << 20
COVER = ROWS + 8
TENSOR_ROWS = (32768, 8192, 8192, 8192, 208)
STARTS = (0, 32768, 40960, 49152, 57344, 57552)
PERM_LO, PERM_HI = 32768, 49152
LOADS = (32, 64, 128, 256, 448)
E_SLOTS = 9
AHEAD = 3
FRONT = AHEAD * 32


def bounds(sizes):
    out, at = [], 0
    for n in sizes:
        out.append((at, n))
        at += n
    return out


LOAD = bounds(LOADS)
PIECES = HALF // GROUP
LAGS = ((0, 3, 6, 8, 12, 19, 32, 36, 53), (0, 3, 6, 10, 16, 20, 31, 35, 52))
SEQUENCE = ((8, 0), (6, 0), (8, 1), (7, 0), (2, 0), (3, 1), (1, 0), (0, 0), (5, 1), (5, 0), (4, 1), (6, 1), (4, 0), (2, 1), (1, 1), (0, 1), (3, 0), (7, 1))
STEPS = PIECES + max(map(max, LAGS))
FIRST_ADAM = min(lags[4] for lags in LAGS)
LAST_ADAM = max(lags[4] for lags in LAGS) + PIECES - 1
MOVES = FIRST_ADAM - 6


def start_row(d):
    return LAST_START if d == LAST else 32 * (SPAN * d // 64)


def merge_row(d):
    return 32 * (SPAN * d // 64)


def segments(row, n):
    out = []
    for t in range(5):
        lo, hi = max(row, STARTS[t]), min(row + n, STARTS[t + 1])
        if lo < hi:
            out.append((t, lo - STARTS[t], lo - row, hi - lo))
    return out


def slot_of(color, k):
    x, y, z0, z1 = k % 2, k // 2 % 2, k // 4 % 2, k // 8
    return (x * 8 + z0 * 4 + y * 2 + z1) if color == 0 else (y * 8 + z0 * 4 + x * 2 + z1)


def big_kernel(ge, ga, gf1, gf2, gb, m_in, v_in, w_in, gat, stage, acc_a, acc_b, pair_a, pair_b, last_a, last_b, line_m, line_v, line_w, cov, ld_sem, pr_recv, pr_send, rs_recv, rs_send, ag_recv, ag_send, dag_recv, dag_send, state_sem):
    grads = (ge, ga, gf1, gf2, gb)
    acc, pair, final = (acc_a, acc_b), (pair_a, pair_b), (last_a, last_b)
    z, y, inner = lax.axis_index('outer'), lax.axis_index('middle'), lax.axis_index('inner')
    x, c = inner // 2, inner % 2
    z0, z1 = z % 2, z // 2
    dev = (z * 2 + y) * 4 + inner
    to_pair = {'inner': inner + 1 - 2 * c}
    to_x = {'inner': inner + 2 - 4 * x}
    to_y = {'middle': 1 - y}
    to_z0 = {'outer': z + 1 - 2 * z0}
    to_z1 = {'outer': z + 2 - 4 * z1}
    routes = ((to_x, to_z0, to_y, to_z1), (to_y, to_z0, to_x, to_z1))
    bits = ((x, z0, y, z1), (y, z0, x, z1))

    barrier = pltpu.get_barrier_semaphore()
    for to in (to_pair, to_x, to_y, to_z0, to_z1):
        pl.semaphore_signal(barrier, inc=1, device_id=to, device_id_type=MESH)

    lines = (line_m, line_v, line_w)
    state_in = [pltpu.make_async_copy(src, lines[i], state_sem.at[i]) for i, src in enumerate((m_in, v_in, w_in))]
    for copy in state_in:
        copy.start()
    pl.semaphore_wait(barrier, 5)

    def load_one(color, i, tensor, row, slot, at, n, mine):
        src = grads[tensor].at[pl.ds(row, n)]
        if mine:
            pltpu.make_async_copy(src, acc[color].at[slot, pl.ds(at, n)], ld_sem.at[color, i]).start()
        else:
            pltpu.make_async_remote_copy(src, pair[color].at[slot, pl.ds(FRONT + at, n)], pr_send.at[color], pr_recv.at[color, i], device_id=to_pair, device_id_type=MESH).start()

    def load(i):
        at, n = LOAD[i]
        for color in COLORS:
            @pl.loop(0, E_SLOTS)
            def _(k):
                slot = slot_of(color, k)
                for mine in (False, True):
                    d = 2 * k + (c if mine else 1 - c)
                    row = pl.multiple_of(GROUP * ((SPAN * d) // 64), GROUP) + color * HALF + at
                    load_one(color, i, 0, row, slot, at, n, mine)
            for core in COLORS:
                @pl.when(c == core)
                def _():
                    for k in range(E_SLOTS, NDEV // 2):
                        slot = slot_of(color, k)
                        for mine in (False, True):
                            d = 2 * k + (core if mine else 1 - core)
                            for tensor, row, off, rows in segments(start_row(d) + color * HALF + at, n):
                                load_one(color, i, tensor, row, slot, at + off, rows, mine)

    def wait_on(ref, sem):
        pltpu.make_async_copy(ref, ref, sem).wait()

    def rows_at(p):
        return pl.ds(pl.multiple_of(p * GROUP, GROUP), GROUP)

    def rows_at(p):
        return pl.ds(pl.multiple_of(p * GROUP, GROUP), GROUP)

    def add(color, into, slots, first, p, block):
        acc[color][pl.ds(into, slots), rows_at(p), :] += pair[color][pl.ds(first, slots), rows_at(block), :]

    def landing(color, s, p):
        if s == 3:
            return final[color].at[:, rows_at(p)]
        return pair[color].at[pl.ds(16 - (16 >> s), TILE >> s), rows_at(p)]

    def base(color, level):
        return sum((bits[color][i] * (TILE >> i) for i in range(level)), 0 * c)

    def reduce_send(color, s, p):
        size = TILE >> s
        first = base(color, s) + (1 - bits[color][s]) * size
        pltpu.make_async_remote_copy(acc[color].at[pl.ds(first, size), rows_at(p)], landing(color, s, p), rs_send.at[color, s], rs_recv.at[color, s, p], device_id=routes[color][s], device_id_type=MESH).start()

    def pair_out(color, slot, size, p):
        block = gat.at[color, c, pl.ds(slot, size), rows_at(p)]
        pltpu.make_async_remote_copy(block, block, dag_send.at[color], dag_recv.at[color], device_id=to_pair, device_id_type=MESH).start()

    def adam_block(g, load_state, store_state):
        g = g * (1.0 / NDEV)
        m = BETA1 * load_state(0) + (1.0 - BETA1) * g
        v = BETA2 * load_state(1) + (1.0 - BETA2) * (g * g)
        m_hat = m / (1.0 - BETA1 ** STEP)
        v_hat = v / (1.0 - BETA2 ** STEP)
        w = load_state(2) - RATE * m_hat / (jnp.sqrt(v_hat) + EPS)
        store_state(0, m)
        store_state(1, v)
        store_state(2, w)
        return w

    cover_start = jnp.where(dev == LAST, LAST_START, GROUP * ((SPAN * dev) // 64))

    def adam(color, p):
        slot = base(color, 4)
        r = pl.multiple_of(p * GROUP, GROUP)
        f = pl.multiple_of(color * HALF + r, GROUP)
        row = cover_start + f
        permuted = (row >= PERM_LO) & (row < PERM_HI)

        def group(index):
            for t in range(2):
                parts = []
                for q in (2 * t, 2 * t + 1):
                    where = index(f, q)

                    def keep(i, value, where=where):
                        cov[i, where, :] = value

                    parts.append(adam_block(acc[color][slot, pl.ds(r + TILE * q, TILE), :], lambda i, where=where: cov[i, where, :], keep))
                gat[color, c, slot, pl.ds(r + 16 * t, 16), :] = jnp.concatenate(parts, axis=0).astype(jnp.bfloat16)

        @pl.when(permuted)
        def _():
            group(lambda f, q: pl.ds(f + q, TILE, stride=4))

        @pl.when(jnp.logical_not(permuted))
        def _():
            group(lambda f, q: pl.ds(f + TILE * q, TILE))

    half_rows = jnp.where(dev == LAST, 115, (SPAN * dev) % 64)
    shift = half_rows // 2
    lane = lax.broadcasted_iota(jnp.int32, (GROUP, LANES), 1)

    def moved(first, second):
        return jnp.where(lane < 64, pltpu.roll(first, 64, 1), pltpu.roll(second, 64, 1))

    def state_rows():
        for i, copy in enumerate(state_in):
            copy.wait()
            stage[i, 0:MARGIN, :] = jnp.zeros((MARGIN, LANES), jnp.float32)
            stage[i, MARGIN + SLICE_ROWS - TILE:, :] = jnp.zeros((MARGIN + TILE, LANES), jnp.float32)
            cov[i, ROWS:, :] = jnp.zeros((COVER - ROWS, LANES), jnp.float32)
            for r in range(REST, 1798):
                stage[i, MARGIN + r:MARGIN + r + 1, :] = lines[i][LANES * r:LANES * r + LANES].reshape(1, LANES)
            stage[i, MARGIN + 1798:MARGIN + 1799, 0:64] = lines[i][SLICE - 64:].reshape(1, 64)

    def state_rows_part(t):
        @pl.loop(0, 56)
        def _(k):
            j = t * 56 + k
            for i in range(3):
                stage[i, pl.ds(pl.multiple_of(MARGIN + j * TILE, TILE), TILE), :] = lines[i][pl.ds(pl.multiple_of(j * BLOCK, BLOCK), BLOCK)].reshape(TILE, LANES)

    def state_to_cover(t):
        @pl.loop(0, -(-ROWS // GROUP // MOVES))
        def _(k):
            f = pl.multiple_of(jnp.minimum((t + k * MOVES) * GROUP, ROWS - GROUP), GROUP)
            r = MARGIN + f - shift
            for i in range(3):
                here = stage[i, pl.ds(r, GROUP), :]
                before = stage[i, pl.ds(r - 1, GROUP), :]
                cov[i, pl.ds(f, GROUP), :] = jnp.where(c == 1, moved(before, here), here)

    def cover_to_state(t):
        @pl.loop(0, 15)
        def _(k):
            r = pl.multiple_of((t * 15 + k) * TILE, TILE)
            for i in range(3):
                here = cov[i, pl.ds(r + shift, TILE), :]
                after = cov[i, pl.ds(r + shift + 1, TILE), :]
                both = jnp.where(lane[:TILE] < 64, pltpu.roll(here, 64, 1), pltpu.roll(after, 64, 1))
                stage[i, pl.ds(pl.multiple_of(MARGIN + r, TILE), TILE), :] = jnp.where(c == 1, both, here)

    def state_out():
        for i, dst in enumerate((m_out, v_out, w_out)):
            pltpu.make_async_copy(stage.at[i, pl.ds(MARGIN, SLICE_ROWS)], dst, state_sem.at[i]).start()

    def start_pieces(color, p):
        for i, (first, n) in enumerate(LOAD):
            @pl.when(p == first // GROUP)
            def _():
                wait_on(acc[color].at[:, pl.ds(first, n)], ld_sem.at[color, i])
                wait_on(pair[color].at[:, pl.ds(FRONT + first, n)], pr_recv.at[color, i])
        bit = bits[color][0]
        for slot in ((1 - bit) * TILE, bit * TILE):
            add(color, slot, TILE, slot, p, p + AHEAD)
        reduce_send(color, 0, p)

    def reduce_piece(color, stage_no, p):
        s = stage_no - 1
        wait_on(landing(color, s, p), rs_recv.at[color, s, p])
        first, size, bit = base(color, stage_no), 4 >> s, bits[color][stage_no]
        for half in (1 - bit, bit):
            add(color, first + half * size, size, 16 - (16 >> s) + half * size, p, p)
        reduce_send(color, stage_no, p)

    def adam_piece(color, p):
        wait_on(landing(color, 3, p), rs_recv.at[color, 3, p])
        slot = base(color, 4)
        acc[color][slot, rows_at(p), :] += final[color][0, rows_at(p), :]
        adam(color, p)
        gather_send(color, 0, slot, 1, p)
        pair_out(color, slot, 1, p)

    def gather_send(color, s, first, size, p):
        block = gat.at[color, c, pl.ds(first, size), rows_at(p)]
        pltpu.make_async_remote_copy(block, block, ag_send.at[color, s], ag_recv.at[color, s, p], device_id=routes[color][3 - s], device_id_type=MESH).start()

    def gather_piece(color, s, p):
        level, size = 4 - s, 1 << s
        arrived = base(color, level - 1) + (1 - bits[color][level - 1]) * size
        wait_on(gat.at[color, c, pl.ds(arrived, size), rows_at(p)], ag_recv.at[color, s, p])
        if s < 3:
            gather_send(color, s + 1, base(color, level - 1), 2 * size, p)
        pair_out(color, arrived, size, p)

    load(0)
    load(1)

    @pl.loop(0, STEPS)
    def _(t):
        for i in range(2, len(LOAD)):
            pl.when(t == LOAD[i - 1][0] // GROUP)(functools.partial(load, i))
        for stage_no, color in SEQUENCE:
            p = t - LAGS[color][stage_no]

            @pl.when((p >= 0) & (p < PIECES))
            def _():
                if stage_no == 0:
                    start_pieces(color, p)
                elif stage_no < 4:
                    reduce_piece(color, stage_no, p)
                elif stage_no == 4:
                    adam_piece(color, p)
                else:
                    gather_piece(color, stage_no - 5, p)

        @pl.when(t == 1)
        def _():
            state_rows()

        @pl.when((t >= 2) & (t < 6))
        def _():
            state_rows_part(t - 2)

        @pl.when((t >= 6) & (t < FIRST_ADAM))
        def _():
            state_to_cover(t - 6)

        @pl.when((t > LAST_ADAM) & (t <= LAST_ADAM + 15))
        def _():
            cover_to_state(t - LAST_ADAM - 1)

    for color in COLORS:
        wait_on(gat.at[color, 1 - c], dag_recv.at[color])
        wait_on(gat.at[color, c], dag_send.at[color])
        wait_on(acc[color], pr_send.at[color])
        for s in range(4):
            wait_on(acc[color].at[pl.ds(0, TILE >> s)], rs_send.at[color, s])
            wait_on(gat.at[color, 0, pl.ds(0, 1 << s)], ag_send.at[color, s])


def place_kernel(gat, stage, e_out, a_out, f1_out, f2_out, b_out, m_out, v_out, w_out, chip_out, merged, loose, vec, tail, block, out_sem, edge_sem, state_sem, chip_sem):
    outs = (e_out, a_out, f1_out, f2_out, b_out)
    chip = (lax.axis_index('outer') * 2 + lax.axis_index('middle')) * 2 + lax.axis_index('inner') // 2
    started = [pltpu.make_async_copy(stage.at[i, pl.ds(MARGIN, SLICE_ROWS)], dst, state_sem.at[i]) for i, dst in enumerate((m_out, v_out, w_out))]

    def rows_from(d, at, n):
        color = at // HALF
        return gat.at[color, d % 2, slot_of(color, d // 2), pl.ds(at - color * HALF, n)]

    row = lax.broadcasted_iota(jnp.int32, (GROUP, LANES), 0)
    lane = lax.broadcasted_iota(jnp.int32, (GROUP, LANES), 1)
    tile_order = (row % TILE) * 4 + row // TILE
    count = 0
    for d in range(NDEV):
        first = merge_row(d)
        last = merge_row(d + 1) if d < LAST else STARTS[-1]
        begin = start_row(d)
        for color in COLORS:
            lo = max(first + (GROUP if d else 0), begin + color * HALF)
            for tensor, at, off, n in segments(lo, min(last, begin + (color + 1) * HALF) - lo):
                started.append(pltpu.make_async_copy(rows_from(d, lo + off - begin, n), outs[tensor].at[pl.ds(at, n)], out_sem.at[count]))
                count += 1
    for copy in started:
        copy.start()
    for d in range(1, NDEV):
        first = merge_row(d)
        flat = tile_order if PERM_LO <= first < PERM_HI else row
        keep = 2 * flat + lane // 64 >= SPAN * d - 2 * first
        new, old = (rows_from(e, first - start_row(e), GROUP)[...].astype(jnp.float32) for e in (d, d - 1))
        merged[d] = jnp.where(keep, new, old).astype(jnp.bfloat16)
        (tensor, at, _, _), = segments(first, GROUP)
        copy = pltpu.make_async_copy(merged.at[d], outs[tensor].at[pl.ds(at, GROUP)], edge_sem.at[d])
        copy.start()
        started.append(copy)

    def rows_of(group):
        d = (64 * group + 63) // SPAN
        begin = jnp.where(d == LAST, LAST_START, GROUP * ((SPAN * d) // 64))
        k = d // 2
        x, y, z0, z1 = k % 2, k // 2 % 2, k // 4 % 2, k // TILE
        halves = []
        for h in COLORS:
            at = GROUP * group - begin + 16 * h
            color = at // HALF
            slot = jnp.where(color == 0, x, y) * TILE + z0 * 4 + jnp.where(color == 0, y, x) * 2 + z1
            halves.append(gat[color, d % 2, slot, pl.ds(pl.multiple_of(at - color * HALF, 16), 16), :])
        edge = (d > 0) & ((SPAN * d) // 64 == group)
        return jnp.where(edge, merged[d].astype(jnp.float32), jnp.concatenate(halves, axis=0).astype(jnp.float32))

    def put(at, rows):
        block[0:1, pl.ds(pl.multiple_of(at * LANES, BLOCK), BLOCK)] = rows.reshape(1, BLOCK).astype(jnp.bfloat16)
    @pl.loop(0, 64)
    def _(j):
        rows = rows_of(chip * 64 + j)
        for q in range(4):
            put(GROUP * j + TILE * q, rows[TILE * q:TILE * q + TILE])

    @pl.loop(0, 16)
    def _(layer):
        for t in (1, 2):
            rows = rows_of(STARTS[t] // GROUP + layer * 16 + chip)
            for q in range(4):
                loose[t - 1, pl.ds(q, TILE, stride=4), :] = rows[TILE * q:TILE * q + TILE]
            for q in range(4):
                put(1536 + 512 * t + GROUP * layer + TILE * q, loose[t - 1, TILE * q:TILE * q + TILE, :])
        rows = rows_of(STARTS[3] // GROUP + layer * 16 + chip)
        for q in range(4):
            put(3072 + GROUP * layer + TILE * q, rows[TILE * q:TILE * q + TILE])

    at = STARTS[4] - start_row(LAST)
    vec[0:208, :] = rows_from(LAST, at, 208)[...].astype(jnp.float32)
    vec[208:, :] = jnp.zeros((16, LANES), jnp.float32)
    tail[...] = jnp.zeros_like(tail)
    begin = (104 * chip) % LANES
    line = lax.broadcasted_iota(jnp.int32, (TILE, LANES), 1)
    for layer in range(16):
        source = layer * 13 + (104 * chip) // LANES
        to = layer * 104 // LANES
        off = layer * 104 % LANES
        turn = (off - begin + LANES) % LANES
        one = pltpu.roll(vec[pl.ds(source, TILE), :], turn, 1)
        two = pltpu.roll(vec[pl.ds(source + 1, TILE), :], turn, 1)
        t = (line - off + LANES) % LANES
        got = jnp.where(begin + t < LANES, one, two)
        here = (t < 104) & (line >= off)
        tail[to:to + 1, :] = jnp.where(here, got, tail[pl.ds(to, TILE), :])[0:1]
        if off + 104 > LANES:
            there = (t < 104) & (line < off)
            tail[to + 1:to + 2, :] = jnp.where(there, got, tail[pl.ds(to + 1, TILE), :])[0:1]
    put(3584, tail[0:TILE, :])
    block[0:1, 3592 * LANES:] = tail[TILE:16, :].reshape(1, BLOCK)[:, 0:640].astype(jnp.bfloat16)
    send = pltpu.make_async_copy(block, chip_out, chip_sem)
    send.start()
    for copy in started:
        copy.wait()
    send.wait()


def tile_rows(tensor):
    return tensor.reshape(-1, TILE, 4, LANES).transpose(0, 2, 1, 3).reshape(-1, LANES)


def untile(rows, shape):
    return rows.reshape(-1, 4, TILE, LANES).transpose(0, 2, 1, 3).reshape(shape)


def solution(mesh):
    def local_step(g_embed, g_attn, g_ffn_in, g_ffn_out, g_vec, m_shard, v_shard, w_shard):
        grads = (g_embed[0], tile_rows(g_attn[0]), tile_rows(g_ffn_in[0]), g_ffn_out[0].reshape(-1, LANES), g_vec[0].reshape(-1, LANES))
        any_spec, vmem_spec = pl.BlockSpec(memory_space=pl.ANY), pl.BlockSpec(memory_space=pltpu.VMEM)
        f32, bf16 = jnp.float32, jnp.bfloat16
        flat = jax.ShapeDtypeStruct((SLICE_ROWS, LANES), f32)
        dma = pltpu.SemaphoreType.DMA
        gathered, stage = pl.pallas_call(
            big_kernel,
            out_shape=(pltpu.VMEM((2, 2, 16, HALF, LANES), bf16), pltpu.VMEM((3, SLICE_ROWS + 2 * MARGIN, LANES), f32)),
            in_specs=[any_spec] * 8,
            out_specs=[vmem_spec] * 2,
            scratch_shapes=[pltpu.VMEM((16, HALF, LANES), f32)] * 2 + [pltpu.VMEM((16, HALF + FRONT, LANES), f32)] * 2 + [pltpu.VMEM((1, HALF, LANES), f32)] * 2 + [pltpu.VMEM((SLICE,), f32)] * 3 + [pltpu.VMEM((3, COVER, LANES), f32)]
            + [dma((2, len(LOADS))), dma((2, len(LOADS))), dma((2,)), dma((2, 4, PIECES)), dma((2, 4)), dma((2, 4, PIECES)), dma((2, 4)), dma((2,)), dma((2,)), dma((3,))],
            compiler_params=pltpu.CompilerParams(collective_id=0, has_side_effects=True, vmem_limit_bytes=BIG_VMEM),
            name='reduce_adam_gather',
        )(*grads, m_shard, v_shard, w_shard)
        placed = pl.pallas_call(
            place_kernel,
            out_shape=[jax.ShapeDtypeStruct((n, LANES), bf16) for n in TENSOR_ROWS] + [flat] * 3 + [jax.ShapeDtypeStruct((1, 2 * SLICE), bf16)],
            in_specs=[vmem_spec] * 2,
            out_specs=[any_spec] * 9,
            scratch_shapes=[pltpu.VMEM((NDEV, GROUP, LANES), bf16), pltpu.VMEM((2, GROUP, LANES), f32), pltpu.VMEM((224, LANES), f32), pltpu.VMEM((24, LANES), f32), pltpu.VMEM((1, 2 * SLICE), bf16)]
            + [dma((2 * NDEV + TILE,)), dma((NDEV,)), dma((3,)), dma(())],
            compiler_params=pltpu.CompilerParams(vmem_limit_bytes=PLACE_VMEM),
            name='place',
        )(gathered, stage)
        e, a, f1, f2, b, *state, w_chip = placed
        tensors = (e, untile(a, (16, LANES, 512)), untile(f1, (16, LANES, 512)), f2.reshape(16, 512, LANES), b.reshape(16, 1664))
        return tuple(t.reshape(-1)[:SLICE] for t in state) + tensors + (w_chip,)

    return jax.shard_map(local_step, mesh=mesh, in_specs=(P(MESH_AXES),) * TILE, out_specs=(P(MESH_AXES),) * 3 + (P(),) * 5 + (P(MESH_AXES),), check_vma=False)
```

```python
import functools

import jax
import jax.numpy as jnp
from jax import lax
from jax.experimental import pallas as pl
from jax.experimental.pallas import tpu as pltpu
from jax.sharding import PartitionSpec as P

MESH_AXES = ('outer', 'middle', 'inner')
MESH = pl.DeviceIdType.MESH
BETA1, BETA2, EPS, RATE, STEP = 0.9, 0.98, 1e-9, 0.05, 3

NDEV = 32
GROUP = 32
LANES = 128
TILE = 8
BLOCK = 1024
LAST = NDEV - 1
LAST_START = 55696
SPAN = 3597
COLORS = (0, 1)
REST = 1792
ROWS = 1856
HALF = ROWS // 2
SLICE = 230208
SLICE_ROWS = 1800
MARGIN = 64
BIG_VMEM, PLACE_VMEM = 43 << 20, 8 << 20
COVER = ROWS + 8
TENSOR_ROWS = (32768, 8192, 8192, 8192, 208)
STARTS = (0, 32768, 40960, 49152, 57344, 57552)
VEC_TILES = 13
INVERSE = (9329, 25)
PERM_LO, PERM_HI = 32768, 49152
LOADS = (32, 64, 128, 256, 448)
E_SLOTS = 9
AHEAD = 3
FRONT = AHEAD * 32


def bounds(sizes):
    out, at = [], 0
    for n in sizes:
        out.append((at, n))
        at += n
    return out


LOAD = bounds(LOADS)
PIECES = HALF // GROUP
LAGS = ((0, 3, 6, 8, 12, 19, 32, 36, 53), (0, 3, 6, 10, 16, 20, 31, 35, 52))
SEQUENCE = ((8, 0), (6, 0), (8, 1), (7, 0), (2, 0), (3, 1), (1, 0), (0, 0), (5, 1), (5, 0), (4, 1), (6, 1), (4, 0), (2, 1), (1, 1), (0, 1), (3, 0), (7, 1))
STEPS = PIECES + max(map(max, LAGS))
FIRST_ADAM = min(lags[4] for lags in LAGS)
LAST_ADAM = max(lags[4] for lags in LAGS) + PIECES - 1
MOVES = FIRST_ADAM - 6


def start_row(d):
    return LAST_START if d == LAST else 32 * (SPAN * d // 64)


def merge_row(d):
    return 32 * (SPAN * d // 64)


def segments(row, n):
    out = []
    for t in range(5):
        lo, hi = max(row, STARTS[t]), min(row + n, STARTS[t + 1])
        if lo < hi:
            out.append((t, lo - STARTS[t], lo - row, hi - lo))
    return out


def slot_of(color, k):
    x, y, z0, z1 = k % 2, k // 2 % 2, k // 4 % 2, k // 8
    return (x * 8 + z0 * 4 + y * 2 + z1) if color == 0 else (y * 8 + z0 * 4 + x * 2 + z1)


def big_kernel(ge, ga, gf1, gf2, gb, m_in, v_in, w_in, gat, stage, acc_a, acc_b, pair_a, pair_b, last_a, last_b, line_m, line_v, line_w, cov, ld_sem, pr_recv, pr_send, rs_recv, rs_send, ag_recv, ag_send, dag_recv, dag_send, state_sem):
    grads = (ge, ga, gf1, gf2, gb)
    acc, pair, final = (acc_a, acc_b), (pair_a, pair_b), (last_a, last_b)
    z, y, inner = lax.axis_index('outer'), lax.axis_index('middle'), lax.axis_index('inner')
    x, c = inner // 2, inner % 2
    z0, z1 = z % 2, z // 2
    dev = (z * 2 + y) * 4 + inner
    to_pair = {'inner': inner + 1 - 2 * c}
    to_x = {'inner': inner + 2 - 4 * x}
    to_y = {'middle': 1 - y}
    to_z0 = {'outer': z + 1 - 2 * z0}
    to_z1 = {'outer': z + 2 - 4 * z1}
    routes = ((to_x, to_z0, to_y, to_z1), (to_y, to_z0, to_x, to_z1))
    bits = ((x, z0, y, z1), (y, z0, x, z1))

    barrier = pltpu.get_barrier_semaphore()
    for to in (to_pair, to_x, to_y, to_z0, to_z1):
        pl.semaphore_signal(barrier, inc=1, device_id=to, device_id_type=MESH)

    lines = (line_m, line_v, line_w)
    state_in = [pltpu.make_async_copy(src, lines[i], state_sem.at[i]) for i, src in enumerate((m_in, v_in, w_in))]
    for copy in state_in:
        copy.start()
    pl.semaphore_wait(barrier, 5)

    def load_one(color, i, tensor, row, slot, at, n, mine):
        src = grads[tensor].at[pl.ds(row, n)]
        if mine:
            pltpu.make_async_copy(src, acc[color].at[slot, pl.ds(at, n)], ld_sem.at[color, i]).start()
        else:
            pltpu.make_async_remote_copy(src, pair[color].at[slot, pl.ds(FRONT + at, n)], pr_send.at[color], pr_recv.at[color, i], device_id=to_pair, device_id_type=MESH).start()

    def load(i):
        at, n = LOAD[i]
        for color in COLORS:
            @pl.loop(0, E_SLOTS)
            def _(k):
                slot = slot_of(color, k)
                for mine in (False, True):
                    d = 2 * k + (c if mine else 1 - c)
                    row = pl.multiple_of(GROUP * ((SPAN * d) // 64), GROUP) + color * HALF + at
                    load_one(color, i, 0, row, slot, at, n, mine)
            for core in COLORS:
                @pl.when(c == core)
                def _():
                    for k in range(E_SLOTS, NDEV // 2):
                        slot = slot_of(color, k)
                        for mine in (False, True):
                            d = 2 * k + (core if mine else 1 - core)
                            for tensor, row, off, rows in segments(start_row(d) + color * HALF + at, n):
                                load_one(color, i, tensor, row, slot, at + off, rows, mine)

    def wait_on(ref, sem):
        pltpu.make_async_copy(ref, ref, sem).wait()

    def rows_at(p):
        return pl.ds(pl.multiple_of(p * GROUP, GROUP), GROUP)

    def rows_at(p):
        return pl.ds(pl.multiple_of(p * GROUP, GROUP), GROUP)

    def add(color, into, slots, first, p, block):
        acc[color][pl.ds(into, slots), rows_at(p), :] += pair[color][pl.ds(first, slots), rows_at(block), :]

    def landing(color, s, p):
        if s == 3:
            return final[color].at[:, rows_at(p)]
        return pair[color].at[pl.ds(16 - (16 >> s), TILE >> s), rows_at(p)]

    def base(color, level):
        return sum((bits[color][i] * (TILE >> i) for i in range(level)), 0 * c)

    def reduce_send(color, s, p):
        size = TILE >> s
        first = base(color, s) + (1 - bits[color][s]) * size
        pltpu.make_async_remote_copy(acc[color].at[pl.ds(first, size), rows_at(p)], landing(color, s, p), rs_send.at[color, s], rs_recv.at[color, s, p], device_id=routes[color][s], device_id_type=MESH).start()

    def pair_out(color, slot, size, p):
        block = gat.at[color, c, pl.ds(slot, size), rows_at(p)]
        pltpu.make_async_remote_copy(block, block, dag_send.at[color], dag_recv.at[color], device_id=to_pair, device_id_type=MESH).start()

    def adam_block(g, load_state, store_state):
        g = g * (1.0 / NDEV)
        m = BETA1 * load_state(0) + (1.0 - BETA1) * g
        v = BETA2 * load_state(1) + (1.0 - BETA2) * (g * g)
        m_hat = m / (1.0 - BETA1 ** STEP)
        v_hat = v / (1.0 - BETA2 ** STEP)
        w = load_state(2) - RATE * m_hat / (jnp.sqrt(v_hat) + EPS)
        store_state(0, m)
        store_state(1, v)
        store_state(2, w)
        return w

    cover_start = jnp.where(dev == LAST, LAST_START, GROUP * ((SPAN * dev) // 64))

    def adam(color, p):
        slot = base(color, 4)
        r = pl.multiple_of(p * GROUP, GROUP)
        f = pl.multiple_of(color * HALF + r, GROUP)
        row = cover_start + f
        permuted = (row >= PERM_LO) & (row < PERM_HI)
        vectors = row + GROUP > STARTS[4]

        def tiles(t, index):
            parts = []
            for q in (2 * t, 2 * t + 1):
                where = index(q)

                def keep(i, value, where=where):
                    cov[i, where, :] = value

                parts.append(adam_block(acc[color][slot, pl.ds(r + TILE * q, TILE), :], lambda i, where=where: cov[i, where, :], keep))
            gat[color, c, slot, pl.ds(r + 16 * t, 16), :] = jnp.concatenate(parts, axis=0).astype(jnp.bfloat16)

        def plain(q):
            return pl.ds(f + TILE * q, TILE)

        def vector_tile(q):
            tile = (row + TILE * q - STARTS[4]) // TILE
            return pl.ds(STARTS[4] - LAST_START + tile // VEC_TILES * VEC_TILES * TILE + tile % VEC_TILES, TILE, stride=VEC_TILES)

        @pl.when(permuted)
        def _():
            for t in COLORS:
                tiles(t, lambda q: pl.ds(f + q, TILE, stride=4))

        @pl.when(jnp.logical_not(permuted | vectors))
        def _():
            for t in COLORS:
                tiles(t, plain)

        @pl.when(vectors)
        def _():
            for t in COLORS:
                inside = row + 16 * t >= STARTS[4]
                pl.when(inside)(functools.partial(tiles, t, vector_tile))
                pl.when(jnp.logical_not(inside))(functools.partial(tiles, t, plain))

    half_rows = jnp.where(dev == LAST, 115, (SPAN * dev) % 64)
    shift = half_rows // 2
    lane = lax.broadcasted_iota(jnp.int32, (GROUP, LANES), 1)

    def moved(first, second):
        return jnp.where(lane < 64, pltpu.roll(first, 64, 1), pltpu.roll(second, 64, 1))

    def state_rows():
        for i, copy in enumerate(state_in):
            copy.wait()
            stage[i, 0:MARGIN, :] = jnp.zeros((MARGIN, LANES), jnp.float32)
            stage[i, MARGIN + SLICE_ROWS - TILE:, :] = jnp.zeros((MARGIN + TILE, LANES), jnp.float32)
            cov[i, ROWS:, :] = jnp.zeros((COVER - ROWS, LANES), jnp.float32)
            for r in range(REST, 1798):
                stage[i, MARGIN + r:MARGIN + r + 1, :] = lines[i][LANES * r:LANES * r + LANES].reshape(1, LANES)
            stage[i, MARGIN + 1798:MARGIN + 1799, 0:64] = lines[i][SLICE - 64:].reshape(1, 64)

    def state_rows_part(t):
        @pl.loop(0, 56)
        def _(k):
            j = t * 56 + k
            for i in range(3):
                stage[i, pl.ds(pl.multiple_of(MARGIN + j * TILE, TILE), TILE), :] = lines[i][pl.ds(pl.multiple_of(j * BLOCK, BLOCK), BLOCK)].reshape(TILE, LANES)

    def state_to_cover(t):
        @pl.loop(0, -(-ROWS // GROUP // MOVES))
        def _(k):
            f = pl.multiple_of(jnp.minimum((t + k * MOVES) * GROUP, ROWS - GROUP), GROUP)
            r = MARGIN + f - shift
            for i in range(3):
                here = stage[i, pl.ds(r, GROUP), :]
                before = stage[i, pl.ds(r - 1, GROUP), :]
                cov[i, pl.ds(f, GROUP), :] = jnp.where(c == 1, moved(before, here), here)

    def cover_to_state(t):
        @pl.loop(0, 15)
        def _(k):
            r = pl.multiple_of((t * 15 + k) * TILE, TILE)
            for i in range(3):
                here = cov[i, pl.ds(r + shift, TILE), :]
                after = cov[i, pl.ds(r + shift + 1, TILE), :]
                both = jnp.where(lane[:TILE] < 64, pltpu.roll(here, 64, 1), pltpu.roll(after, 64, 1))
                stage[i, pl.ds(pl.multiple_of(MARGIN + r, TILE), TILE), :] = jnp.where(c == 1, both, here)

    def state_out():
        for i, dst in enumerate((m_out, v_out, w_out)):
            pltpu.make_async_copy(stage.at[i, pl.ds(MARGIN, SLICE_ROWS)], dst, state_sem.at[i]).start()

    def start_pieces(color, p):
        for i, (first, n) in enumerate(LOAD):
            @pl.when(p == first // GROUP)
            def _():
                wait_on(acc[color].at[:, pl.ds(first, n)], ld_sem.at[color, i])
                wait_on(pair[color].at[:, pl.ds(FRONT + first, n)], pr_recv.at[color, i])
        bit = bits[color][0]
        for slot in ((1 - bit) * TILE, bit * TILE):
            add(color, slot, TILE, slot, p, p + AHEAD)
        reduce_send(color, 0, p)

    def reduce_piece(color, stage_no, p):
        s = stage_no - 1
        wait_on(landing(color, s, p), rs_recv.at[color, s, p])
        first, size, bit = base(color, stage_no), 4 >> s, bits[color][stage_no]
        for half in (1 - bit, bit):
            add(color, first + half * size, size, 16 - (16 >> s) + half * size, p, p)
        reduce_send(color, stage_no, p)

    def adam_piece(color, p):
        wait_on(landing(color, 3, p), rs_recv.at[color, 3, p])
        slot = base(color, 4)
        acc[color][slot, rows_at(p), :] += final[color][0, rows_at(p), :]
        adam(color, p)
        gather_send(color, 0, slot, 1, p)
        pair_out(color, slot, 1, p)

    def gather_send(color, s, first, size, p):
        block = gat.at[color, c, pl.ds(first, size), rows_at(p)]
        pltpu.make_async_remote_copy(block, block, ag_send.at[color, s], ag_recv.at[color, s, p], device_id=routes[color][3 - s], device_id_type=MESH).start()

    def gather_piece(color, s, p):
        level, size = 4 - s, 1 << s
        arrived = base(color, level - 1) + (1 - bits[color][level - 1]) * size
        wait_on(gat.at[color, c, pl.ds(arrived, size), rows_at(p)], ag_recv.at[color, s, p])
        if s < 3:
            gather_send(color, s + 1, base(color, level - 1), 2 * size, p)
        pair_out(color, arrived, size, p)

    load(0)
    load(1)

    @pl.loop(0, STEPS)
    def _(t):
        for i in range(2, len(LOAD)):
            pl.when(t == LOAD[i - 1][0] // GROUP)(functools.partial(load, i))
        for stage_no, color in SEQUENCE:
            p = t - LAGS[color][stage_no]

            @pl.when((p >= 0) & (p < PIECES))
            def _():
                if stage_no == 0:
                    start_pieces(color, p)
                elif stage_no < 4:
                    reduce_piece(color, stage_no, p)
                elif stage_no == 4:
                    adam_piece(color, p)
                else:
                    gather_piece(color, stage_no - 5, p)

        @pl.when(t == 1)
        def _():
            state_rows()

        @pl.when((t >= 2) & (t < 6))
        def _():
            state_rows_part(t - 2)

        @pl.when((t >= 6) & (t < FIRST_ADAM))
        def _():
            state_to_cover(t - 6)

        @pl.when((t > LAST_ADAM) & (t <= LAST_ADAM + 15))
        def _():
            cover_to_state(t - LAST_ADAM - 1)

    for color in COLORS:
        wait_on(gat.at[color, 1 - c], dag_recv.at[color])
        wait_on(gat.at[color, c], dag_send.at[color])
        wait_on(acc[color], pr_send.at[color])
        for s in range(4):
            wait_on(acc[color].at[pl.ds(0, TILE >> s)], rs_send.at[color, s])
            wait_on(gat.at[color, 0, pl.ds(0, 1 << s)], ag_send.at[color, s])


def place_kernel(gat, stage, e_out, a_out, f1_out, f2_out, b_out, m_out, v_out, w_out, chip_out, merged, loose, vec, tail, block, out_sem, edge_sem, state_sem, chip_sem):
    outs = (e_out, a_out, f1_out, f2_out, b_out)
    chip = (lax.axis_index('outer') * 2 + lax.axis_index('middle')) * 2 + lax.axis_index('inner') // 2
    started = [pltpu.make_async_copy(stage.at[i, pl.ds(MARGIN, SLICE_ROWS)], dst, state_sem.at[i]) for i, dst in enumerate((m_out, v_out, w_out))]

    def rows_from(d, at, n):
        color = at // HALF
        return gat.at[color, d % 2, slot_of(color, d // 2), pl.ds(at - color * HALF, n)]

    row = lax.broadcasted_iota(jnp.int32, (GROUP, LANES), 0)
    lane = lax.broadcasted_iota(jnp.int32, (GROUP, LANES), 1)
    tile_order = (row % TILE) * 4 + row // TILE
    count = 0
    for d in range(NDEV):
        first = merge_row(d)
        last = merge_row(d + 1) if d < LAST else STARTS[-1]
        begin = start_row(d)
        for color in COLORS:
            lo = max(first + (GROUP if d else 0), begin + color * HALF)
            for tensor, at, off, n in segments(lo, min(last, begin + (color + 1) * HALF) - lo):
                started.append(pltpu.make_async_copy(rows_from(d, lo + off - begin, n), outs[tensor].at[pl.ds(at, n)], out_sem.at[count]))
                count += 1
    for copy in started:
        copy.start()
    for d in range(1, NDEV):
        first = merge_row(d)
        flat = tile_order if PERM_LO <= first < PERM_HI else row
        keep = 2 * flat + lane // 64 >= SPAN * d - 2 * first
        new, old = (rows_from(e, first - start_row(e), GROUP)[...].astype(jnp.float32) for e in (d, d - 1))
        merged[d] = jnp.where(keep, new, old).astype(jnp.bfloat16)
        (tensor, at, _, _), = segments(first, GROUP)
        copy = pltpu.make_async_copy(merged.at[d], outs[tensor].at[pl.ds(at, GROUP)], edge_sem.at[d])
        copy.start()
        started.append(copy)

    def rows_of(group):
        d = (64 * group + 63) * INVERSE[0] >> INVERSE[1]
        begin = jnp.where(d == LAST, LAST_START, (SPAN * d >> 6) * GROUP)
        x, y, z0, z1 = ((d >> i) & 1 for i in range(1, 5))
        halves = []
        for h in COLORS:
            at = GROUP * group - begin + 16 * h
            color = (at >= HALF).astype(jnp.int32)
            slot = jnp.where(color == 0, x, y) * TILE + z0 * 4 + jnp.where(color == 0, y, x) * 2 + z1
            halves.append(gat[color, d & 1, slot, pl.ds(pl.multiple_of(at - color * HALF, 16), 16), :])
        return halves

    def put(at, rows):
        block[0:1, pl.ds(pl.multiple_of(at * LANES, BLOCK), BLOCK)] = rows.reshape(1, BLOCK).astype(jnp.bfloat16)
    def put_rows(at, halves):
        for h, half in enumerate(halves):
            rows = half.astype(jnp.float32)
            for q in COLORS:
                put(at + 16 * h + TILE * q, rows[TILE * q:TILE * q + TILE])

    def put_tiles(at, halves, t):
        for h, half in enumerate(halves):
            rows = half.astype(jnp.float32)
            for q in COLORS:
                loose[t, pl.ds(2 * h + q, TILE, stride=4), :] = rows[TILE * q:TILE * q + TILE]
        for q in range(4):
            put(at + TILE * q, loose[t, TILE * q:TILE * q + TILE, :])

    @pl.loop(0, 64)
    def _(j):
        put_rows(GROUP * j, rows_of(chip * 64 + j))

    @pl.loop(0, 16)
    def _(layer):
        for t in (1, 2):
            put_tiles(1536 + 512 * t + GROUP * layer, rows_of(STARTS[t] // GROUP + layer * 16 + chip), t - 1)
        put_rows(3072 + GROUP * layer, rows_of(STARTS[3] // GROUP + layer * 16 + chip))

    for d in range(1, NDEV):
        (tensor, at, _, _), = segments(merge_row(d), GROUP)
        layer, owner = divmod(at // GROUP, 16)

        @pl.when(chip == (owner if tensor else at // 2048))
        def _():
            halves = (merged[d, 0:16, :], merged[d, 16:, :])
            if tensor in (1, 2):
                put_tiles(1536 + 512 * tensor + GROUP * layer, halves, tensor - 1)
            else:
                put_rows(3072 + GROUP * layer if tensor else at % 2048, halves)

    at = STARTS[4] - start_row(LAST)
    vec[0:208, :] = rows_from(LAST, at, 208)[...].astype(jnp.float32)
    vec[208:, :] = jnp.zeros((16, LANES), jnp.float32)
    tail[...] = jnp.zeros_like(tail)
    begin = (104 * chip) % LANES
    line = lax.broadcasted_iota(jnp.int32, (TILE, LANES), 1)
    for layer in range(16):
        source = layer // TILE * TILE * VEC_TILES + layer % TILE + (104 * chip) // LANES * TILE
        to = layer * 104 // LANES
        off = layer * 104 % LANES
        turn = (off - begin + LANES) % LANES
        one = pltpu.roll(vec[pl.ds(source, TILE), :], turn, 1)
        two = pltpu.roll(vec[pl.ds(source + TILE, TILE), :], turn, 1)
        t = (line - off + LANES) % LANES
        got = jnp.where(begin + t < LANES, one, two)
        here = (t < 104) & (line >= off)
        tail[to:to + 1, :] = jnp.where(here, got, tail[pl.ds(to, TILE), :])[0:1]
        if off + 104 > LANES:
            there = (t < 104) & (line < off)
            tail[to + 1:to + 2, :] = jnp.where(there, got, tail[pl.ds(to + 1, TILE), :])[0:1]
    put(3584, tail[0:TILE, :])
    block[0:1, 3592 * LANES:] = tail[TILE:16, :].reshape(1, BLOCK)[:, 0:640].astype(jnp.bfloat16)
    send = pltpu.make_async_copy(block, chip_out, chip_sem)
    send.start()
    for copy in started:
        copy.wait()
    send.wait()


def tile_rows(tensor, tiles=4):
    return tensor.reshape(-1, TILE, tiles, LANES).transpose(0, 2, 1, 3).reshape(-1, LANES)


def untile(rows, shape, tiles=4):
    return rows.reshape(-1, tiles, TILE, LANES).transpose(0, 2, 1, 3).reshape(shape)


def solution(mesh):
    def local_step(g_embed, g_attn, g_ffn_in, g_ffn_out, g_vec, m_shard, v_shard, w_shard):
        grads = (g_embed[0], tile_rows(g_attn[0]), tile_rows(g_ffn_in[0]), g_ffn_out[0].reshape(-1, LANES), tile_rows(g_vec[0], VEC_TILES))
        any_spec, vmem_spec = pl.BlockSpec(memory_space=pl.ANY), pl.BlockSpec(memory_space=pltpu.VMEM)
        f32, bf16 = jnp.float32, jnp.bfloat16
        flat = jax.ShapeDtypeStruct((SLICE_ROWS, LANES), f32)
        dma = pltpu.SemaphoreType.DMA
        gathered, stage = pl.pallas_call(
            big_kernel,
            out_shape=(pltpu.VMEM((2, 2, 16, HALF, LANES), bf16), pltpu.VMEM((3, SLICE_ROWS + 2 * MARGIN, LANES), f32)),
            in_specs=[any_spec] * 8,
            out_specs=[vmem_spec] * 2,
            scratch_shapes=[pltpu.VMEM((16, HALF, LANES), f32)] * 2 + [pltpu.VMEM((16, HALF + FRONT, LANES), f32)] * 2 + [pltpu.VMEM((1, HALF, LANES), f32)] * 2 + [pltpu.VMEM((SLICE,), f32)] * 3 + [pltpu.VMEM((3, COVER, LANES), f32)]
            + [dma((2, len(LOADS))), dma((2, len(LOADS))), dma((2,)), dma((2, 4, PIECES)), dma((2, 4)), dma((2, 4, PIECES)), dma((2, 4)), dma((2,)), dma((2,)), dma((3,))],
            compiler_params=pltpu.CompilerParams(collective_id=0, has_side_effects=True, vmem_limit_bytes=BIG_VMEM),
            name='reduce_adam_gather',
        )(*grads, m_shard, v_shard, w_shard)
        placed = pl.pallas_call(
            place_kernel,
            out_shape=[jax.ShapeDtypeStruct((n, LANES), bf16) for n in TENSOR_ROWS] + [flat] * 3 + [jax.ShapeDtypeStruct((1, 2 * SLICE), bf16)],
            in_specs=[vmem_spec] * 2,
            out_specs=[any_spec] * 9,
            scratch_shapes=[pltpu.VMEM((NDEV, GROUP, LANES), bf16), pltpu.VMEM((2, GROUP, LANES), f32), pltpu.VMEM((224, LANES), f32), pltpu.VMEM((24, LANES), f32), pltpu.VMEM((1, 2 * SLICE), bf16)]
            + [dma((2 * NDEV + TILE,)), dma((NDEV,)), dma((3,)), dma(())],
            compiler_params=pltpu.CompilerParams(vmem_limit_bytes=PLACE_VMEM),
            name='place',
        )(gathered, stage)
        e, a, f1, f2, b, *state, w_chip = placed
        tensors = (e, untile(a, (16, LANES, 512)), untile(f1, (16, LANES, 512)), f2.reshape(16, 512, LANES), untile(b, (16, 1664), VEC_TILES))
        return tuple(t.reshape(-1)[:SLICE] for t in state) + tensors + (w_chip,)

    return jax.shard_map(local_step, mesh=mesh, in_specs=(P(MESH_AXES),) * TILE, out_specs=(P(MESH_AXES),) * 3 + (P(),) * 5 + (P(MESH_AXES),), check_vma=False)
```

```python
import functools

import jax
import jax.numpy as jnp
from jax import lax
from jax.experimental import pallas as pl
from jax.experimental.pallas import tpu as pltpu
from jax.sharding import PartitionSpec as P

MESH_AXES = ('outer', 'middle', 'inner')
MESH = pl.DeviceIdType.MESH
BETA1, BETA2, EPS, RATE, STEP = 0.9, 0.98, 1e-9, 0.05, 3

NDEV = 32
GROUP = 32
LANES = 128
TILE = 8
BLOCK = 1024
LAST = NDEV - 1
LAST_START = 55696
SPAN = 3597
COLORS = (0, 1)
REST = 1792
ROWS = 1856
HALF = ROWS // 2
SLICE = 230208
SLICE_ROWS = 1800
MARGIN = 64
BIG_VMEM, PLACE_VMEM = 43 << 20, 8 << 20
COVER = ROWS + 8
TENSOR_ROWS = (32768, 8192, 8192, 8192, 208)
STARTS = (0, 32768, 40960, 49152, 57344, 57552)
VEC_TILES = 13
INVERSE = (9329, 25)
PERM_LO, PERM_HI = 32768, 49152
LOADS = (32, 64, 128, 256, 288, 160)
E_SLOTS = 9
LATE = 24
AHEAD = 4
FRONT = AHEAD * 32


def bounds(sizes):
    out, at = [], 0
    for n in sizes:
        out.append((at, n))
        at += n
    return out


LOAD = bounds(LOADS)
PIECES = HALF // GROUP
LAGS = ((0, 3, 6, 9, 14, 20, 25, 29, 41), (0, 3, 6, 10, 16, 20, 24, 30, 45))
SEQUENCE = ((0, 0), (8, 1), (4, 1), (5, 0), (3, 1), (6, 0), (7, 1), (1, 0), (2, 1), (3, 0), (8, 0), (7, 0), (4, 0), (1, 1), (5, 1), (2, 0), (0, 1), (6, 1))
STEPS = PIECES + max(map(max, LAGS))
FIRST_ADAM = min(lags[4] for lags in LAGS)
LAST_ADAM = max(lags[4] for lags in LAGS) + PIECES - 1
MOVES = FIRST_ADAM - 6


def start_row(d):
    return LAST_START if d == LAST else 32 * (SPAN * d // 64)


def merge_row(d):
    return 32 * (SPAN * d // 64)


def segments(row, n):
    out = []
    for t in range(5):
        lo, hi = max(row, STARTS[t]), min(row + n, STARTS[t + 1])
        if lo < hi:
            out.append((t, lo - STARTS[t], lo - row, hi - lo))
    return out


def slot_of(color, k, late=False):
    x, y, z0, z1 = k % 2, k // 2 % 2, k // 4 % 2, k // 8
    first, third = (x, y) if color == 0 else (y, x)
    return first * 8 + (third * 4 + z0 * 2 if late else z0 * 4 + third * 2) + z1


def big_kernel(ge, ga, gf1, gf2, gb, m_in, v_in, w_in, gat, stage, acc_a, acc_b, pair_a, pair_b, last_a, last_b, line_m, line_v, line_w, cov, ld_sem, pr_recv, pr_send, rs_recv, rs_send, ag_recv, ag_send, dag_recv, dag_send, state_sem):
    grads = (ge, ga, gf1, gf2, gb)
    acc, pair, final = (acc_a, acc_b), (pair_a, pair_b), (last_a, last_b)
    z, y, inner = lax.axis_index('outer'), lax.axis_index('middle'), lax.axis_index('inner')
    x, c = inner // 2, inner % 2
    z0, z1 = z % 2, z // 2
    dev = (z * 2 + y) * 4 + inner
    to_pair = {'inner': inner + 1 - 2 * c}
    to_x = {'inner': inner + 2 - 4 * x}
    to_y = {'middle': 1 - y}
    to_z0 = {'outer': z + 1 - 2 * z0}
    to_z1 = {'outer': z + 2 - 4 * z1}
    routes = ((to_x, to_z0, to_y, to_z1), (to_y, to_z0, to_x, to_z1))
    bits = ((x, z0, y, z1), (y, z0, x, z1))

    barrier = pltpu.get_barrier_semaphore()
    for to in (to_pair, to_x, to_y, to_z0, to_z1):
        pl.semaphore_signal(barrier, inc=1, device_id=to, device_id_type=MESH)

    lines = (line_m, line_v, line_w)
    state_in = [pltpu.make_async_copy(src, lines[i], state_sem.at[i]) for i, src in enumerate((m_in, v_in, w_in))]
    for copy in state_in:
        copy.start()
    pl.semaphore_wait(barrier, 5)

    def load_one(color, i, tensor, row, slot, at, n, mine):
        src = grads[tensor].at[pl.ds(row, n)]
        if mine:
            pltpu.make_async_copy(src, acc[color].at[slot, pl.ds(at, n)], ld_sem.at[color, i]).start()
        else:
            pltpu.make_async_remote_copy(src, pair[color].at[slot, pl.ds(FRONT + at, n)], pr_send.at[color], pr_recv.at[color, i], device_id=to_pair, device_id_type=MESH).start()

    def load(i):
        at, n = LOAD[i]
        for color in COLORS:
            @pl.loop(0, E_SLOTS)
            def _(k):
                slot = slot_of(color, k, at >= LATE * GROUP)
                for mine in (False, True):
                    d = 2 * k + (c if mine else 1 - c)
                    row = pl.multiple_of(GROUP * ((SPAN * d) // 64), GROUP) + color * HALF + at
                    load_one(color, i, 0, row, slot, at, n, mine)
            for core in COLORS:
                @pl.when(c == core)
                def _():
                    for k in range(E_SLOTS, NDEV // 2):
                        slot = slot_of(color, k, at >= LATE * GROUP)
                        for mine in (False, True):
                            d = 2 * k + (core if mine else 1 - core)
                            for tensor, row, off, rows in segments(start_row(d) + color * HALF + at, n):
                                load_one(color, i, tensor, row, slot, at + off, rows, mine)

    def wait_on(ref, sem):
        pltpu.make_async_copy(ref, ref, sem).wait()

    def rows_at(p):
        return pl.ds(pl.multiple_of(p * GROUP, GROUP), GROUP)

    def rows_at(p):
        return pl.ds(pl.multiple_of(p * GROUP, GROUP), GROUP)

    def add(color, into, slots, first, p, block):
        acc[color][pl.ds(into, slots), rows_at(p), :] += pair[color][pl.ds(first, slots), rows_at(block), :]

    def landing(color, s, p):
        if s == 3:
            return final[color].at[:, rows_at(p)]
        return pair[color].at[pl.ds(16 - (16 >> s), TILE >> s), rows_at(p)]

    def base(color, level):
        return sum((bits[color][i] * (TILE >> i) for i in range(level)), 0 * c)

    def halved(color, level, p):
        one, other = bits[color][level], bits[color][3 - level if level in (1, 2) else level]
        return jnp.where(p >= LATE, other, one)

    def reduce_base(color, level, p):
        return sum((halved(color, i, p) * (TILE >> i) for i in range(level)), 0 * c)

    def reduce_to(color, s, p):
        if s in (0, 3):
            return routes[color][s]
        along_z = p < LATE if s == 1 else p >= LATE
        across_y = jnp.logical_not(along_z) & (color == 0)
        across_x = jnp.logical_not(along_z) & (color == 1)
        return {'outer': jnp.where(along_z, to_z0['outer'], z), 'middle': jnp.where(across_y, 1 - y, y), 'inner': jnp.where(across_x, to_x['inner'], inner)}

    def reduce_send(color, s, p):
        size = TILE >> s
        first = reduce_base(color, s, p) + (1 - halved(color, s, p)) * size
        pltpu.make_async_remote_copy(acc[color].at[pl.ds(first, size), rows_at(p)], landing(color, s, p), rs_send.at[color, s], rs_recv.at[color, s, p], device_id=reduce_to(color, s, p), device_id_type=MESH).start()

    def pair_out(color, slot, size, p):
        block = gat.at[color, c, pl.ds(slot, size), rows_at(p)]
        pltpu.make_async_remote_copy(block, block, dag_send.at[color], dag_recv.at[color], device_id=to_pair, device_id_type=MESH).start()

    def adam_block(g, load_state, store_state):
        g = g * (1.0 / NDEV)
        m = BETA1 * load_state(0) + (1.0 - BETA1) * g
        v = BETA2 * load_state(1) + (1.0 - BETA2) * (g * g)
        m_hat = m / (1.0 - BETA1 ** STEP)
        v_hat = v / (1.0 - BETA2 ** STEP)
        w = load_state(2) - RATE * m_hat / (jnp.sqrt(v_hat) + EPS)
        store_state(0, m)
        store_state(1, v)
        store_state(2, w)
        return w

    cover_start = jnp.where(dev == LAST, LAST_START, GROUP * ((SPAN * dev) // 64))

    def adam(color, p):
        slot, summed = base(color, 4), reduce_base(color, 4, p)
        r = pl.multiple_of(p * GROUP, GROUP)
        f = pl.multiple_of(color * HALF + r, GROUP)
        row = cover_start + f
        permuted = (row >= PERM_LO) & (row < PERM_HI)
        vectors = row + GROUP > STARTS[4]

        def tiles(t, index):
            parts = []
            for q in (2 * t, 2 * t + 1):
                where = index(q)

                def keep(i, value, where=where):
                    cov[i, where, :] = value

                parts.append(adam_block(acc[color][summed, pl.ds(r + TILE * q, TILE), :], lambda i, where=where: cov[i, where, :], keep))
            gat[color, c, slot, pl.ds(r + 16 * t, 16), :] = jnp.concatenate(parts, axis=0).astype(jnp.bfloat16)

        def plain(q):
            return pl.ds(f + TILE * q, TILE)

        def vector_tile(q):
            tile = (row + TILE * q - STARTS[4]) // TILE
            return pl.ds(STARTS[4] - LAST_START + tile // VEC_TILES * VEC_TILES * TILE + tile % VEC_TILES, TILE, stride=VEC_TILES)

        @pl.when(permuted)
        def _():
            for t in COLORS:
                tiles(t, lambda q: pl.ds(f + q, TILE, stride=4))

        @pl.when(jnp.logical_not(permuted | vectors))
        def _():
            for t in COLORS:
                tiles(t, plain)

        @pl.when(vectors)
        def _():
            for t in COLORS:
                inside = row + 16 * t >= STARTS[4]
                pl.when(inside)(functools.partial(tiles, t, vector_tile))
                pl.when(jnp.logical_not(inside))(functools.partial(tiles, t, plain))

    half_rows = jnp.where(dev == LAST, 115, (SPAN * dev) % 64)
    shift = half_rows // 2
    lane = lax.broadcasted_iota(jnp.int32, (GROUP, LANES), 1)

    def moved(first, second):
        return jnp.where(lane < 64, pltpu.roll(first, 64, 1), pltpu.roll(second, 64, 1))

    def state_rows():
        for i, copy in enumerate(state_in):
            copy.wait()
            stage[i, 0:MARGIN, :] = jnp.zeros((MARGIN, LANES), jnp.float32)
            stage[i, MARGIN + SLICE_ROWS - TILE:, :] = jnp.zeros((MARGIN + TILE, LANES), jnp.float32)
            cov[i, ROWS:, :] = jnp.zeros((COVER - ROWS, LANES), jnp.float32)
            for r in range(REST, 1798):
                stage[i, MARGIN + r:MARGIN + r + 1, :] = lines[i][LANES * r:LANES * r + LANES].reshape(1, LANES)
            stage[i, MARGIN + 1798:MARGIN + 1799, 0:64] = lines[i][SLICE - 64:].reshape(1, 64)

    def state_rows_part(t):
        @pl.loop(0, 56)
        def _(k):
            j = t * 56 + k
            for i in range(3):
                stage[i, pl.ds(pl.multiple_of(MARGIN + j * TILE, TILE), TILE), :] = lines[i][pl.ds(pl.multiple_of(j * BLOCK, BLOCK), BLOCK)].reshape(TILE, LANES)

    def state_to_cover(t):
        @pl.loop(0, -(-ROWS // GROUP // MOVES))
        def _(k):
            f = pl.multiple_of(jnp.minimum((t + k * MOVES) * GROUP, ROWS - GROUP), GROUP)
            r = MARGIN + f - shift
            for i in range(3):
                here = stage[i, pl.ds(r, GROUP), :]
                before = stage[i, pl.ds(r - 1, GROUP), :]
                cov[i, pl.ds(f, GROUP), :] = jnp.where(c == 1, moved(before, here), here)

    def cover_to_state(t):
        @pl.loop(0, 15)
        def _(k):
            r = pl.multiple_of((t * 15 + k) * TILE, TILE)
            for i in range(3):
                here = cov[i, pl.ds(r + shift, TILE), :]
                after = cov[i, pl.ds(r + shift + 1, TILE), :]
                both = jnp.where(lane[:TILE] < 64, pltpu.roll(here, 64, 1), pltpu.roll(after, 64, 1))
                stage[i, pl.ds(pl.multiple_of(MARGIN + r, TILE), TILE), :] = jnp.where(c == 1, both, here)

    def state_out():
        for i, dst in enumerate((m_out, v_out, w_out)):
            pltpu.make_async_copy(stage.at[i, pl.ds(MARGIN, SLICE_ROWS)], dst, state_sem.at[i]).start()

    def start_pieces(color, p):
        for i, (first, n) in enumerate(LOAD):
            @pl.when(p == first // GROUP)
            def _():
                wait_on(acc[color].at[:, pl.ds(first, n)], ld_sem.at[color, i])
                wait_on(pair[color].at[:, pl.ds(FRONT + first, n)], pr_recv.at[color, i])
        bit = bits[color][0]
        for slot in ((1 - bit) * TILE, bit * TILE):
            add(color, slot, TILE, slot, p, p + AHEAD)
        reduce_send(color, 0, p)

    def reduce_piece(color, stage_no, p):
        s = stage_no - 1
        wait_on(landing(color, s, p), rs_recv.at[color, s, p])
        first, size, bit = reduce_base(color, stage_no, p), 4 >> s, halved(color, stage_no, p)
        for half in (1 - bit, bit):
            add(color, first + half * size, size, 16 - (16 >> s) + half * size, p, p)
        reduce_send(color, stage_no, p)

    def adam_piece(color, p):
        wait_on(landing(color, 3, p), rs_recv.at[color, 3, p])
        slot = base(color, 4)
        acc[color][reduce_base(color, 4, p), rows_at(p), :] += final[color][0, rows_at(p), :]
        adam(color, p)
        gather_send(color, 0, slot, 1, p)
        pair_out(color, slot, 1, p)

    def gather_send(color, s, first, size, p):
        block = gat.at[color, c, pl.ds(first, size), rows_at(p)]
        pltpu.make_async_remote_copy(block, block, ag_send.at[color, s], ag_recv.at[color, s, p], device_id=routes[color][3 - s], device_id_type=MESH).start()

    def gather_piece(color, s, p):
        level, size = 4 - s, 1 << s
        arrived = base(color, level - 1) + (1 - bits[color][level - 1]) * size
        wait_on(gat.at[color, c, pl.ds(arrived, size), rows_at(p)], ag_recv.at[color, s, p])
        if s < 3:
            gather_send(color, s + 1, base(color, level - 1), 2 * size, p)
        pair_out(color, arrived, size, p)

    load(0)

    @pl.loop(0, STEPS)
    def _(t):
        for i in range(2, len(LOAD)):
            pl.when(t == LOAD[i - 1][0] // GROUP)(functools.partial(load, i))
        for stage_no, color in SEQUENCE:
            p = t - LAGS[color][stage_no]

            @pl.when((p >= 0) & (p < PIECES))
            def _():
                if stage_no == 0:
                    start_pieces(color, p)
                elif stage_no < 4:
                    reduce_piece(color, stage_no, p)
                elif stage_no == 4:
                    adam_piece(color, p)
                else:
                    gather_piece(color, stage_no - 5, p)

        pl.when(t == 0)(functools.partial(load, 1))

        @pl.when(t == 1)
        def _():
            state_rows()

        @pl.when((t >= 2) & (t < 6))
        def _():
            state_rows_part(t - 2)

        @pl.when((t >= 6) & (t < FIRST_ADAM))
        def _():
            state_to_cover(t - 6)

        @pl.when((t > LAST_ADAM) & (t <= LAST_ADAM + 15))
        def _():
            cover_to_state(t - LAST_ADAM - 1)

    for color in COLORS:
        wait_on(gat.at[color, 1 - c], dag_recv.at[color])
        wait_on(gat.at[color, c], dag_send.at[color])
        wait_on(acc[color], pr_send.at[color])
        for s in range(4):
            wait_on(acc[color].at[pl.ds(0, TILE >> s)], rs_send.at[color, s])
            wait_on(gat.at[color, 0, pl.ds(0, 1 << s)], ag_send.at[color, s])


def place_kernel(gat, stage, e_out, a_out, f1_out, f2_out, b_out, m_out, v_out, w_out, chip_out, merged, loose, vec, tail, block, out_sem, edge_sem, state_sem, chip_sem):
    outs = (e_out, a_out, f1_out, f2_out, b_out)
    chip = (lax.axis_index('outer') * 2 + lax.axis_index('middle')) * 2 + lax.axis_index('inner') // 2
    started = [pltpu.make_async_copy(stage.at[i, pl.ds(MARGIN, SLICE_ROWS)], dst, state_sem.at[i]) for i, dst in enumerate((m_out, v_out, w_out))]

    def rows_from(d, at, n):
        color = at // HALF
        return gat.at[color, d % 2, slot_of(color, d // 2), pl.ds(at - color * HALF, n)]

    row = lax.broadcasted_iota(jnp.int32, (GROUP, LANES), 0)
    lane = lax.broadcasted_iota(jnp.int32, (GROUP, LANES), 1)
    tile_order = (row % TILE) * 4 + row // TILE
    count = 0
    for d in range(NDEV):
        first = merge_row(d)
        last = merge_row(d + 1) if d < LAST else STARTS[-1]
        begin = start_row(d)
        for color in COLORS:
            lo = max(first + (GROUP if d else 0), begin + color * HALF)
            for tensor, at, off, n in segments(lo, min(last, begin + (color + 1) * HALF) - lo):
                started.append(pltpu.make_async_copy(rows_from(d, lo + off - begin, n), outs[tensor].at[pl.ds(at, n)], out_sem.at[count]))
                count += 1
    for copy in started:
        copy.start()
    for d in range(1, NDEV):
        first = merge_row(d)
        flat = tile_order if PERM_LO <= first < PERM_HI else row
        keep = 2 * flat + lane // 64 >= SPAN * d - 2 * first
        new, old = (rows_from(e, first - start_row(e), GROUP)[...].astype(jnp.float32) for e in (d, d - 1))
        merged[d] = jnp.where(keep, new, old).astype(jnp.bfloat16)
        (tensor, at, _, _), = segments(first, GROUP)
        copy = pltpu.make_async_copy(merged.at[d], outs[tensor].at[pl.ds(at, GROUP)], edge_sem.at[d])
        copy.start()
        started.append(copy)

    def rows_of(group):
        d = (64 * group + 63) * INVERSE[0] >> INVERSE[1]
        begin = jnp.where(d == LAST, LAST_START, (SPAN * d >> 6) * GROUP)
        x, y, z0, z1 = ((d >> i) & 1 for i in range(1, 5))
        halves = []
        for h in COLORS:
            at = GROUP * group - begin + 16 * h
            color = (at >= HALF).astype(jnp.int32)
            slot = jnp.where(color == 0, x, y) * TILE + z0 * 4 + jnp.where(color == 0, y, x) * 2 + z1
            halves.append(gat[color, d & 1, slot, pl.ds(pl.multiple_of(at - color * HALF, 16), 16), :])
        return halves

    def put(at, rows):
        block[0:1, pl.ds(pl.multiple_of(at * LANES, BLOCK), BLOCK)] = rows.reshape(1, BLOCK).astype(jnp.bfloat16)
    def put_rows(at, halves):
        for h, half in enumerate(halves):
            rows = half.astype(jnp.float32)
            for q in COLORS:
                put(at + 16 * h + TILE * q, rows[TILE * q:TILE * q + TILE])

    def put_tiles(at, halves, t):
        for h, half in enumerate(halves):
            rows = half.astype(jnp.float32)
            for q in COLORS:
                loose[t, pl.ds(2 * h + q, TILE, stride=4), :] = rows[TILE * q:TILE * q + TILE]
        for q in range(4):
            put(at + TILE * q, loose[t, TILE * q:TILE * q + TILE, :])

    @pl.loop(0, 64)
    def _(j):
        put_rows(GROUP * j, rows_of(chip * 64 + j))

    @pl.loop(0, 16)
    def _(layer):
        for t in (1, 2):
            put_tiles(1536 + 512 * t + GROUP * layer, rows_of(STARTS[t] // GROUP + layer * 16 + chip), t - 1)
        put_rows(3072 + GROUP * layer, rows_of(STARTS[3] // GROUP + layer * 16 + chip))

    for d in range(1, NDEV):
        (tensor, at, _, _), = segments(merge_row(d), GROUP)
        layer, owner = divmod(at // GROUP, 16)

        @pl.when(chip == (owner if tensor else at // 2048))
        def _():
            halves = (merged[d, 0:16, :], merged[d, 16:, :])
            if tensor in (1, 2):
                put_tiles(1536 + 512 * tensor + GROUP * layer, halves, tensor - 1)
            else:
                put_rows(3072 + GROUP * layer if tensor else at % 2048, halves)

    at = STARTS[4] - start_row(LAST)
    vec[0:208, :] = rows_from(LAST, at, 208)[...].astype(jnp.float32)
    vec[208:, :] = jnp.zeros((16, LANES), jnp.float32)
    tail[...] = jnp.zeros_like(tail)
    begin = (104 * chip) % LANES
    line = lax.broadcasted_iota(jnp.int32, (TILE, LANES), 1)
    for layer in range(16):
        source = layer // TILE * TILE * VEC_TILES + layer % TILE + (104 * chip) // LANES * TILE
        to = layer * 104 // LANES
        off = layer * 104 % LANES
        turn = (off - begin + LANES) % LANES
        one = pltpu.roll(vec[pl.ds(source, TILE), :], turn, 1)
        two = pltpu.roll(vec[pl.ds(source + TILE, TILE), :], turn, 1)
        t = (line - off + LANES) % LANES
        got = jnp.where(begin + t < LANES, one, two)
        here = (t < 104) & (line >= off)
        tail[to:to + 1, :] = jnp.where(here, got, tail[pl.ds(to, TILE), :])[0:1]
        if off + 104 > LANES:
            there = (t < 104) & (line < off)
            tail[to + 1:to + 2, :] = jnp.where(there, got, tail[pl.ds(to + 1, TILE), :])[0:1]
    put(3584, tail[0:TILE, :])
    block[0:1, 3592 * LANES:] = tail[TILE:16, :].reshape(1, BLOCK)[:, 0:640].astype(jnp.bfloat16)
    send = pltpu.make_async_copy(block, chip_out, chip_sem)
    send.start()
    for copy in started:
        copy.wait()
    send.wait()


def tile_rows(tensor, tiles=4):
    return tensor.reshape(-1, TILE, tiles, LANES).transpose(0, 2, 1, 3).reshape(-1, LANES)


def untile(rows, shape, tiles=4):
    return rows.reshape(-1, tiles, TILE, LANES).transpose(0, 2, 1, 3).reshape(shape)


def solution(mesh):
    def local_step(g_embed, g_attn, g_ffn_in, g_ffn_out, g_vec, m_shard, v_shard, w_shard):
        grads = (g_embed[0], tile_rows(g_attn[0]), tile_rows(g_ffn_in[0]), g_ffn_out[0].reshape(-1, LANES), tile_rows(g_vec[0], VEC_TILES))
        any_spec, vmem_spec = pl.BlockSpec(memory_space=pl.ANY), pl.BlockSpec(memory_space=pltpu.VMEM)
        f32, bf16 = jnp.float32, jnp.bfloat16
        flat = jax.ShapeDtypeStruct((SLICE_ROWS, LANES), f32)
        dma = pltpu.SemaphoreType.DMA
        gathered, stage = pl.pallas_call(
            big_kernel,
            out_shape=(pltpu.VMEM((2, 2, 16, HALF, LANES), bf16), pltpu.VMEM((3, SLICE_ROWS + 2 * MARGIN, LANES), f32)),
            in_specs=[any_spec] * 8,
            out_specs=[vmem_spec] * 2,
            scratch_shapes=[pltpu.VMEM((16, HALF, LANES), f32)] * 2 + [pltpu.VMEM((16, HALF + FRONT, LANES), f32)] * 2 + [pltpu.VMEM((1, HALF, LANES), f32)] * 2 + [pltpu.VMEM((SLICE,), f32)] * 3 + [pltpu.VMEM((3, COVER, LANES), f32)]
            + [dma((2, len(LOADS))), dma((2, len(LOADS))), dma((2,)), dma((2, 4, PIECES)), dma((2, 4)), dma((2, 4, PIECES)), dma((2, 4)), dma((2,)), dma((2,)), dma((3,))],
            compiler_params=pltpu.CompilerParams(collective_id=0, has_side_effects=True, vmem_limit_bytes=BIG_VMEM),
            name='reduce_adam_gather',
        )(*grads, m_shard, v_shard, w_shard)
        placed = pl.pallas_call(
            place_kernel,
            out_shape=[jax.ShapeDtypeStruct((n, LANES), bf16) for n in TENSOR_ROWS] + [flat] * 3 + [jax.ShapeDtypeStruct((1, 2 * SLICE), bf16)],
            in_specs=[vmem_spec] * 2,
            out_specs=[any_spec] * 9,
            scratch_shapes=[pltpu.VMEM((NDEV, GROUP, LANES), bf16), pltpu.VMEM((2, GROUP, LANES), f32), pltpu.VMEM((224, LANES), f32), pltpu.VMEM((24, LANES), f32), pltpu.VMEM((1, 2 * SLICE), bf16)]
            + [dma((2 * NDEV + TILE,)), dma((NDEV,)), dma((3,)), dma(())],
            compiler_params=pltpu.CompilerParams(vmem_limit_bytes=PLACE_VMEM),
            name='place',
        )(gathered, stage)
        e, a, f1, f2, b, *state, w_chip = placed
        tensors = (e, untile(a, (16, LANES, 512)), untile(f1, (16, LANES, 512)), f2.reshape(16, 512, LANES), untile(b, (16, 1664), VEC_TILES))
        return tuple(t.reshape(-1)[:SLICE] for t in state) + tensors + (w_chip,)

    return jax.shard_map(local_step, mesh=mesh, in_specs=(P(MESH_AXES),) * TILE, out_specs=(P(MESH_AXES),) * 3 + (P(),) * 5 + (P(MESH_AXES),), check_vma=False)
```

```python
import functools

import jax
import jax.numpy as jnp
from jax import lax
from jax.experimental import pallas as pl
from jax.experimental.pallas import tpu as pltpu
from jax.sharding import PartitionSpec as P

MESH_AXES = ('outer', 'middle', 'inner')
MESH = pl.DeviceIdType.MESH
BETA1, BETA2, EPS, RATE, STEP = 0.9, 0.98, 1e-9, 0.05, 3

NDEV = 32
GROUP = 32
LANES = 128
TILE = 8
BLOCK = 1024
LAST = NDEV - 1
LAST_START = 55696
SPAN = 3597
COLORS = (0, 1)
REST = 1792
ROWS = 1856
HALF = ROWS // 2
SLICE = 230208
SLICE_ROWS = 1800
MARGIN = 64
BIG_VMEM, PLACE_VMEM = 43 << 20, 8 << 20
COVER = ROWS + 8
TENSOR_ROWS = (32768, 8192, 8192, 8192, 208)
STARTS = (0, 32768, 40960, 49152, 57344, 57552)
VEC_TILES = 13
INVERSE = (9329, 25)
PERM_LO, PERM_HI = 32768, 49152
LOADS = (32, 64, 128, 256, 288, 160)
E_SLOTS = 9
E_ROWS = 2048
LATE = 24
AHEAD = 4
FRONT = AHEAD * 32


def bounds(sizes):
    out, at = [], 0
    for n in sizes:
        out.append((at, n))
        at += n
    return out


LOAD = bounds(LOADS)
PIECES = HALF // GROUP
LAGS = ((0, 3, 6, 9, 14, 20, 25, 29, 41), (0, 3, 6, 10, 16, 20, 24, 30, 45))
SEQUENCE = ((0, 0), (8, 1), (4, 1), (5, 0), (3, 1), (6, 0), (7, 1), (1, 0), (2, 1), (3, 0), (8, 0), (7, 0), (4, 0), (1, 1), (5, 1), (2, 0), (0, 1), (6, 1))
STEPS = PIECES + max(map(max, LAGS))
FIRST_ADAM = min(lags[4] for lags in LAGS)
LAST_ADAM = max(lags[4] for lags in LAGS) + PIECES - 1
MOVES = FIRST_ADAM - 6


def start_row(d):
    return LAST_START if d == LAST else 32 * (SPAN * d // 64)


def merge_row(d):
    return 32 * (SPAN * d // 64)


def segments(row, n):
    out = []
    for t in range(5):
        lo, hi = max(row, STARTS[t]), min(row + n, STARTS[t + 1])
        if lo < hi:
            out.append((t, lo - STARTS[t], lo - row, hi - lo))
    return out


def slot_of(color, k, late=False):
    x, y, z0, z1 = k % 2, k // 2 % 2, k // 4 % 2, k // 8
    first, third = (x, y) if color == 0 else (y, x)
    return first * 8 + (third * 4 + z0 * 2 if late else z0 * 4 + third * 2) + z1


def big_kernel(ge, ga, gf1, gf2, gb, m_in, v_in, w_in, gat, stage, acc_a, acc_b, pair_a, pair_b, last_a, last_b, line_m, line_v, line_w, cov, ld_sem, pr_recv, pr_send, rs_recv, rs_send, ag_recv, ag_send, dag_recv, dag_send, state_sem):
    grads = (ge, ga, gf1, gf2, gb)
    acc, pair, final = (acc_a, acc_b), (pair_a, pair_b), (last_a, last_b)
    z, y, inner = lax.axis_index('outer'), lax.axis_index('middle'), lax.axis_index('inner')
    x, c = inner // 2, inner % 2
    z0, z1 = z % 2, z // 2
    dev = (z * 2 + y) * 4 + inner
    to_pair = {'inner': inner + 1 - 2 * c}
    to_x = {'inner': inner + 2 - 4 * x}
    to_y = {'middle': 1 - y}
    to_z0 = {'outer': z + 1 - 2 * z0}
    to_z1 = {'outer': z + 2 - 4 * z1}
    routes = ((to_x, to_z0, to_y, to_z1), (to_y, to_z0, to_x, to_z1))
    bits = ((x, z0, y, z1), (y, z0, x, z1))

    barrier = pltpu.get_barrier_semaphore()
    for to in (to_pair, to_x, to_y, to_z0, to_z1):
        pl.semaphore_signal(barrier, inc=1, device_id=to, device_id_type=MESH)

    def load_one(color, i, tensor, row, slot, at, n, mine):
        src = grads[tensor].at[pl.ds(row, n)]
        if mine:
            pltpu.make_async_copy(src, acc[color].at[slot, pl.ds(at, n)], ld_sem.at[color, i]).start()
        else:
            pltpu.make_async_remote_copy(src, pair[color].at[slot, pl.ds(FRONT + at, n)], pr_send.at[color], pr_recv.at[color, i], device_id=to_pair, device_id_type=MESH).start()

    def load(i, sides=(True, False)):
        at, n = LOAD[i]
        for color in COLORS:
            @pl.loop(0, E_SLOTS)
            def _(k):
                slot = slot_of(color, k, at >= LATE * GROUP)
                for mine in sides:
                    d = 2 * k + (c if mine else 1 - c)
                    row = pl.multiple_of(GROUP * ((SPAN * d) // 64), GROUP) + color * HALF + at
                    load_one(color, i, 0, row, slot, at, n, mine)
            for core in COLORS:
                @pl.when(c == core)
                def _():
                    for k in range(E_SLOTS, NDEV // 2):
                        slot = slot_of(color, k, at >= LATE * GROUP)
                        for mine in sides:
                            d = 2 * k + (core if mine else 1 - core)
                            for tensor, row, off, rows in segments(start_row(d) + color * HALF + at, n):
                                load_one(color, i, tensor, row, slot, at + off, rows, mine)

    load(0, (True,))
    lines = (line_m, line_v, line_w)
    state_in = [pltpu.make_async_copy(src, lines[i], state_sem.at[i]) for i, src in enumerate((m_in, v_in, w_in))]
    for copy in state_in:
        copy.start()
    pl.semaphore_wait(barrier, 5)

    def wait_on(ref, sem):
        pltpu.make_async_copy(ref, ref, sem).wait()

    def rows_at(p):
        return pl.ds(pl.multiple_of(p * GROUP, GROUP), GROUP)

    def rows_at(p):
        return pl.ds(pl.multiple_of(p * GROUP, GROUP), GROUP)

    def add(color, into, slots, first, p, block):
        acc[color][pl.ds(into, slots), rows_at(p), :] += pair[color][pl.ds(first, slots), rows_at(block), :]

    def landing(color, s, p):
        if s == 3:
            return final[color].at[:, rows_at(p)]
        return pair[color].at[pl.ds(16 - (16 >> s), TILE >> s), rows_at(p)]

    def base(color, level):
        return sum((bits[color][i] * (TILE >> i) for i in range(level)), 0 * c)

    def halved(color, level, p):
        one, other = bits[color][level], bits[color][3 - level if level in (1, 2) else level]
        return jnp.where(p >= LATE, other, one)

    def reduce_base(color, level, p):
        return sum((halved(color, i, p) * (TILE >> i) for i in range(level)), 0 * c)

    def reduce_to(color, s, p):
        if s in (0, 3):
            return routes[color][s]
        along_z = p < LATE if s == 1 else p >= LATE
        across_y = jnp.logical_not(along_z) & (color == 0)
        across_x = jnp.logical_not(along_z) & (color == 1)
        return {'outer': jnp.where(along_z, to_z0['outer'], z), 'middle': jnp.where(across_y, 1 - y, y), 'inner': jnp.where(across_x, to_x['inner'], inner)}

    def reduce_send(color, s, p):
        size = TILE >> s
        first = reduce_base(color, s, p) + (1 - halved(color, s, p)) * size
        pltpu.make_async_remote_copy(acc[color].at[pl.ds(first, size), rows_at(p)], landing(color, s, p), rs_send.at[color, s], rs_recv.at[color, s, p], device_id=reduce_to(color, s, p), device_id_type=MESH).start()

    def pair_out(color, slot, size, p):
        block = gat.at[color, c, pl.ds(slot, size), rows_at(p)]
        pltpu.make_async_remote_copy(block, block, dag_send.at[color], dag_recv.at[color], device_id=to_pair, device_id_type=MESH).start()

    def adam_block(g, load_state, store_state):
        g = g * (1.0 / NDEV)
        m = BETA1 * load_state(0) + (1.0 - BETA1) * g
        v = BETA2 * load_state(1) + (1.0 - BETA2) * (g * g)
        m_hat = m / (1.0 - BETA1 ** STEP)
        v_hat = v / (1.0 - BETA2 ** STEP)
        w = load_state(2) - RATE * m_hat / (jnp.sqrt(v_hat) + EPS)
        store_state(0, m)
        store_state(1, v)
        store_state(2, w)
        return w

    cover_start = jnp.where(dev == LAST, LAST_START, GROUP * ((SPAN * dev) // 64))

    def adam(color, p):
        slot, summed = base(color, 4), reduce_base(color, 4, p)
        r = pl.multiple_of(p * GROUP, GROUP)
        f = pl.multiple_of(color * HALF + r, GROUP)
        row = cover_start + f
        permuted = (row >= PERM_LO) & (row < PERM_HI)
        vectors = row + GROUP > STARTS[4]

        def tiles(t, index):
            parts = []
            for q in (2 * t, 2 * t + 1):
                where = index(q)

                def keep(i, value, where=where):
                    cov[i, where, :] = value

                parts.append(adam_block(acc[color][summed, pl.ds(r + TILE * q, TILE), :], lambda i, where=where: cov[i, where, :], keep))
            gat[color, c, slot, pl.ds(r + 16 * t, 16), :] = jnp.concatenate(parts, axis=0).astype(jnp.bfloat16)

        def plain(q):
            return pl.ds(f + TILE * q, TILE)

        def vector_tile(q):
            tile = (row + TILE * q - STARTS[4]) // TILE
            return pl.ds(STARTS[4] - LAST_START + tile // VEC_TILES * VEC_TILES * TILE + tile % VEC_TILES, TILE, stride=VEC_TILES)

        @pl.when(permuted)
        def _():
            for t in COLORS:
                tiles(t, lambda q: pl.ds(f + q, TILE, stride=4))

        @pl.when(jnp.logical_not(permuted | vectors))
        def _():
            for t in COLORS:
                tiles(t, plain)

        @pl.when(vectors)
        def _():
            for t in COLORS:
                inside = row + 16 * t >= STARTS[4]
                pl.when(inside)(functools.partial(tiles, t, vector_tile))
                pl.when(jnp.logical_not(inside))(functools.partial(tiles, t, plain))

    half_rows = jnp.where(dev == LAST, 115, (SPAN * dev) % 64)
    shift = half_rows // 2
    lane = lax.broadcasted_iota(jnp.int32, (GROUP, LANES), 1)

    def moved(first, second):
        return jnp.where(lane < 64, pltpu.roll(first, 64, 1), pltpu.roll(second, 64, 1))

    def state_rows():
        for i, copy in enumerate(state_in):
            copy.wait()
            stage[i, 0:MARGIN, :] = jnp.zeros((MARGIN, LANES), jnp.float32)
            stage[i, MARGIN + SLICE_ROWS - TILE:, :] = jnp.zeros((MARGIN + TILE, LANES), jnp.float32)
            cov[i, ROWS:, :] = jnp.zeros((COVER - ROWS, LANES), jnp.float32)
            for r in range(REST, 1798):
                stage[i, MARGIN + r:MARGIN + r + 1, :] = lines[i][LANES * r:LANES * r + LANES].reshape(1, LANES)
            stage[i, MARGIN + 1798:MARGIN + 1799, 0:64] = lines[i][SLICE - 64:].reshape(1, 64)

    def state_rows_part(t):
        @pl.loop(0, 56)
        def _(k):
            j = t * 56 + k
            for i in range(3):
                stage[i, pl.ds(pl.multiple_of(MARGIN + j * TILE, TILE), TILE), :] = lines[i][pl.ds(pl.multiple_of(j * BLOCK, BLOCK), BLOCK)].reshape(TILE, LANES)

    def state_to_cover(t):
        @pl.loop(0, -(-ROWS // GROUP // MOVES))
        def _(k):
            f = pl.multiple_of(jnp.minimum((t + k * MOVES) * GROUP, ROWS - GROUP), GROUP)
            r = MARGIN + f - shift
            for i in range(3):
                here = stage[i, pl.ds(r, GROUP), :]
                before = stage[i, pl.ds(r - 1, GROUP), :]
                cov[i, pl.ds(f, GROUP), :] = jnp.where(c == 1, moved(before, here), here)

    def cover_to_state(t):
        @pl.loop(0, 15)
        def _(k):
            r = pl.multiple_of((t * 15 + k) * TILE, TILE)
            for i in range(3):
                here = cov[i, pl.ds(r + shift, TILE), :]
                after = cov[i, pl.ds(r + shift + 1, TILE), :]
                both = jnp.where(lane[:TILE] < 64, pltpu.roll(here, 64, 1), pltpu.roll(after, 64, 1))
                stage[i, pl.ds(pl.multiple_of(MARGIN + r, TILE), TILE), :] = jnp.where(c == 1, both, here)

    def state_out():
        for i, dst in enumerate((m_out, v_out, w_out)):
            pltpu.make_async_copy(stage.at[i, pl.ds(MARGIN, SLICE_ROWS)], dst, state_sem.at[i]).start()

    def start_pieces(color, p):
        for i, (first, n) in enumerate(LOAD):
            @pl.when(p == first // GROUP)
            def _():
                wait_on(acc[color].at[:, pl.ds(first, n)], ld_sem.at[color, i])
                wait_on(pair[color].at[:, pl.ds(FRONT + first, n)], pr_recv.at[color, i])
        bit = bits[color][0]
        for slot in ((1 - bit) * TILE, bit * TILE):
            add(color, slot, TILE, slot, p, p + AHEAD)
        reduce_send(color, 0, p)

    def reduce_piece(color, stage_no, p):
        s = stage_no - 1
        wait_on(landing(color, s, p), rs_recv.at[color, s, p])
        first, size, bit = reduce_base(color, stage_no, p), 4 >> s, halved(color, stage_no, p)
        for half in (1 - bit, bit):
            add(color, first + half * size, size, 16 - (16 >> s) + half * size, p, p)
        reduce_send(color, stage_no, p)

    def adam_piece(color, p):
        wait_on(landing(color, 3, p), rs_recv.at[color, 3, p])
        slot = base(color, 4)
        acc[color][reduce_base(color, 4, p), rows_at(p), :] += final[color][0, rows_at(p), :]
        adam(color, p)
        gather_send(color, 0, slot, 1, p)
        pair_out(color, slot, 1, p)

    def gather_send(color, s, first, size, p):
        block = gat.at[color, c, pl.ds(first, size), rows_at(p)]
        pltpu.make_async_remote_copy(block, block, ag_send.at[color, s], ag_recv.at[color, s, p], device_id=routes[color][3 - s], device_id_type=MESH).start()

    def gather_piece(color, s, p):
        level, size = 4 - s, 1 << s
        arrived = base(color, level - 1) + (1 - bits[color][level - 1]) * size
        wait_on(gat.at[color, c, pl.ds(arrived, size), rows_at(p)], ag_recv.at[color, s, p])
        if s < 3:
            gather_send(color, s + 1, base(color, level - 1), 2 * size, p)
        pair_out(color, arrived, size, p)

    load(0, (False,))

    @pl.loop(0, STEPS)
    def _(t):
        for i in range(2, len(LOAD)):
            pl.when(t == LOAD[i - 1][0] // GROUP)(functools.partial(load, i))
        for stage_no, color in SEQUENCE:
            p = t - LAGS[color][stage_no]

            @pl.when((p >= 0) & (p < PIECES))
            def _():
                if stage_no == 0:
                    start_pieces(color, p)
                elif stage_no < 4:
                    reduce_piece(color, stage_no, p)
                elif stage_no == 4:
                    adam_piece(color, p)
                else:
                    gather_piece(color, stage_no - 5, p)

        pl.when(t == 0)(functools.partial(load, 1))

        @pl.when(t == 1)
        def _():
            state_rows()

        @pl.when((t >= 2) & (t < 6))
        def _():
            state_rows_part(t - 2)

        @pl.when((t >= 6) & (t < FIRST_ADAM))
        def _():
            state_to_cover(t - 6)

        @pl.when((t > LAST_ADAM) & (t <= LAST_ADAM + 15))
        def _():
            cover_to_state(t - LAST_ADAM - 1)

    for color in COLORS:
        wait_on(gat.at[color, 1 - c], dag_recv.at[color])
        wait_on(gat.at[color, c], dag_send.at[color])
        wait_on(acc[color], pr_send.at[color])
        for s in range(4):
            wait_on(acc[color].at[pl.ds(0, TILE >> s)], rs_send.at[color, s])
            wait_on(gat.at[color, 0, pl.ds(0, 1 << s)], ag_send.at[color, s])


def place_kernel(gat, stage, e_out, a_out, f1_out, f2_out, b_out, m_out, v_out, w_out, chip_out, merged, loose, vec, tail, block, out_sem, edge_sem, state_sem, chip_sem):
    outs = (e_out, a_out, f1_out, f2_out, b_out)
    chip = (lax.axis_index('outer') * 2 + lax.axis_index('middle')) * 2 + lax.axis_index('inner') // 2
    started = [pltpu.make_async_copy(stage.at[i, pl.ds(MARGIN, SLICE_ROWS)], dst, state_sem.at[i]) for i, dst in enumerate((m_out, v_out, w_out))]

    def rows_from(d, at, n):
        color = at // HALF
        return gat.at[color, d % 2, slot_of(color, d // 2), pl.ds(at - color * HALF, n)]

    row = lax.broadcasted_iota(jnp.int32, (GROUP, LANES), 0)
    lane = lax.broadcasted_iota(jnp.int32, (GROUP, LANES), 1)
    tile_order = (row % TILE) * 4 + row // TILE
    count = 0
    for d in range(NDEV):
        first = merge_row(d)
        last = merge_row(d + 1) if d < LAST else STARTS[-1]
        begin = start_row(d)
        for color in COLORS:
            lo = max(first + (GROUP if d else 0), begin + color * HALF)
            for tensor, at, off, n in segments(lo, min(last, begin + (color + 1) * HALF) - lo):
                started.append(pltpu.make_async_copy(rows_from(d, lo + off - begin, n), outs[tensor].at[pl.ds(at, n)], out_sem.at[count]))
                count += 1
    for copy in started:
        copy.start()
    for d in range(1, NDEV):
        first = merge_row(d)
        flat = tile_order if PERM_LO <= first < PERM_HI else row
        keep = 2 * flat + lane // 64 >= SPAN * d - 2 * first
        new, old = (rows_from(e, first - start_row(e), GROUP)[...].astype(jnp.float32) for e in (d, d - 1))
        merged[d] = jnp.where(keep, new, old).astype(jnp.bfloat16)
        (tensor, at, _, _), = segments(first, GROUP)
        copy = pltpu.make_async_copy(merged.at[d], outs[tensor].at[pl.ds(at, GROUP)], edge_sem.at[d])
        copy.start()
        started.append(copy)

    def rows_of(group):
        d = (64 * group + 63) * INVERSE[0] >> INVERSE[1]
        begin = jnp.where(d == LAST, LAST_START, (SPAN * d >> 6) * GROUP)
        x, y, z0, z1 = ((d >> i) & 1 for i in range(1, 5))
        halves = []
        for h in COLORS:
            at = GROUP * group - begin + 16 * h
            color = (at >= HALF).astype(jnp.int32)
            slot = jnp.where(color == 0, x, y) * TILE + z0 * 4 + jnp.where(color == 0, y, x) * 2 + z1
            halves.append(gat[color, d & 1, slot, pl.ds(pl.multiple_of(at - color * HALF, 16), 16), :])
        return halves

    def put(at, rows):
        block[0:1, pl.ds(pl.multiple_of(at * LANES, BLOCK), BLOCK)] = rows.reshape(1, BLOCK).astype(jnp.bfloat16)
    def put_rows(at, halves):
        for h, half in enumerate(halves):
            rows = half.astype(jnp.float32)
            for q in COLORS:
                put(at + 16 * h + TILE * q, rows[TILE * q:TILE * q + TILE])

    def put_tiles(at, halves, t):
        for h, half in enumerate(halves):
            rows = half.astype(jnp.float32)
            for q in COLORS:
                loose[t, pl.ds(2 * h + q, TILE, stride=4), :] = rows[TILE * q:TILE * q + TILE]
        for q in range(4):
            put(at + TILE * q, loose[t, TILE * q:TILE * q + TILE, :])

    def put_edges(tensors):
        for d in range(1, NDEV):
            (tensor, at, _, _), = segments(merge_row(d), GROUP)
            if tensor not in tensors:
                continue
            layer, owner = divmod(at // GROUP, 16)

            @pl.when(chip == (owner if tensor else at // E_ROWS))
            def _():
                halves = (merged[d, 0:16, :], merged[d, 16:, :])
                if tensor in (1, 2):
                    put_tiles(1536 + 512 * tensor + GROUP * layer, halves, tensor - 1)
                else:
                    put_rows(3072 + GROUP * layer if tensor else at % E_ROWS, halves)

    @pl.loop(0, 64, unroll=4)
    def _(j):
        put_rows(GROUP * j, rows_of(chip * 64 + j))

    put_edges((0,))
    split = E_ROWS * LANES
    sends = [pltpu.make_async_copy(block.at[:, pl.ds(at, n)], chip_out.at[:, pl.ds(at, n)], chip_sem.at[i]) for i, (at, n) in enumerate(((0, split), (split, 2 * SLICE - split)))]
    sends[0].start()

    @pl.loop(0, 16, unroll=2)
    def _(layer):
        for t in (1, 2):
            put_tiles(1536 + 512 * t + GROUP * layer, rows_of(STARTS[t] // GROUP + layer * 16 + chip), t - 1)
        put_rows(3072 + GROUP * layer, rows_of(STARTS[3] // GROUP + layer * 16 + chip))

    put_edges((1, 2, 3))
    at = STARTS[4] - start_row(LAST)
    vec[0:208, :] = rows_from(LAST, at, 208)[...].astype(jnp.float32)
    vec[208:, :] = jnp.zeros((16, LANES), jnp.float32)
    tail[...] = jnp.zeros_like(tail)
    begin = (104 * chip) % LANES
    line = lax.broadcasted_iota(jnp.int32, (TILE, LANES), 1)
    for layer in range(16):
        source = layer // TILE * TILE * VEC_TILES + layer % TILE + (104 * chip) // LANES * TILE
        to = layer * 104 // LANES
        off = layer * 104 % LANES
        turn = (off - begin + LANES) % LANES
        one = pltpu.roll(vec[pl.ds(source, TILE), :], turn, 1)
        two = pltpu.roll(vec[pl.ds(source + TILE, TILE), :], turn, 1)
        t = (line - off + LANES) % LANES
        got = jnp.where(begin + t < LANES, one, two)
        here = (t < 104) & (line >= off)
        tail[to:to + 1, :] = jnp.where(here, got, tail[pl.ds(to, TILE), :])[0:1]
        if off + 104 > LANES:
            there = (t < 104) & (line < off)
            tail[to + 1:to + 2, :] = jnp.where(there, got, tail[pl.ds(to + 1, TILE), :])[0:1]
    put(3584, tail[0:TILE, :])
    block[0:1, 3592 * LANES:] = tail[TILE:16, :].reshape(1, BLOCK)[:, 0:640].astype(jnp.bfloat16)
    sends[1].start()
    for copy in started + sends:
        copy.wait()


def tile_rows(tensor, tiles=4):
    return tensor.reshape(-1, TILE, tiles, LANES).transpose(0, 2, 1, 3).reshape(-1, LANES)


def untile(rows, shape, tiles=4):
    return rows.reshape(-1, tiles, TILE, LANES).transpose(0, 2, 1, 3).reshape(shape)


def solution(mesh):
    def local_step(g_embed, g_attn, g_ffn_in, g_ffn_out, g_vec, m_shard, v_shard, w_shard):
        grads = (g_embed[0], tile_rows(g_attn[0]), tile_rows(g_ffn_in[0]), g_ffn_out[0].reshape(-1, LANES), tile_rows(g_vec[0], VEC_TILES))
        any_spec, vmem_spec = pl.BlockSpec(memory_space=pl.ANY), pl.BlockSpec(memory_space=pltpu.VMEM)
        f32, bf16 = jnp.float32, jnp.bfloat16
        flat = jax.ShapeDtypeStruct((SLICE_ROWS, LANES), f32)
        dma = pltpu.SemaphoreType.DMA
        gathered, stage = pl.pallas_call(
            big_kernel,
            out_shape=(pltpu.VMEM((2, 2, 16, HALF, LANES), bf16), pltpu.VMEM((3, SLICE_ROWS + 2 * MARGIN, LANES), f32)),
            in_specs=[any_spec] * 8,
            out_specs=[vmem_spec] * 2,
            scratch_shapes=[pltpu.VMEM((16, HALF, LANES), f32)] * 2 + [pltpu.VMEM((16, HALF + FRONT, LANES), f32)] * 2 + [pltpu.VMEM((1, HALF, LANES), f32)] * 2 + [pltpu.VMEM((SLICE,), f32)] * 3 + [pltpu.VMEM((3, COVER, LANES), f32)]
            + [dma((2, len(LOADS))), dma((2, len(LOADS))), dma((2,)), dma((2, 4, PIECES)), dma((2, 4)), dma((2, 4, PIECES)), dma((2, 4)), dma((2,)), dma((2,)), dma((3,))],
            compiler_params=pltpu.CompilerParams(collective_id=0, has_side_effects=True, vmem_limit_bytes=BIG_VMEM),
            name='reduce_adam_gather',
        )(*grads, m_shard, v_shard, w_shard)
        placed = pl.pallas_call(
            place_kernel,
            out_shape=[jax.ShapeDtypeStruct((n, LANES), bf16) for n in TENSOR_ROWS] + [flat] * 3 + [jax.ShapeDtypeStruct((1, 2 * SLICE), bf16)],
            in_specs=[vmem_spec] * 2,
            out_specs=[any_spec] * 9,
            scratch_shapes=[pltpu.VMEM((NDEV, GROUP, LANES), bf16), pltpu.VMEM((2, GROUP, LANES), f32), pltpu.VMEM((224, LANES), f32), pltpu.VMEM((24, LANES), f32), pltpu.VMEM((1, 2 * SLICE), bf16)]
            + [dma((2 * NDEV + TILE,)), dma((NDEV,)), dma((3,)), dma((2,))],
            compiler_params=pltpu.CompilerParams(vmem_limit_bytes=PLACE_VMEM),
            name='place',
        )(gathered, stage)
        e, a, f1, f2, b, *state, w_chip = placed
        tensors = (e, untile(a, (16, LANES, 512)), untile(f1, (16, LANES, 512)), f2.reshape(16, 512, LANES), untile(b, (16, 1664), VEC_TILES))
        return tuple(t.reshape(-1)[:SLICE] for t in state) + tensors + (w_chip,)

    return jax.shard_map(local_step, mesh=mesh, in_specs=(P(MESH_AXES),) * TILE, out_specs=(P(MESH_AXES),) * 3 + (P(),) * 5 + (P(MESH_AXES),), check_vma=False)
```

```python
import functools

import jax
import jax.numpy as jnp
from jax import lax
from jax.experimental import pallas as pl
from jax.experimental.pallas import tpu as pltpu
from jax.sharding import PartitionSpec as P

MESH_AXES = ('outer', 'middle', 'inner')
MESH = pl.DeviceIdType.MESH
BETA1, BETA2, EPS, RATE, STEP = 0.9, 0.98, 1e-9, 0.05, 3

NDEV = 32
GROUP = 32
LANES = 128
TILE = 8
BLOCK = 1024
LAST = NDEV - 1
LAST_START = 55696
SPAN = 3597
COLORS = (0, 1)
REST = 1792
ROWS = 1856
HALF = ROWS // 2
SLICE = 230208
SLICE_ROWS = 1800
MARGIN = 64
BIG_VMEM, PLACE_VMEM = 43 << 20, 8 << 20
COVER = ROWS + 8
TENSOR_ROWS = (32768, 8192, 8192, 8192, 208)
STARTS = (0, 32768, 40960, 49152, 57344, 57552)
VEC_TILES = 13
INVERSE = (9329, 25)
PERM_LO, PERM_HI = 32768, 49152
LOADS = (32, 64, 128, 256, 288, 160)
E_SLOTS = 9
E_ROWS = 2048
LATE = 24
AHEAD = 4
FRONT = AHEAD * 32


def bounds(sizes):
    out, at = [], 0
    for n in sizes:
        out.append((at, n))
        at += n
    return out


LOAD = bounds(LOADS)
PIECES = HALF // GROUP
LAGS = ((0, 3, 6, 9, 14, 20, 25, 29, 41), (0, 3, 6, 10, 16, 20, 24, 30, 45))
SEQUENCE = ((0, 0), (8, 1), (4, 1), (5, 0), (3, 1), (6, 0), (7, 1), (1, 0), (2, 1), (3, 0), (8, 0), (7, 0), (4, 0), (1, 1), (5, 1), (2, 0), (0, 1), (6, 1))
STEPS = PIECES + max(map(max, LAGS))
FIRST_ADAM = min(lags[4] for lags in LAGS)
LAST_ADAM = max(lags[4] for lags in LAGS) + PIECES - 1
MOVES = FIRST_ADAM - 6


def start_row(d):
    return LAST_START if d == LAST else 32 * (SPAN * d // 64)


def merge_row(d):
    return 32 * (SPAN * d // 64)


def segments(row, n):
    out = []
    for t in range(5):
        lo, hi = max(row, STARTS[t]), min(row + n, STARTS[t + 1])
        if lo < hi:
            out.append((t, lo - STARTS[t], lo - row, hi - lo))
    return out


def slot_of(color, k, late=False):
    x, y, z0, z1 = k % 2, k // 2 % 2, k // 4 % 2, k // 8
    first, third = (x, y) if color == 0 else (y, x)
    return first * 8 + (third * 4 + z0 * 2 if late else z0 * 4 + third * 2) + z1


def big_kernel(ge, ga, gf1, gf2, gb, m_in, v_in, w_in, gat, stage, acc_a, acc_b, pair_a, pair_b, last_a, last_b, line_m, line_v, line_w, cov, ld_sem, pr_recv, pr_send, rs_recv, rs_send, ag_recv, ag_send, dag_recv, dag_send, state_sem):
    grads = (ge, ga, gf1, gf2, gb)
    acc, pair, final = (acc_a, acc_b), (pair_a, pair_b), (last_a, last_b)
    z, y, inner = lax.axis_index('outer'), lax.axis_index('middle'), lax.axis_index('inner')
    x, c = inner // 2, inner % 2
    z0, z1 = z % 2, z // 2
    dev = (z * 2 + y) * 4 + inner
    to_pair = {'inner': inner + 1 - 2 * c}
    to_x = {'inner': inner + 2 - 4 * x}
    to_y = {'middle': 1 - y}
    to_z0 = {'outer': z + 1 - 2 * z0}
    to_z1 = {'outer': z + 2 - 4 * z1}
    routes = ((to_x, to_z0, to_y, to_z1), (to_y, to_z0, to_x, to_z1))
    bits = ((x, z0, y, z1), (y, z0, x, z1))

    barrier = pltpu.get_barrier_semaphore()
    for to in (to_pair, to_x, to_y, to_z0, to_z1):
        pl.semaphore_signal(barrier, inc=1, device_id=to, device_id_type=MESH)

    def load_one(color, i, tensor, row, slot, at, n, mine):
        src = grads[tensor].at[pl.ds(row, n)]
        if mine:
            pltpu.make_async_copy(src, acc[color].at[slot, pl.ds(at, n)], ld_sem.at[color, i]).start()
        else:
            pltpu.make_async_remote_copy(src, pair[color].at[slot, pl.ds(FRONT + at, n)], pr_send.at[color], pr_recv.at[color, i], device_id=to_pair, device_id_type=MESH).start()

    def load(i, sides=(True, False)):
        at, n = LOAD[i]
        for color in COLORS:
            @pl.loop(0, E_SLOTS)
            def _(k):
                slot = slot_of(color, k, at >= LATE * GROUP)
                for mine in sides:
                    d = 2 * k + (c if mine else 1 - c)
                    row = pl.multiple_of(GROUP * ((SPAN * d) // 64), GROUP) + color * HALF + at
                    load_one(color, i, 0, row, slot, at, n, mine)
            for core in COLORS:
                @pl.when(c == core)
                def _():
                    for k in range(E_SLOTS, NDEV // 2):
                        slot = slot_of(color, k, at >= LATE * GROUP)
                        for mine in sides:
                            d = 2 * k + (core if mine else 1 - core)
                            for tensor, row, off, rows in segments(start_row(d) + color * HALF + at, n):
                                load_one(color, i, tensor, row, slot, at + off, rows, mine)

    load(0, (True,))
    lines = (line_m, line_v, line_w)
    state_in = [pltpu.make_async_copy(src, lines[i], state_sem.at[i]) for i, src in enumerate((m_in, v_in, w_in))]
    for copy in state_in:
        copy.start()
    pl.semaphore_wait(barrier, 5)

    def wait_on(ref, sem):
        pltpu.make_async_copy(ref, ref, sem).wait()

    def rows_at(p):
        return pl.ds(pl.multiple_of(p * GROUP, GROUP), GROUP)

    def rows_at(p):
        return pl.ds(pl.multiple_of(p * GROUP, GROUP), GROUP)

    def add(color, into, slots, first, p, block):
        acc[color][pl.ds(into, slots), rows_at(p), :] += pair[color][pl.ds(first, slots), rows_at(block), :]

    def landing(color, s, p):
        if s == 3:
            return final[color].at[:, rows_at(p)]
        return pair[color].at[pl.ds(16 - (16 >> s), TILE >> s), rows_at(p)]

    def base(color, level):
        return sum((bits[color][i] * (TILE >> i) for i in range(level)), 0 * c)

    def halved(color, level, p):
        one, other = bits[color][level], bits[color][3 - level if level in (1, 2) else level]
        return jnp.where(p >= LATE, other, one)

    def reduce_base(color, level, p):
        return sum((halved(color, i, p) * (TILE >> i) for i in range(level)), 0 * c)

    def reduce_to(color, s, p):
        if s in (0, 3):
            return routes[color][s]
        along_z = p < LATE if s == 1 else p >= LATE
        across_y = jnp.logical_not(along_z) & (color == 0)
        across_x = jnp.logical_not(along_z) & (color == 1)
        return {'outer': jnp.where(along_z, to_z0['outer'], z), 'middle': jnp.where(across_y, 1 - y, y), 'inner': jnp.where(across_x, to_x['inner'], inner)}

    def reduce_send(color, s, p):
        size = TILE >> s
        first = reduce_base(color, s, p) + (1 - halved(color, s, p)) * size
        pltpu.make_async_remote_copy(acc[color].at[pl.ds(first, size), rows_at(p)], landing(color, s, p), rs_send.at[color, s], rs_recv.at[color, s, p], device_id=reduce_to(color, s, p), device_id_type=MESH).start()

    def pair_out(color, slot, size, p):
        block = gat.at[color, c, pl.ds(slot, size), rows_at(p)]
        pltpu.make_async_remote_copy(block, block, dag_send.at[color], dag_recv.at[color], device_id=to_pair, device_id_type=MESH).start()

    def adam_block(g, load_state, store_state):
        g = g * (1.0 / NDEV)
        m = BETA1 * load_state(0) + (1.0 - BETA1) * g
        v = BETA2 * load_state(1) + (1.0 - BETA2) * (g * g)
        m_hat = m / (1.0 - BETA1 ** STEP)
        v_hat = v / (1.0 - BETA2 ** STEP)
        w = load_state(2) - RATE * m_hat / (jnp.sqrt(v_hat) + EPS)
        store_state(0, m)
        store_state(1, v)
        store_state(2, w)
        return w

    cover_start = jnp.where(dev == LAST, LAST_START, GROUP * ((SPAN * dev) // 64))

    def adam(color, p):
        slot, summed = base(color, 4), reduce_base(color, 4, p)
        r = pl.multiple_of(p * GROUP, GROUP)
        f = pl.multiple_of(color * HALF + r, GROUP)
        row = cover_start + f
        permuted = (row >= PERM_LO) & (row < PERM_HI)
        vectors = row + GROUP > STARTS[4]

        def tiles(t, index):
            parts = []
            for q in (2 * t, 2 * t + 1):
                where = index(q)

                def keep(i, value, where=where):
                    cov[i, where, :] = value

                parts.append(adam_block(acc[color][summed, pl.ds(r + TILE * q, TILE), :], lambda i, where=where: cov[i, where, :], keep))
            gat[color, c, slot, pl.ds(r + 16 * t, 16), :] = jnp.concatenate(parts, axis=0).astype(jnp.bfloat16)

        def plain(q):
            return pl.ds(f + TILE * q, TILE)

        def vector_tile(q):
            tile = (row + TILE * q - STARTS[4]) // TILE
            return pl.ds(STARTS[4] - LAST_START + tile // VEC_TILES * VEC_TILES * TILE + tile % VEC_TILES, TILE, stride=VEC_TILES)

        @pl.when(permuted)
        def _():
            for t in COLORS:
                tiles(t, lambda q: pl.ds(f + q, TILE, stride=4))

        @pl.when(jnp.logical_not(permuted | vectors))
        def _():
            for t in COLORS:
                tiles(t, plain)

        @pl.when(vectors)
        def _():
            for t in COLORS:
                inside = row + 16 * t >= STARTS[4]
                pl.when(inside)(functools.partial(tiles, t, vector_tile))
                pl.when(jnp.logical_not(inside))(functools.partial(tiles, t, plain))

    half_rows = jnp.where(dev == LAST, 115, (SPAN * dev) % 64)
    shift = half_rows // 2
    lane = lax.broadcasted_iota(jnp.int32, (GROUP, LANES), 1)

    def moved(first, second):
        return jnp.where(lane < 64, pltpu.roll(first, 64, 1), pltpu.roll(second, 64, 1))

    def state_rows():
        for i, copy in enumerate(state_in):
            copy.wait()
            stage[i, 0:MARGIN, :] = jnp.zeros((MARGIN, LANES), jnp.float32)
            stage[i, MARGIN + SLICE_ROWS - TILE:, :] = jnp.zeros((MARGIN + TILE, LANES), jnp.float32)
            cov[i, ROWS:, :] = jnp.zeros((COVER - ROWS, LANES), jnp.float32)
            for r in range(REST, 1798):
                stage[i, MARGIN + r:MARGIN + r + 1, :] = lines[i][LANES * r:LANES * r + LANES].reshape(1, LANES)
            stage[i, MARGIN + 1798:MARGIN + 1799, 0:64] = lines[i][SLICE - 64:].reshape(1, 64)

    def state_rows_part(t):
        @pl.loop(0, 56)
        def _(k):
            j = t * 56 + k
            for i in range(3):
                stage[i, pl.ds(pl.multiple_of(MARGIN + j * TILE, TILE), TILE), :] = lines[i][pl.ds(pl.multiple_of(j * BLOCK, BLOCK), BLOCK)].reshape(TILE, LANES)

    def state_to_cover(t):
        @pl.loop(0, -(-ROWS // GROUP // MOVES))
        def _(k):
            f = pl.multiple_of(jnp.minimum((t + k * MOVES) * GROUP, ROWS - GROUP), GROUP)
            r = MARGIN + f - shift
            for i in range(3):
                here = stage[i, pl.ds(r, GROUP), :]
                before = stage[i, pl.ds(r - 1, GROUP), :]
                cov[i, pl.ds(f, GROUP), :] = jnp.where(c == 1, moved(before, here), here)

    def cover_to_state(t):
        @pl.loop(0, 15)
        def _(k):
            r = pl.multiple_of((t * 15 + k) * TILE, TILE)
            for i in range(3):
                here = cov[i, pl.ds(r + shift, TILE), :]
                after = cov[i, pl.ds(r + shift + 1, TILE), :]
                both = jnp.where(lane[:TILE] < 64, pltpu.roll(here, 64, 1), pltpu.roll(after, 64, 1))
                stage[i, pl.ds(pl.multiple_of(MARGIN + r, TILE), TILE), :] = jnp.where(c == 1, both, here)

    def state_out():
        for i, dst in enumerate((m_out, v_out, w_out)):
            pltpu.make_async_copy(stage.at[i, pl.ds(MARGIN, SLICE_ROWS)], dst, state_sem.at[i]).start()

    def start_pieces(color, p):
        for i, (first, n) in enumerate(LOAD):
            @pl.when(p == first // GROUP)
            def _():
                wait_on(acc[color].at[:, pl.ds(first, n)], ld_sem.at[color, i])
                wait_on(pair[color].at[:, pl.ds(FRONT + first, n)], pr_recv.at[color, i])
        bit = bits[color][0]
        for slot in ((1 - bit) * TILE, bit * TILE):
            add(color, slot, TILE, slot, p, p + AHEAD)
        reduce_send(color, 0, p)

    def reduce_piece(color, stage_no, p):
        s = stage_no - 1
        wait_on(landing(color, s, p), rs_recv.at[color, s, p])
        first, size, bit = reduce_base(color, stage_no, p), 4 >> s, halved(color, stage_no, p)
        for half in (1 - bit, bit):
            add(color, first + half * size, size, 16 - (16 >> s) + half * size, p, p)
        reduce_send(color, stage_no, p)

    def adam_piece(color, p):
        wait_on(landing(color, 3, p), rs_recv.at[color, 3, p])
        slot = base(color, 4)
        acc[color][reduce_base(color, 4, p), rows_at(p), :] += final[color][0, rows_at(p), :]
        adam(color, p)
        gather_send(color, 0, slot, 1, p)

    def gather_send(color, s, first, size, p):
        block = gat.at[color, c, pl.ds(first, size), rows_at(p)]
        pltpu.make_async_remote_copy(block, block, ag_send.at[color, s], ag_recv.at[color, s, p], device_id=routes[color][3 - s], device_id_type=MESH).start()

    def gather_piece(color, s, p):
        level, size = 4 - s, 1 << s
        arrived = base(color, level - 1) + (1 - bits[color][level - 1]) * size
        wait_on(gat.at[color, c, pl.ds(arrived, size), rows_at(p)], ag_recv.at[color, s, p])
        if s < 3:
            gather_send(color, s + 1, base(color, level - 1), 2 * size, p)
        if s > 1:
            pair_out(color, arrived if s == 3 else base(color, 1), TILE, p)

    load(0, (False,))

    @pl.loop(0, STEPS)
    def _(t):
        for i in range(2, len(LOAD)):
            pl.when(t == LOAD[i - 1][0] // GROUP)(functools.partial(load, i))
        for stage_no, color in SEQUENCE:
            p = t - LAGS[color][stage_no]

            @pl.when((p >= 0) & (p < PIECES))
            def _():
                if stage_no == 0:
                    start_pieces(color, p)
                elif stage_no < 4:
                    reduce_piece(color, stage_no, p)
                elif stage_no == 4:
                    adam_piece(color, p)
                else:
                    gather_piece(color, stage_no - 5, p)

        pl.when(t == 0)(functools.partial(load, 1))

        @pl.when(t == 1)
        def _():
            state_rows()

        @pl.when((t >= 2) & (t < 6))
        def _():
            state_rows_part(t - 2)

        @pl.when((t >= 6) & (t < FIRST_ADAM))
        def _():
            state_to_cover(t - 6)

        @pl.when((t > LAST_ADAM) & (t <= LAST_ADAM + 15))
        def _():
            cover_to_state(t - LAST_ADAM - 1)

    for color in COLORS:
        wait_on(gat.at[color, 1 - c], dag_recv.at[color])
        wait_on(gat.at[color, c], dag_send.at[color])
        wait_on(acc[color], pr_send.at[color])
        for s in range(4):
            wait_on(acc[color].at[pl.ds(0, TILE >> s)], rs_send.at[color, s])
            wait_on(gat.at[color, 0, pl.ds(0, 1 << s)], ag_send.at[color, s])


def place_kernel(gat, stage, e_out, a_out, f1_out, f2_out, b_out, m_out, v_out, w_out, chip_out, merged, loose, vec, tail, block, out_sem, edge_sem, state_sem, chip_sem):
    outs = (e_out, a_out, f1_out, f2_out, b_out)
    chip = (lax.axis_index('outer') * 2 + lax.axis_index('middle')) * 2 + lax.axis_index('inner') // 2
    started = [pltpu.make_async_copy(stage.at[i, pl.ds(MARGIN, SLICE_ROWS)], dst, state_sem.at[i]) for i, dst in enumerate((m_out, v_out, w_out))]

    def rows_from(d, at, n):
        color = at // HALF
        return gat.at[color, d % 2, slot_of(color, d // 2), pl.ds(at - color * HALF, n)]

    row = lax.broadcasted_iota(jnp.int32, (GROUP, LANES), 0)
    lane = lax.broadcasted_iota(jnp.int32, (GROUP, LANES), 1)
    tile_order = (row % TILE) * 4 + row // TILE
    count = 0
    for d in range(NDEV):
        first = merge_row(d)
        last = merge_row(d + 1) if d < LAST else STARTS[-1]
        begin = start_row(d)
        for color in COLORS:
            lo = max(first + (GROUP if d else 0), begin + color * HALF)
            for tensor, at, off, n in segments(lo, min(last, begin + (color + 1) * HALF) - lo):
                started.append(pltpu.make_async_copy(rows_from(d, lo + off - begin, n), outs[tensor].at[pl.ds(at, n)], out_sem.at[count]))
                count += 1
    for copy in started:
        copy.start()
    for d in range(1, NDEV):
        first = merge_row(d)
        flat = tile_order if PERM_LO <= first < PERM_HI else row
        keep = 2 * flat + lane // 64 >= SPAN * d - 2 * first
        new, old = (rows_from(e, first - start_row(e), GROUP)[...].astype(jnp.float32) for e in (d, d - 1))
        merged[d] = jnp.where(keep, new, old).astype(jnp.bfloat16)
        (tensor, at, _, _), = segments(first, GROUP)
        copy = pltpu.make_async_copy(merged.at[d], outs[tensor].at[pl.ds(at, GROUP)], edge_sem.at[d])
        copy.start()
        started.append(copy)

    def rows_of(group):
        d = (64 * group + 63) * INVERSE[0] >> INVERSE[1]
        begin = jnp.where(d == LAST, LAST_START, (SPAN * d >> 6) * GROUP)
        x, y, z0, z1 = ((d >> i) & 1 for i in range(1, 5))
        halves = []
        for h in COLORS:
            at = GROUP * group - begin + 16 * h
            color = (at >= HALF).astype(jnp.int32)
            slot = jnp.where(color == 0, x, y) * TILE + z0 * 4 + jnp.where(color == 0, y, x) * 2 + z1
            halves.append(gat[color, d & 1, slot, pl.ds(pl.multiple_of(at - color * HALF, 16), 16), :])
        return halves

    def put(at, rows):
        block[0:1, pl.ds(pl.multiple_of(at * LANES, BLOCK), BLOCK)] = rows.reshape(1, BLOCK).astype(jnp.bfloat16)
    def put_rows(at, halves):
        for h, half in enumerate(halves):
            rows = half.astype(jnp.float32)
            for q in COLORS:
                put(at + 16 * h + TILE * q, rows[TILE * q:TILE * q + TILE])

    def put_tiles(at, halves, t):
        for h, half in enumerate(halves):
            rows = half.astype(jnp.float32)
            for q in COLORS:
                loose[t, pl.ds(2 * h + q, TILE, stride=4), :] = rows[TILE * q:TILE * q + TILE]
        for q in range(4):
            put(at + TILE * q, loose[t, TILE * q:TILE * q + TILE, :])

    def put_edges(tensors):
        for d in range(1, NDEV):
            (tensor, at, _, _), = segments(merge_row(d), GROUP)
            if tensor not in tensors:
                continue
            layer, owner = divmod(at // GROUP, 16)

            @pl.when(chip == (owner if tensor else at // E_ROWS))
            def _():
                halves = (merged[d, 0:16, :], merged[d, 16:, :])
                if tensor in (1, 2):
                    put_tiles(1536 + 512 * tensor + GROUP * layer, halves, tensor - 1)
                else:
                    put_rows(3072 + GROUP * layer if tensor else at % E_ROWS, halves)

    @pl.loop(0, 64, unroll=4)
    def _(j):
        put_rows(GROUP * j, rows_of(chip * 64 + j))

    put_edges((0,))
    split = E_ROWS * LANES
    sends = [pltpu.make_async_copy(block.at[:, pl.ds(at, n)], chip_out.at[:, pl.ds(at, n)], chip_sem.at[i]) for i, (at, n) in enumerate(((0, split), (split, 2 * SLICE - split)))]
    sends[0].start()

    @pl.loop(0, 16, unroll=2)
    def _(layer):
        for t in (1, 2):
            put_tiles(1536 + 512 * t + GROUP * layer, rows_of(STARTS[t] // GROUP + layer * 16 + chip), t - 1)
        put_rows(3072 + GROUP * layer, rows_of(STARTS[3] // GROUP + layer * 16 + chip))

    put_edges((1, 2, 3))
    at = STARTS[4] - start_row(LAST)
    vec[0:208, :] = rows_from(LAST, at, 208)[...].astype(jnp.float32)
    vec[208:, :] = jnp.zeros((16, LANES), jnp.float32)
    tail[...] = jnp.zeros_like(tail)
    begin = (104 * chip) % LANES
    line = lax.broadcasted_iota(jnp.int32, (TILE, LANES), 1)
    for layer in range(16):
        source = layer // TILE * TILE * VEC_TILES + layer % TILE + (104 * chip) // LANES * TILE
        to = layer * 104 // LANES
        off = layer * 104 % LANES
        turn = (off - begin + LANES) % LANES
        one = pltpu.roll(vec[pl.ds(source, TILE), :], turn, 1)
        two = pltpu.roll(vec[pl.ds(source + TILE, TILE), :], turn, 1)
        t = (line - off + LANES) % LANES
        got = jnp.where(begin + t < LANES, one, two)
        here = (t < 104) & (line >= off)
        tail[to:to + 1, :] = jnp.where(here, got, tail[pl.ds(to, TILE), :])[0:1]
        if off + 104 > LANES:
            there = (t < 104) & (line < off)
            tail[to + 1:to + 2, :] = jnp.where(there, got, tail[pl.ds(to + 1, TILE), :])[0:1]
    put(3584, tail[0:TILE, :])
    block[0:1, 3592 * LANES:] = tail[TILE:16, :].reshape(1, BLOCK)[:, 0:640].astype(jnp.bfloat16)
    sends[1].start()
    for copy in started + sends:
        copy.wait()


def tile_rows(tensor, tiles=4):
    return tensor.reshape(-1, TILE, tiles, LANES).transpose(0, 2, 1, 3).reshape(-1, LANES)


def untile(rows, shape, tiles=4):
    return rows.reshape(-1, tiles, TILE, LANES).transpose(0, 2, 1, 3).reshape(shape)


def solution(mesh):
    def local_step(g_embed, g_attn, g_ffn_in, g_ffn_out, g_vec, m_shard, v_shard, w_shard):
        grads = (g_embed[0], tile_rows(g_attn[0]), tile_rows(g_ffn_in[0]), g_ffn_out[0].reshape(-1, LANES), tile_rows(g_vec[0], VEC_TILES))
        any_spec, vmem_spec = pl.BlockSpec(memory_space=pl.ANY), pl.BlockSpec(memory_space=pltpu.VMEM)
        f32, bf16 = jnp.float32, jnp.bfloat16
        flat = jax.ShapeDtypeStruct((SLICE_ROWS, LANES), f32)
        dma = pltpu.SemaphoreType.DMA
        gathered, stage = pl.pallas_call(
            big_kernel,
            out_shape=(pltpu.VMEM((2, 2, 16, HALF, LANES), bf16), pltpu.VMEM((3, SLICE_ROWS + 2 * MARGIN, LANES), f32)),
            in_specs=[any_spec] * 8,
            out_specs=[vmem_spec] * 2,
            scratch_shapes=[pltpu.VMEM((16, HALF, LANES), f32)] * 2 + [pltpu.VMEM((16, HALF + FRONT, LANES), f32)] * 2 + [pltpu.VMEM((1, HALF, LANES), f32)] * 2 + [pltpu.VMEM((SLICE,), f32)] * 3 + [pltpu.VMEM((3, COVER, LANES), f32)]
            + [dma((2, len(LOADS))), dma((2, len(LOADS))), dma((2,)), dma((2, 4, PIECES)), dma((2, 4)), dma((2, 4, PIECES)), dma((2, 4)), dma((2,)), dma((2,)), dma((3,))],
            compiler_params=pltpu.CompilerParams(collective_id=0, has_side_effects=True, vmem_limit_bytes=BIG_VMEM),
            name='reduce_adam_gather',
        )(*grads, m_shard, v_shard, w_shard)
        placed = pl.pallas_call(
            place_kernel,
            out_shape=[jax.ShapeDtypeStruct((n, LANES), bf16) for n in TENSOR_ROWS] + [flat] * 3 + [jax.ShapeDtypeStruct((1, 2 * SLICE), bf16)],
            in_specs=[vmem_spec] * 2,
            out_specs=[any_spec] * 9,
            scratch_shapes=[pltpu.VMEM((NDEV, GROUP, LANES), bf16), pltpu.VMEM((2, GROUP, LANES), f32), pltpu.VMEM((224, LANES), f32), pltpu.VMEM((24, LANES), f32), pltpu.VMEM((1, 2 * SLICE), bf16)]
            + [dma((2 * NDEV + TILE,)), dma((NDEV,)), dma((3,)), dma((2,))],
            compiler_params=pltpu.CompilerParams(vmem_limit_bytes=PLACE_VMEM),
            name='place',
        )(gathered, stage)
        e, a, f1, f2, b, *state, w_chip = placed
        tensors = (e, untile(a, (16, LANES, 512)), untile(f1, (16, LANES, 512)), f2.reshape(16, 512, LANES), untile(b, (16, 1664), VEC_TILES))
        return tuple(t.reshape(-1)[:SLICE] for t in state) + tensors + (w_chip,)

    return jax.shard_map(local_step, mesh=mesh, in_specs=(P(MESH_AXES),) * TILE, out_specs=(P(MESH_AXES),) * 3 + (P(),) * 5 + (P(MESH_AXES),), check_vma=False)
```

```python
import functools

import jax
import jax.numpy as jnp
from jax import lax
from jax.experimental import pallas as pl
from jax.experimental.pallas import tpu as pltpu
from jax.sharding import PartitionSpec as P

MESH_AXES = ('outer', 'middle', 'inner')
MESH = pl.DeviceIdType.MESH
BETA1, BETA2, EPS, RATE, STEP = 0.9, 0.98, 1e-9, 0.05, 3

NDEV = 32
GROUP = 32
LANES = 128
TILE = 8
BLOCK = 1024
LAST = NDEV - 1
LAST_START = 55696
SPAN = 3597
COLORS = (0, 1)
REST = 1792
ROWS = 1856
HALF = ROWS // 2
SLICE = 230208
SLICE_ROWS = 1800
MARGIN = 64
BIG_VMEM, PLACE_VMEM = 43 << 20, 8 << 20
COVER = ROWS + 8
TENSOR_ROWS = (32768, 8192, 8192, 8192, 208)
STARTS = (0, 32768, 40960, 49152, 57344, 57552)
VEC_TILES = 13
INVERSE = (9329, 25)
PERM_LO, PERM_HI = 32768, 49152
LOADS = (32, 64, 128, 256, 256, 192)
E_SLOTS = 9
E_ROWS = 2048
LATE = 23
AHEAD = 4
FRONT = AHEAD * 32


def bounds(sizes):
    out, at = [], 0
    for n in sizes:
        out.append((at, n))
        at += n
    return out


LOAD = bounds(LOADS)
PIECES = HALF // GROUP
LAGS = ((0, 3, 6, 9, 15, 20, 25, 29, 33), (0, 3, 5, 8, 14, 19, 24, 29, 33))
SEQUENCE = ((8, 0), (7, 1), (4, 1), (6, 0), (1, 1), (0, 0), (4, 0), (3, 1), (1, 0), (0, 1), (2, 0), (6, 1), (5, 1), (2, 1), (5, 0), (7, 0), (8, 1), (3, 0))
STEPS = PIECES + max(map(max, LAGS))
FIRST_ADAM = min(lags[4] for lags in LAGS)
LAST_ADAM = max(lags[4] for lags in LAGS) + PIECES - 1
MOVES = FIRST_ADAM - 6


def start_row(d):
    return LAST_START if d == LAST else 32 * (SPAN * d // 64)


def merge_row(d):
    return 32 * (SPAN * d // 64)


def segments(row, n):
    out = []
    for t in range(5):
        lo, hi = max(row, STARTS[t]), min(row + n, STARTS[t + 1])
        if lo < hi:
            out.append((t, lo - STARTS[t], lo - row, hi - lo))
    return out


def slot_of(color, k, late=False):
    x, y, z0, z1 = k % 2, k // 2 % 2, k // 4 % 2, k // 8
    first, third = (x, y) if color == 0 else (y, x)
    return first * 8 + (third * 4 + z0 * 2 if late else z0 * 4 + third * 2) + z1


def big_kernel(ge, ga, gf1, gf2, gb, m_in, v_in, w_in, gat, stage, acc_a, acc_b, pair_a, pair_b, last_a, last_b, line_m, line_v, line_w, cov, ld_sem, pr_recv, pr_send, rs_recv, rs_send, ag_recv, ag_send, dag_recv, dag_send, state_sem):
    grads = (ge, ga, gf1, gf2, gb)
    acc, pair, final = (acc_a, acc_b), (pair_a, pair_b), (last_a, last_b)
    z, y, inner = lax.axis_index('outer'), lax.axis_index('middle'), lax.axis_index('inner')
    x, c = inner // 2, inner % 2
    z0, z1 = z % 2, z // 2
    dev = (z * 2 + y) * 4 + inner
    to_pair = {'inner': inner + 1 - 2 * c}
    to_x = {'inner': inner + 2 - 4 * x}
    to_y = {'middle': 1 - y}
    to_z0 = {'outer': z + 1 - 2 * z0}
    to_z1 = {'outer': z + 2 - 4 * z1}
    routes = ((to_x, to_z0, to_y, to_z1), (to_y, to_z0, to_x, to_z1))
    bits = ((x, z0, y, z1), (y, z0, x, z1))

    barrier = pltpu.get_barrier_semaphore()
    for to in (to_pair, to_x, to_y, to_z0, to_z1):
        pl.semaphore_signal(barrier, inc=1, device_id=to, device_id_type=MESH)

    def load_one(color, i, tensor, row, slot, at, n, mine):
        src = grads[tensor].at[pl.ds(row, n)]
        if mine:
            pltpu.make_async_copy(src, acc[color].at[slot, pl.ds(at, n)], ld_sem.at[color, i]).start()
        else:
            pltpu.make_async_remote_copy(src, pair[color].at[slot, pl.ds(FRONT + at, n)], pr_send.at[color], pr_recv.at[color, i], device_id=to_pair, device_id_type=MESH).start()

    def load(i, sides=(True, False)):
        at, n = LOAD[i]
        for color in COLORS:
            @pl.loop(0, E_SLOTS)
            def _(k):
                slot = slot_of(color, k, at >= LATE * GROUP)
                for mine in sides:
                    d = 2 * k + (c if mine else 1 - c)
                    row = pl.multiple_of(GROUP * ((SPAN * d) // 64), GROUP) + color * HALF + at
                    load_one(color, i, 0, row, slot, at, n, mine)
            for core in COLORS:
                @pl.when(c == core)
                def _():
                    for k in range(E_SLOTS, NDEV // 2):
                        slot = slot_of(color, k, at >= LATE * GROUP)
                        for mine in sides:
                            d = 2 * k + (core if mine else 1 - core)
                            for tensor, row, off, rows in segments(start_row(d) + color * HALF + at, n):
                                load_one(color, i, tensor, row, slot, at + off, rows, mine)

    load(0, (True,))
    lines = (line_m, line_v, line_w)
    state_in = [pltpu.make_async_copy(src, lines[i], state_sem.at[i]) for i, src in enumerate((m_in, v_in, w_in))]
    for copy in state_in:
        copy.start()
    pl.semaphore_wait(barrier, 5)

    def wait_on(ref, sem):
        pltpu.make_async_copy(ref, ref, sem).wait()

    def rows_at(p):
        return pl.ds(pl.multiple_of(p * GROUP, GROUP), GROUP)

    def rows_at(p):
        return pl.ds(pl.multiple_of(p * GROUP, GROUP), GROUP)

    def add(color, into, slots, first, p, block):
        acc[color][pl.ds(into, slots), rows_at(p), :] += pair[color][pl.ds(first, slots), rows_at(block), :]

    def landing(color, s, p):
        if s == 3:
            return final[color].at[:, rows_at(p)]
        return pair[color].at[pl.ds(16 - (16 >> s), TILE >> s), rows_at(p)]

    def base(color, level):
        return sum((bits[color][i] * (TILE >> i) for i in range(level)), 0 * c)

    def halved(color, level, p):
        one, other = bits[color][level], bits[color][3 - level if level in (1, 2) else level]
        return jnp.where(p >= LATE, other, one)

    def reduce_base(color, level, p):
        return sum((halved(color, i, p) * (TILE >> i) for i in range(level)), 0 * c)

    def reduce_to(color, s, p):
        if s in (0, 3):
            return routes[color][s]
        along_z = p < LATE if s == 1 else p >= LATE
        across_y = jnp.logical_not(along_z) & (color == 0)
        across_x = jnp.logical_not(along_z) & (color == 1)
        return {'outer': jnp.where(along_z, to_z0['outer'], z), 'middle': jnp.where(across_y, 1 - y, y), 'inner': jnp.where(across_x, to_x['inner'], inner)}

    def reduce_send(color, s, p):
        size = TILE >> s
        first = reduce_base(color, s, p) + (1 - halved(color, s, p)) * size
        pltpu.make_async_remote_copy(acc[color].at[pl.ds(first, size), rows_at(p)], landing(color, s, p), rs_send.at[color, s], rs_recv.at[color, s, p], device_id=reduce_to(color, s, p), device_id_type=MESH).start()

    def pair_out(color, slot, size, p):
        block = gat.at[color, c, pl.ds(slot, size), rows_at(p)]
        pltpu.make_async_remote_copy(block, block, dag_send.at[color], dag_recv.at[color], device_id=to_pair, device_id_type=MESH).start()

    def adam_block(g, load_state, store_state):
        g = g * (1.0 / NDEV)
        m = BETA1 * load_state(0) + (1.0 - BETA1) * g
        v = BETA2 * load_state(1) + (1.0 - BETA2) * (g * g)
        m_hat = m / (1.0 - BETA1 ** STEP)
        v_hat = v / (1.0 - BETA2 ** STEP)
        w = load_state(2) - RATE * m_hat / (jnp.sqrt(v_hat) + EPS)
        store_state(0, m)
        store_state(1, v)
        store_state(2, w)
        return w

    cover_start = jnp.where(dev == LAST, LAST_START, GROUP * ((SPAN * dev) // 64))

    def adam(color, p):
        slot, summed = base(color, 4), reduce_base(color, 4, p)
        r = pl.multiple_of(p * GROUP, GROUP)
        f = pl.multiple_of(color * HALF + r, GROUP)
        row = cover_start + f
        permuted = (row >= PERM_LO) & (row < PERM_HI)
        vectors = row + GROUP > STARTS[4]

        def tiles(t, index):
            parts = []
            for q in (2 * t, 2 * t + 1):
                where = index(q)

                def keep(i, value, where=where):
                    cov[i, where, :] = value

                parts.append(adam_block(acc[color][summed, pl.ds(r + TILE * q, TILE), :], lambda i, where=where: cov[i, where, :], keep))
            gat[color, c, slot, pl.ds(r + 16 * t, 16), :] = jnp.concatenate(parts, axis=0).astype(jnp.bfloat16)

        def plain(q):
            return pl.ds(f + TILE * q, TILE)

        def vector_tile(q):
            tile = (row + TILE * q - STARTS[4]) // TILE
            return pl.ds(STARTS[4] - LAST_START + tile // VEC_TILES * VEC_TILES * TILE + tile % VEC_TILES, TILE, stride=VEC_TILES)

        @pl.when(permuted)
        def _():
            for t in COLORS:
                tiles(t, lambda q: pl.ds(f + q, TILE, stride=4))

        @pl.when(jnp.logical_not(permuted | vectors))
        def _():
            for t in COLORS:
                tiles(t, plain)

        @pl.when(vectors)
        def _():
            for t in COLORS:
                inside = row + 16 * t >= STARTS[4]
                pl.when(inside)(functools.partial(tiles, t, vector_tile))
                pl.when(jnp.logical_not(inside))(functools.partial(tiles, t, plain))

    half_rows = jnp.where(dev == LAST, 115, (SPAN * dev) % 64)
    shift = half_rows // 2
    lane = lax.broadcasted_iota(jnp.int32, (GROUP, LANES), 1)

    def moved(first, second):
        return jnp.where(lane < 64, pltpu.roll(first, 64, 1), pltpu.roll(second, 64, 1))

    def state_rows():
        for i, copy in enumerate(state_in):
            copy.wait()
            stage[i, 0:MARGIN, :] = jnp.zeros((MARGIN, LANES), jnp.float32)
            stage[i, MARGIN + SLICE_ROWS - TILE:, :] = jnp.zeros((MARGIN + TILE, LANES), jnp.float32)
            cov[i, ROWS:, :] = jnp.zeros((COVER - ROWS, LANES), jnp.float32)
            for r in range(REST, 1798):
                stage[i, MARGIN + r:MARGIN + r + 1, :] = lines[i][LANES * r:LANES * r + LANES].reshape(1, LANES)
            stage[i, MARGIN + 1798:MARGIN + 1799, 0:64] = lines[i][SLICE - 64:].reshape(1, 64)

    def state_rows_part(t):
        @pl.loop(0, 56)
        def _(k):
            j = t * 56 + k
            for i in range(3):
                stage[i, pl.ds(pl.multiple_of(MARGIN + j * TILE, TILE), TILE), :] = lines[i][pl.ds(pl.multiple_of(j * BLOCK, BLOCK), BLOCK)].reshape(TILE, LANES)

    def state_to_cover(t):
        @pl.loop(0, -(-ROWS // GROUP // MOVES))
        def _(k):
            f = pl.multiple_of(jnp.minimum((t + k * MOVES) * GROUP, ROWS - GROUP), GROUP)
            r = MARGIN + f - shift
            for i in range(3):
                here = stage[i, pl.ds(r, GROUP), :]
                before = stage[i, pl.ds(r - 1, GROUP), :]
                cov[i, pl.ds(f, GROUP), :] = jnp.where(c == 1, moved(before, here), here)

    def cover_to_state(t):
        @pl.loop(0, 15)
        def _(k):
            r = pl.multiple_of((t * 15 + k) * TILE, TILE)
            for i in range(3):
                here = cov[i, pl.ds(r + shift, TILE), :]
                after = cov[i, pl.ds(r + shift + 1, TILE), :]
                both = jnp.where(lane[:TILE] < 64, pltpu.roll(here, 64, 1), pltpu.roll(after, 64, 1))
                stage[i, pl.ds(pl.multiple_of(MARGIN + r, TILE), TILE), :] = jnp.where(c == 1, both, here)

    def state_out():
        for i, dst in enumerate((m_out, v_out, w_out)):
            pltpu.make_async_copy(stage.at[i, pl.ds(MARGIN, SLICE_ROWS)], dst, state_sem.at[i]).start()

    def start_pieces(color, p):
        for i, (first, n) in enumerate(LOAD):
            @pl.when(p == first // GROUP)
            def _():
                wait_on(acc[color].at[:, pl.ds(first, n)], ld_sem.at[color, i])
                wait_on(pair[color].at[:, pl.ds(FRONT + first, n)], pr_recv.at[color, i])
        bit = bits[color][0]
        for slot in ((1 - bit) * TILE, bit * TILE):
            add(color, slot, TILE, slot, p, p + AHEAD)
        reduce_send(color, 0, p)

    def reduce_piece(color, stage_no, p):
        s = stage_no - 1
        wait_on(landing(color, s, p), rs_recv.at[color, s, p])
        first, size, bit = reduce_base(color, stage_no, p), 4 >> s, halved(color, stage_no, p)
        for half in (1 - bit, bit):
            add(color, first + half * size, size, 16 - (16 >> s) + half * size, p, p)
        reduce_send(color, stage_no, p)

    def adam_piece(color, p):
        wait_on(landing(color, 3, p), rs_recv.at[color, 3, p])
        slot = base(color, 4)
        acc[color][reduce_base(color, 4, p), rows_at(p), :] += final[color][0, rows_at(p), :]
        adam(color, p)
        gather_send(color, 0, slot, 1, p)

    def gather_send(color, s, first, size, p):
        block = gat.at[color, c, pl.ds(first, size), rows_at(p)]
        pltpu.make_async_remote_copy(block, block, ag_send.at[color, s], ag_recv.at[color, s, p], device_id=routes[color][3 - s], device_id_type=MESH).start()

    def gather_piece(color, s, p):
        level, size = 4 - s, 1 << s
        arrived = base(color, level - 1) + (1 - bits[color][level - 1]) * size
        wait_on(gat.at[color, c, pl.ds(arrived, size), rows_at(p)], ag_recv.at[color, s, p])
        if s < 3:
            gather_send(color, s + 1, base(color, level - 1), 2 * size, p)
        if s > 1:
            pair_out(color, arrived if s == 3 else base(color, 1), TILE, p)

    load(0, (False,))

    @pl.loop(0, STEPS)
    def _(t):
        for i in range(2, len(LOAD)):
            pl.when(t == LOAD[i - 1][0] // GROUP)(functools.partial(load, i))
        for stage_no, color in SEQUENCE:
            p = t - LAGS[color][stage_no]

            @pl.when((p >= 0) & (p < PIECES))
            def _():
                if stage_no == 0:
                    start_pieces(color, p)
                elif stage_no < 4:
                    reduce_piece(color, stage_no, p)
                elif stage_no == 4:
                    adam_piece(color, p)
                else:
                    gather_piece(color, stage_no - 5, p)

        pl.when(t == 0)(functools.partial(load, 1))

        @pl.when(t == 1)
        def _():
            state_rows()

        @pl.when((t >= 2) & (t < 6))
        def _():
            state_rows_part(t - 2)

        @pl.when((t >= 6) & (t < FIRST_ADAM))
        def _():
            state_to_cover(t - 6)

        @pl.when((t > LAST_ADAM) & (t <= LAST_ADAM + 15))
        def _():
            cover_to_state(t - LAST_ADAM - 1)

    for color in COLORS:
        wait_on(gat.at[color, 1 - c], dag_recv.at[color])
        wait_on(gat.at[color, c], dag_send.at[color])
        wait_on(acc[color], pr_send.at[color])
        for s in range(4):
            wait_on(acc[color].at[pl.ds(0, TILE >> s)], rs_send.at[color, s])
            wait_on(gat.at[color, 0, pl.ds(0, 1 << s)], ag_send.at[color, s])


def place_kernel(gat, stage, e_out, a_out, f1_out, f2_out, b_out, m_out, v_out, w_out, chip_out, merged, loose, vec, tail, block, out_sem, edge_sem, state_sem, chip_sem):
    outs = (e_out, a_out, f1_out, f2_out, b_out)
    chip = (lax.axis_index('outer') * 2 + lax.axis_index('middle')) * 2 + lax.axis_index('inner') // 2
    started = [pltpu.make_async_copy(stage.at[i, pl.ds(MARGIN, SLICE_ROWS)], dst, state_sem.at[i]) for i, dst in enumerate((m_out, v_out, w_out))]

    def rows_from(d, at, n):
        color = at // HALF
        return gat.at[color, d % 2, slot_of(color, d // 2), pl.ds(at - color * HALF, n)]

    row = lax.broadcasted_iota(jnp.int32, (GROUP, LANES), 0)
    lane = lax.broadcasted_iota(jnp.int32, (GROUP, LANES), 1)
    tile_order = (row % TILE) * 4 + row // TILE
    count = 0
    for d in range(NDEV):
        first = merge_row(d)
        last = merge_row(d + 1) if d < LAST else STARTS[-1]
        begin = start_row(d)
        for color in COLORS:
            lo = max(first + (GROUP if d else 0), begin + color * HALF)
            for tensor, at, off, n in segments(lo, min(last, begin + (color + 1) * HALF) - lo):
                started.append(pltpu.make_async_copy(rows_from(d, lo + off - begin, n), outs[tensor].at[pl.ds(at, n)], out_sem.at[count]))
                count += 1
    for copy in started:
        copy.start()
    for d in range(1, NDEV):
        first = merge_row(d)
        flat = tile_order if PERM_LO <= first < PERM_HI else row
        keep = 2 * flat + lane // 64 >= SPAN * d - 2 * first
        new, old = (rows_from(e, first - start_row(e), GROUP)[...].astype(jnp.float32) for e in (d, d - 1))
        merged[d] = jnp.where(keep, new, old).astype(jnp.bfloat16)
        (tensor, at, _, _), = segments(first, GROUP)
        copy = pltpu.make_async_copy(merged.at[d], outs[tensor].at[pl.ds(at, GROUP)], edge_sem.at[d])
        copy.start()
        started.append(copy)

    def rows_of(group):
        d = (64 * group + 63) * INVERSE[0] >> INVERSE[1]
        begin = jnp.where(d == LAST, LAST_START, (SPAN * d >> 6) * GROUP)
        x, y, z0, z1 = ((d >> i) & 1 for i in range(1, 5))
        halves = []
        for h in COLORS:
            at = GROUP * group - begin + 16 * h
            color = (at >= HALF).astype(jnp.int32)
            slot = jnp.where(color == 0, x, y) * TILE + z0 * 4 + jnp.where(color == 0, y, x) * 2 + z1
            halves.append(gat[color, d & 1, slot, pl.ds(pl.multiple_of(at - color * HALF, 16), 16), :])
        return halves

    def put(at, rows):
        block[0:1, pl.ds(pl.multiple_of(at * LANES, BLOCK), BLOCK)] = rows.reshape(1, BLOCK).astype(jnp.bfloat16)
    def put_rows(at, halves):
        for h, half in enumerate(halves):
            rows = half.astype(jnp.float32)
            for q in COLORS:
                put(at + 16 * h + TILE * q, rows[TILE * q:TILE * q + TILE])

    def put_tiles(at, halves, t):
        for h, half in enumerate(halves):
            rows = half.astype(jnp.float32)
            for q in COLORS:
                loose[t, pl.ds(2 * h + q, TILE, stride=4), :] = rows[TILE * q:TILE * q + TILE]
        for q in range(4):
            put(at + TILE * q, loose[t, TILE * q:TILE * q + TILE, :])

    def put_edges(tensors):
        for d in range(1, NDEV):
            (tensor, at, _, _), = segments(merge_row(d), GROUP)
            if tensor not in tensors:
                continue
            layer, owner = divmod(at // GROUP, 16)

            @pl.when(chip == (owner if tensor else at // E_ROWS))
            def _():
                halves = (merged[d, 0:16, :], merged[d, 16:, :])
                if tensor in (1, 2):
                    put_tiles(1536 + 512 * tensor + GROUP * layer, halves, tensor - 1)
                else:
                    put_rows(3072 + GROUP * layer if tensor else at % E_ROWS, halves)

    @pl.loop(0, 64, unroll=4)
    def _(j):
        put_rows(GROUP * j, rows_of(chip * 64 + j))

    put_edges((0,))
    split = E_ROWS * LANES
    sends = [pltpu.make_async_copy(block.at[:, pl.ds(at, n)], chip_out.at[:, pl.ds(at, n)], chip_sem.at[i]) for i, (at, n) in enumerate(((0, split), (split, 2 * SLICE - split)))]
    sends[0].start()

    @pl.loop(0, 16, unroll=2)
    def _(layer):
        for t in (1, 2):
            put_tiles(1536 + 512 * t + GROUP * layer, rows_of(STARTS[t] // GROUP + layer * 16 + chip), t - 1)
        put_rows(3072 + GROUP * layer, rows_of(STARTS[3] // GROUP + layer * 16 + chip))

    put_edges((1, 2, 3))
    at = STARTS[4] - start_row(LAST)
    vec[0:208, :] = rows_from(LAST, at, 208)[...].astype(jnp.float32)
    vec[208:, :] = jnp.zeros((16, LANES), jnp.float32)
    tail[...] = jnp.zeros_like(tail)
    begin = (104 * chip) % LANES
    line = lax.broadcasted_iota(jnp.int32, (TILE, LANES), 1)
    for layer in range(16):
        source = layer // TILE * TILE * VEC_TILES + layer % TILE + (104 * chip) // LANES * TILE
        to = layer * 104 // LANES
        off = layer * 104 % LANES
        turn = (off - begin + LANES) % LANES
        one = pltpu.roll(vec[pl.ds(source, TILE), :], turn, 1)
        two = pltpu.roll(vec[pl.ds(source + TILE, TILE), :], turn, 1)
        t = (line - off + LANES) % LANES
        got = jnp.where(begin + t < LANES, one, two)
        here = (t < 104) & (line >= off)
        tail[to:to + 1, :] = jnp.where(here, got, tail[pl.ds(to, TILE), :])[0:1]
        if off + 104 > LANES:
            there = (t < 104) & (line < off)
            tail[to + 1:to + 2, :] = jnp.where(there, got, tail[pl.ds(to + 1, TILE), :])[0:1]
    put(3584, tail[0:TILE, :])
    block[0:1, 3592 * LANES:] = tail[TILE:16, :].reshape(1, BLOCK)[:, 0:640].astype(jnp.bfloat16)
    sends[1].start()
    for copy in started + sends:
        copy.wait()


def tile_rows(tensor, tiles=4):
    return tensor.reshape(-1, TILE, tiles, LANES).transpose(0, 2, 1, 3).reshape(-1, LANES)


def untile(rows, shape, tiles=4):
    return rows.reshape(-1, tiles, TILE, LANES).transpose(0, 2, 1, 3).reshape(shape)


def solution(mesh):
    def local_step(g_embed, g_attn, g_ffn_in, g_ffn_out, g_vec, m_shard, v_shard, w_shard):
        grads = (g_embed[0], tile_rows(g_attn[0]), tile_rows(g_ffn_in[0]), g_ffn_out[0].reshape(-1, LANES), tile_rows(g_vec[0], VEC_TILES))
        any_spec, vmem_spec = pl.BlockSpec(memory_space=pl.ANY), pl.BlockSpec(memory_space=pltpu.VMEM)
        f32, bf16 = jnp.float32, jnp.bfloat16
        flat = jax.ShapeDtypeStruct((SLICE_ROWS, LANES), f32)
        dma = pltpu.SemaphoreType.DMA
        gathered, stage = pl.pallas_call(
            big_kernel,
            out_shape=(pltpu.VMEM((2, 2, 16, HALF, LANES), bf16), pltpu.VMEM((3, SLICE_ROWS + 2 * MARGIN, LANES), f32)),
            in_specs=[any_spec] * 8,
            out_specs=[vmem_spec] * 2,
            scratch_shapes=[pltpu.VMEM((16, HALF, LANES), f32)] * 2 + [pltpu.VMEM((16, HALF + FRONT, LANES), f32)] * 2 + [pltpu.VMEM((1, HALF, LANES), f32)] * 2 + [pltpu.VMEM((SLICE,), f32)] * 3 + [pltpu.VMEM((3, COVER, LANES), f32)]
            + [dma((2, len(LOADS))), dma((2, len(LOADS))), dma((2,)), dma((2, 4, PIECES)), dma((2, 4)), dma((2, 4, PIECES)), dma((2, 4)), dma((2,)), dma((2,)), dma((3,))],
            compiler_params=pltpu.CompilerParams(collective_id=0, has_side_effects=True, vmem_limit_bytes=BIG_VMEM),
            name='reduce_adam_gather',
        )(*grads, m_shard, v_shard, w_shard)
        placed = pl.pallas_call(
            place_kernel,
            out_shape=[jax.ShapeDtypeStruct((n, LANES), bf16) for n in TENSOR_ROWS] + [flat] * 3 + [jax.ShapeDtypeStruct((1, 2 * SLICE), bf16)],
            in_specs=[vmem_spec] * 2,
            out_specs=[any_spec] * 9,
            scratch_shapes=[pltpu.VMEM((NDEV, GROUP, LANES), bf16), pltpu.VMEM((2, GROUP, LANES), f32), pltpu.VMEM((224, LANES), f32), pltpu.VMEM((24, LANES), f32), pltpu.VMEM((1, 2 * SLICE), bf16)]
            + [dma((2 * NDEV + TILE,)), dma((NDEV,)), dma((3,)), dma((2,))],
            compiler_params=pltpu.CompilerParams(vmem_limit_bytes=PLACE_VMEM),
            name='place',
        )(gathered, stage)
        e, a, f1, f2, b, *state, w_chip = placed
        tensors = (e, untile(a, (16, LANES, 512)), untile(f1, (16, LANES, 512)), f2.reshape(16, 512, LANES), untile(b, (16, 1664), VEC_TILES))
        return tuple(t.reshape(-1)[:SLICE] for t in state) + tensors + (w_chip,)

    return jax.shard_map(local_step, mesh=mesh, in_specs=(P(MESH_AXES),) * TILE, out_specs=(P(MESH_AXES),) * 3 + (P(),) * 5 + (P(MESH_AXES),), check_vma=False)
```

```python
import functools

import jax
import jax.numpy as jnp
from jax import lax
from jax.experimental import pallas as pl
from jax.experimental.pallas import tpu as pltpu
from jax.sharding import PartitionSpec as P

MESH_AXES = ('outer', 'middle', 'inner')
MESH = pl.DeviceIdType.MESH
BETA1, BETA2, EPS, RATE, STEP = 0.9, 0.98, 1e-9, 0.05, 3

NDEV = 32
GROUP = 32
LANES = 128
TILE = 8
BLOCK = 1024
LAST = NDEV - 1
LAST_START = 55696
SPAN = 3597
COLORS = (0, 1)
REST = 1792
ROWS = 1856
HALF = ROWS // 2
SLICE = 230208
SLICE_ROWS = 1800
MARGIN = 64
BIG_VMEM, PLACE_VMEM = 43 << 20, 8 << 20
COVER = ROWS + 8
TENSOR_ROWS = (32768, 8192, 8192, 8192, 208)
STARTS = (0, 32768, 40960, 49152, 57344, 57552)
VEC_TILES = 13
INVERSE = (9329, 25)
PERM_LO, PERM_HI = 32768, 49152
LOADS = (32, 64, 128, 256, 256, 192)
E_SLOTS = 9
E_ROWS = 2048
LATE = 23
AHEAD = 4
FRONT = AHEAD * 32


def bounds(sizes):
    out, at = [], 0
    for n in sizes:
        out.append((at, n))
        at += n
    return out


LOAD = bounds(LOADS)
PIECES = HALF // GROUP
LAGS = ((0, 3, 6, 8, 15, 21, 24, 29, 38), (0, 3, 7, 10, 16, 21, 25, 29, 42))
SEQUENCE = ((7, 0), (8, 1), (8, 0), (6, 1), (4, 1), (5, 0), (0, 0), (3, 1), (2, 0), (2, 1), (1, 0), (6, 0), (7, 1), (5, 1), (3, 0), (0, 1), (4, 0), (1, 1))
STEPS = PIECES + max(map(max, LAGS))
FIRST_ADAM = min(lags[4] for lags in LAGS)
LAST_ADAM = max(lags[4] for lags in LAGS) + PIECES - 1
MOVES = FIRST_ADAM - 6


def start_row(d):
    return LAST_START if d == LAST else 32 * (SPAN * d // 64)


def merge_row(d):
    return 32 * (SPAN * d // 64)


def segments(row, n):
    out = []
    for t in range(5):
        lo, hi = max(row, STARTS[t]), min(row + n, STARTS[t + 1])
        if lo < hi:
            out.append((t, lo - STARTS[t], lo - row, hi - lo))
    return out


def slot_of(color, k, late=False):
    x, y, z0, z1 = k % 2, k // 2 % 2, k // 4 % 2, k // 8
    first, third = (x, y) if color == 0 else (y, x)
    return first * 8 + (third * 4 + z0 * 2 if late else z0 * 4 + third * 2) + z1


def big_kernel(ge, ga, gf1, gf2, gb, m_in, v_in, w_in, gat, stage, acc_a, acc_b, pair_a, pair_b, last_a, last_b, line_m, line_v, line_w, cov, ld_sem, pr_recv, pr_send, rs_recv, rs_send, ag_recv, ag_send, dag_recv, dag_send, state_sem):
    grads = (ge, ga, gf1, gf2, gb)
    acc, pair, final = (acc_a, acc_b), (pair_a, pair_b), (last_a, last_b)
    z, y, inner = lax.axis_index('outer'), lax.axis_index('middle'), lax.axis_index('inner')
    x, c = inner // 2, inner % 2
    z0, z1 = z % 2, z // 2
    dev = (z * 2 + y) * 4 + inner
    to_pair = {'inner': inner + 1 - 2 * c}
    to_x = {'inner': inner + 2 - 4 * x}
    to_y = {'middle': 1 - y}
    to_z0 = {'outer': z + 1 - 2 * z0}
    to_z1 = {'outer': z + 2 - 4 * z1}
    routes = ((to_x, to_z0, to_y, to_z1), (to_y, to_z0, to_x, to_z1))
    bits = ((x, z0, y, z1), (y, z0, x, z1))

    barrier = pltpu.get_barrier_semaphore()
    for to in (to_pair, to_x, to_y, to_z0, to_z1):
        pl.semaphore_signal(barrier, inc=1, device_id=to, device_id_type=MESH)

    def load_one(color, i, tensor, row, slot, at, n, mine):
        src = grads[tensor].at[pl.ds(row, n)]
        if mine:
            pltpu.make_async_copy(src, acc[color].at[slot, pl.ds(at, n)], ld_sem.at[color, i]).start()
        else:
            pltpu.make_async_remote_copy(src, pair[color].at[slot, pl.ds(FRONT + at, n)], pr_send.at[color], pr_recv.at[color, i], device_id=to_pair, device_id_type=MESH).start()

    def load(i, sides=(True, False)):
        at, n = LOAD[i]
        for color in COLORS:
            @pl.loop(0, E_SLOTS)
            def _(k):
                slot = slot_of(color, k, at >= LATE * GROUP)
                for mine in sides:
                    d = 2 * k + (c if mine else 1 - c)
                    row = pl.multiple_of(GROUP * ((SPAN * d) // 64), GROUP) + color * HALF + at
                    load_one(color, i, 0, row, slot, at, n, mine)
            for core in COLORS:
                @pl.when(c == core)
                def _():
                    for k in range(E_SLOTS, NDEV // 2):
                        slot = slot_of(color, k, at >= LATE * GROUP)
                        for mine in sides:
                            d = 2 * k + (core if mine else 1 - core)
                            for tensor, row, off, rows in segments(start_row(d) + color * HALF + at, n):
                                load_one(color, i, tensor, row, slot, at + off, rows, mine)

    load(0, (True,))
    lines = (line_m, line_v, line_w)
    state_in = [pltpu.make_async_copy(src, lines[i], state_sem.at[i]) for i, src in enumerate((m_in, v_in, w_in))]
    for copy in state_in:
        copy.start()
    pl.semaphore_wait(barrier, 5)

    def wait_on(ref, sem):
        pltpu.make_async_copy(ref, ref, sem).wait()

    def rows_at(p):
        return pl.ds(pl.multiple_of(p * GROUP, GROUP), GROUP)

    def rows_at(p):
        return pl.ds(pl.multiple_of(p * GROUP, GROUP), GROUP)

    def add(color, into, slots, first, p, block):
        acc[color][pl.ds(into, slots), rows_at(p), :] += pair[color][pl.ds(first, slots), rows_at(block), :]

    def landing(color, s, p):
        if s == 3:
            return final[color].at[:, rows_at(p)]
        return pair[color].at[pl.ds(16 - (16 >> s), TILE >> s), rows_at(p)]

    def base(color, level):
        return sum((bits[color][i] * (TILE >> i) for i in range(level)), 0 * c)

    def halved(color, level, p):
        one, other = bits[color][level], bits[color][3 - level if level in (1, 2) else level]
        return jnp.where(p >= LATE, other, one)

    def reduce_base(color, level, p):
        return sum((halved(color, i, p) * (TILE >> i) for i in range(level)), 0 * c)

    def reduce_to(color, s, p):
        if s in (0, 3):
            return routes[color][s]
        along_z = p < LATE if s == 1 else p >= LATE
        across_y = jnp.logical_not(along_z) & (color == 0)
        across_x = jnp.logical_not(along_z) & (color == 1)
        return {'outer': jnp.where(along_z, to_z0['outer'], z), 'middle': jnp.where(across_y, 1 - y, y), 'inner': jnp.where(across_x, to_x['inner'], inner)}

    def reduce_send(color, s, p):
        size = TILE >> s
        first = reduce_base(color, s, p) + (1 - halved(color, s, p)) * size
        pltpu.make_async_remote_copy(acc[color].at[pl.ds(first, size), rows_at(p)], landing(color, s, p), rs_send.at[color, s], rs_recv.at[color, s, p], device_id=reduce_to(color, s, p), device_id_type=MESH).start()

    def pair_out(color, slot, size, p):
        block = gat.at[color, c, pl.ds(slot, size), rows_at(p)]
        pltpu.make_async_remote_copy(block, block, dag_send.at[color], dag_recv.at[color], device_id=to_pair, device_id_type=MESH).start()

    def adam_block(g, load_state, store_state):
        g = g * (1.0 / NDEV)
        m = BETA1 * load_state(0) + (1.0 - BETA1) * g
        v = BETA2 * load_state(1) + (1.0 - BETA2) * (g * g)
        m_hat = m / (1.0 - BETA1 ** STEP)
        v_hat = v / (1.0 - BETA2 ** STEP)
        w = load_state(2) - RATE * m_hat / (jnp.sqrt(v_hat) + EPS)
        store_state(0, m)
        store_state(1, v)
        store_state(2, w)
        return w

    cover_start = jnp.where(dev == LAST, LAST_START, GROUP * ((SPAN * dev) // 64))

    def adam(color, p):
        slot, summed = base(color, 4), reduce_base(color, 4, p)
        r = pl.multiple_of(p * GROUP, GROUP)
        f = pl.multiple_of(color * HALF + r, GROUP)
        row = cover_start + f
        permuted = (row >= PERM_LO) & (row < PERM_HI)
        vectors = row + GROUP > STARTS[4]

        def tiles(t, index):
            parts = []
            for q in (2 * t, 2 * t + 1):
                where = index(q)

                def keep(i, value, where=where):
                    cov[i, where, :] = value

                parts.append(adam_block(acc[color][summed, pl.ds(r + TILE * q, TILE), :], lambda i, where=where: cov[i, where, :], keep))
            gat[color, c, slot, pl.ds(r + 16 * t, 16), :] = jnp.concatenate(parts, axis=0).astype(jnp.bfloat16)

        def plain(q):
            return pl.ds(f + TILE * q, TILE)

        def vector_tile(q):
            tile = (row + TILE * q - STARTS[4]) // TILE
            return pl.ds(STARTS[4] - LAST_START + tile // VEC_TILES * VEC_TILES * TILE + tile % VEC_TILES, TILE, stride=VEC_TILES)

        @pl.when(permuted)
        def _():
            for t in COLORS:
                tiles(t, lambda q: pl.ds(f + q, TILE, stride=4))

        @pl.when(jnp.logical_not(permuted | vectors))
        def _():
            for t in COLORS:
                tiles(t, plain)

        @pl.when(vectors)
        def _():
            for t in COLORS:
                inside = row + 16 * t >= STARTS[4]
                pl.when(inside)(functools.partial(tiles, t, vector_tile))
                pl.when(jnp.logical_not(inside))(functools.partial(tiles, t, plain))

    half_rows = jnp.where(dev == LAST, 115, (SPAN * dev) % 64)
    shift = half_rows // 2
    lane = lax.broadcasted_iota(jnp.int32, (GROUP, LANES), 1)

    def moved(first, second):
        return jnp.where(lane < 64, pltpu.roll(first, 64, 1), pltpu.roll(second, 64, 1))

    def state_rows():
        for i, copy in enumerate(state_in):
            copy.wait()
            stage[i, 0:MARGIN, :] = jnp.zeros((MARGIN, LANES), jnp.float32)
            stage[i, MARGIN + SLICE_ROWS - TILE:, :] = jnp.zeros((MARGIN + TILE, LANES), jnp.float32)
            cov[i, ROWS:, :] = jnp.zeros((COVER - ROWS, LANES), jnp.float32)
            for r in range(REST, 1798):
                stage[i, MARGIN + r:MARGIN + r + 1, :] = lines[i][LANES * r:LANES * r + LANES].reshape(1, LANES)
            stage[i, MARGIN + 1798:MARGIN + 1799, 0:64] = lines[i][SLICE - 64:].reshape(1, 64)

    def state_rows_part(t):
        @pl.loop(0, 56)
        def _(k):
            j = t * 56 + k
            for i in range(3):
                stage[i, pl.ds(pl.multiple_of(MARGIN + j * TILE, TILE), TILE), :] = lines[i][pl.ds(pl.multiple_of(j * BLOCK, BLOCK), BLOCK)].reshape(TILE, LANES)

    def state_to_cover(t):
        @pl.loop(0, -(-ROWS // GROUP // MOVES))
        def _(k):
            f = pl.multiple_of(jnp.minimum((t + k * MOVES) * GROUP, ROWS - GROUP), GROUP)
            r = MARGIN + f - shift
            for i in range(3):
                here = stage[i, pl.ds(r, GROUP), :]
                before = stage[i, pl.ds(r - 1, GROUP), :]
                cov[i, pl.ds(f, GROUP), :] = jnp.where(c == 1, moved(before, here), here)

    def cover_to_state(t):
        @pl.loop(0, 15)
        def _(k):
            r = pl.multiple_of((t * 15 + k) * TILE, TILE)
            for i in range(3):
                here = cov[i, pl.ds(r + shift, TILE), :]
                after = cov[i, pl.ds(r + shift + 1, TILE), :]
                both = jnp.where(lane[:TILE] < 64, pltpu.roll(here, 64, 1), pltpu.roll(after, 64, 1))
                stage[i, pl.ds(pl.multiple_of(MARGIN + r, TILE), TILE), :] = jnp.where(c == 1, both, here)

    def state_out():
        for i, dst in enumerate((m_out, v_out, w_out)):
            pltpu.make_async_copy(stage.at[i, pl.ds(MARGIN, SLICE_ROWS)], dst, state_sem.at[i]).start()

    def start_pieces(color, p):
        for i, (first, n) in enumerate(LOAD):
            @pl.when(p == first // GROUP)
            def _():
                wait_on(acc[color].at[:, pl.ds(first, n)], ld_sem.at[color, i])
                wait_on(pair[color].at[:, pl.ds(FRONT + first, n)], pr_recv.at[color, i])
        bit = bits[color][0]
        for slot in ((1 - bit) * TILE, bit * TILE):
            add(color, slot, TILE, slot, p, p + AHEAD)
        reduce_send(color, 0, p)

    def reduce_piece(color, stage_no, p):
        s = stage_no - 1
        wait_on(landing(color, s, p), rs_recv.at[color, s, p])
        first, size, bit = reduce_base(color, stage_no, p), 4 >> s, halved(color, stage_no, p)
        for half in (1 - bit, bit):
            add(color, first + half * size, size, 16 - (16 >> s) + half * size, p, p)
        reduce_send(color, stage_no, p)

    def adam_piece(color, p):
        wait_on(landing(color, 3, p), rs_recv.at[color, 3, p])
        slot = base(color, 4)
        acc[color][reduce_base(color, 4, p), rows_at(p), :] += final[color][0, rows_at(p), :]
        adam(color, p)
        gather_send(color, 0, slot, 1, p)

    def gather_send(color, s, first, size, p):
        block = gat.at[color, c, pl.ds(first, size), rows_at(p)]
        pltpu.make_async_remote_copy(block, block, ag_send.at[color, s], ag_recv.at[color, s, p], device_id=routes[color][3 - s], device_id_type=MESH).start()

    def gather_piece(color, s, p):
        level, size = 4 - s, 1 << s
        arrived = base(color, level - 1) + (1 - bits[color][level - 1]) * size
        wait_on(gat.at[color, c, pl.ds(arrived, size), rows_at(p)], ag_recv.at[color, s, p])
        if s < 3:
            gather_send(color, s + 1, base(color, level - 1), 2 * size, p)
        if s > 1:
            pair_out(color, arrived if s == 3 else base(color, 1), TILE, p)

    load(0, (False,))

    @pl.loop(0, STEPS)
    def _(t):
        for i in range(2, len(LOAD)):
            pl.when(t == LOAD[i - 1][0] // GROUP)(functools.partial(load, i))
        for stage_no, color in SEQUENCE:
            p = t - LAGS[color][stage_no]

            @pl.when((p >= 0) & (p < PIECES))
            def _():
                if stage_no == 0:
                    start_pieces(color, p)
                elif stage_no < 4:
                    reduce_piece(color, stage_no, p)
                elif stage_no == 4:
                    adam_piece(color, p)
                else:
                    gather_piece(color, stage_no - 5, p)

        pl.when(t == 0)(functools.partial(load, 1))

        @pl.when(t == 1)
        def _():
            state_rows()

        @pl.when((t >= 2) & (t < 6))
        def _():
            state_rows_part(t - 2)

        @pl.when((t >= 6) & (t < FIRST_ADAM))
        def _():
            state_to_cover(t - 6)

        @pl.when((t > LAST_ADAM) & (t <= LAST_ADAM + 15))
        def _():
            cover_to_state(t - LAST_ADAM - 1)

    for color in COLORS:
        wait_on(gat.at[color, 1 - c], dag_recv.at[color])
        wait_on(gat.at[color, c], dag_send.at[color])
        wait_on(acc[color], pr_send.at[color])
        for s in range(4):
            wait_on(acc[color].at[pl.ds(0, TILE >> s)], rs_send.at[color, s])
            wait_on(gat.at[color, 0, pl.ds(0, 1 << s)], ag_send.at[color, s])


def place_kernel(gat, stage, e_out, a_out, f1_out, f2_out, b_out, m_out, v_out, w_out, chip_out, merged, loose, vec, tail, block, out_sem, edge_sem, state_sem, chip_sem):
    outs = (e_out, a_out, f1_out, f2_out, b_out)
    chip = (lax.axis_index('outer') * 2 + lax.axis_index('middle')) * 2 + lax.axis_index('inner') // 2
    started = [pltpu.make_async_copy(stage.at[i, pl.ds(MARGIN, SLICE_ROWS)], dst, state_sem.at[i]) for i, dst in enumerate((m_out, v_out, w_out))]

    def rows_from(d, at, n):
        color = at // HALF
        return gat.at[color, d % 2, slot_of(color, d // 2), pl.ds(at - color * HALF, n)]

    row = lax.broadcasted_iota(jnp.int32, (GROUP, LANES), 0)
    lane = lax.broadcasted_iota(jnp.int32, (GROUP, LANES), 1)
    tile_order = (row % TILE) * 4 + row // TILE
    count = 0
    for d in range(NDEV):
        first = merge_row(d)
        last = merge_row(d + 1) if d < LAST else STARTS[-1]
        begin = start_row(d)
        for color in COLORS:
            lo = max(first + (GROUP if d else 0), begin + color * HALF)
            for tensor, at, off, n in segments(lo, min(last, begin + (color + 1) * HALF) - lo):
                started.append(pltpu.make_async_copy(rows_from(d, lo + off - begin, n), outs[tensor].at[pl.ds(at, n)], out_sem.at[count]))
                count += 1
    for copy in started:
        copy.start()
    for d in range(1, NDEV):
        first = merge_row(d)
        flat = tile_order if PERM_LO <= first < PERM_HI else row
        keep = 2 * flat + lane // 64 >= SPAN * d - 2 * first
        new, old = (rows_from(e, first - start_row(e), GROUP)[...].astype(jnp.float32) for e in (d, d - 1))
        merged[d] = jnp.where(keep, new, old).astype(jnp.bfloat16)
        (tensor, at, _, _), = segments(first, GROUP)
        copy = pltpu.make_async_copy(merged.at[d], outs[tensor].at[pl.ds(at, GROUP)], edge_sem.at[d])
        copy.start()
        started.append(copy)

    def rows_of(group):
        d = (64 * group + 63) * INVERSE[0] >> INVERSE[1]
        begin = jnp.where(d == LAST, LAST_START, (SPAN * d >> 6) * GROUP)
        x, y, z0, z1 = ((d >> i) & 1 for i in range(1, 5))
        halves = []
        for h in COLORS:
            at = GROUP * group - begin + 16 * h
            color = (at >= HALF).astype(jnp.int32)
            slot = jnp.where(color == 0, x, y) * TILE + z0 * 4 + jnp.where(color == 0, y, x) * 2 + z1
            halves.append(gat[color, d & 1, slot, pl.ds(pl.multiple_of(at - color * HALF, 16), 16), :])
        return halves

    def put(at, rows):
        block[0:1, pl.ds(pl.multiple_of(at * LANES, BLOCK), BLOCK)] = rows.reshape(1, BLOCK).astype(jnp.bfloat16)
    def put_rows(at, halves):
        for h, half in enumerate(halves):
            rows = half.astype(jnp.float32)
            for q in COLORS:
                put(at + 16 * h + TILE * q, rows[TILE * q:TILE * q + TILE])

    def put_tiles(at, halves, t):
        for h, half in enumerate(halves):
            rows = half.astype(jnp.float32)
            for q in COLORS:
                loose[t, pl.ds(2 * h + q, TILE, stride=4), :] = rows[TILE * q:TILE * q + TILE]
        for q in range(4):
            put(at + TILE * q, loose[t, TILE * q:TILE * q + TILE, :])

    def put_edges(tensors):
        for d in range(1, NDEV):
            (tensor, at, _, _), = segments(merge_row(d), GROUP)
            if tensor not in tensors:
                continue
            layer, owner = divmod(at // GROUP, 16)

            @pl.when(chip == (owner if tensor else at // E_ROWS))
            def _():
                halves = (merged[d, 0:16, :], merged[d, 16:, :])
                if tensor in (1, 2):
                    put_tiles(1536 + 512 * tensor + GROUP * layer, halves, tensor - 1)
                else:
                    put_rows(3072 + GROUP * layer if tensor else at % E_ROWS, halves)

    @pl.loop(0, 64, unroll=4)
    def _(j):
        put_rows(GROUP * j, rows_of(chip * 64 + j))

    put_edges((0,))
    split = E_ROWS * LANES
    sends = [pltpu.make_async_copy(block.at[:, pl.ds(at, n)], chip_out.at[:, pl.ds(at, n)], chip_sem.at[i]) for i, (at, n) in enumerate(((0, split), (split, 2 * SLICE - split)))]
    sends[0].start()

    @pl.loop(0, 16, unroll=2)
    def _(layer):
        for t in (1, 2):
            put_tiles(1536 + 512 * t + GROUP * layer, rows_of(STARTS[t] // GROUP + layer * 16 + chip), t - 1)
        put_rows(3072 + GROUP * layer, rows_of(STARTS[3] // GROUP + layer * 16 + chip))

    put_edges((1, 2, 3))
    at = STARTS[4] - start_row(LAST)
    vec[0:208, :] = rows_from(LAST, at, 208)[...].astype(jnp.float32)
    vec[208:, :] = jnp.zeros((16, LANES), jnp.float32)
    tail[...] = jnp.zeros_like(tail)
    begin = (104 * chip) % LANES
    line = lax.broadcasted_iota(jnp.int32, (TILE, LANES), 1)
    for layer in range(16):
        source = layer // TILE * TILE * VEC_TILES + layer % TILE + (104 * chip) // LANES * TILE
        to = layer * 104 // LANES
        off = layer * 104 % LANES
        turn = (off - begin + LANES) % LANES
        one = pltpu.roll(vec[pl.ds(source, TILE), :], turn, 1)
        two = pltpu.roll(vec[pl.ds(source + TILE, TILE), :], turn, 1)
        t = (line - off + LANES) % LANES
        got = jnp.where(begin + t < LANES, one, two)
        here = (t < 104) & (line >= off)
        tail[to:to + 1, :] = jnp.where(here, got, tail[pl.ds(to, TILE), :])[0:1]
        if off + 104 > LANES:
            there = (t < 104) & (line < off)
            tail[to + 1:to + 2, :] = jnp.where(there, got, tail[pl.ds(to + 1, TILE), :])[0:1]
    put(3584, tail[0:TILE, :])
    block[0:1, 3592 * LANES:] = tail[TILE:16, :].reshape(1, BLOCK)[:, 0:640].astype(jnp.bfloat16)
    sends[1].start()
    for copy in started + sends:
        copy.wait()


def tile_rows(tensor, tiles=4):
    return tensor.reshape(-1, TILE, tiles, LANES).transpose(0, 2, 1, 3).reshape(-1, LANES)


def untile(rows, shape, tiles=4):
    return rows.reshape(-1, tiles, TILE, LANES).transpose(0, 2, 1, 3).reshape(shape)


def solution(mesh):
    def local_step(g_embed, g_attn, g_ffn_in, g_ffn_out, g_vec, m_shard, v_shard, w_shard):
        grads = (g_embed[0], tile_rows(g_attn[0]), tile_rows(g_ffn_in[0]), g_ffn_out[0].reshape(-1, LANES), tile_rows(g_vec[0], VEC_TILES))
        any_spec, vmem_spec = pl.BlockSpec(memory_space=pl.ANY), pl.BlockSpec(memory_space=pltpu.VMEM)
        f32, bf16 = jnp.float32, jnp.bfloat16
        flat = jax.ShapeDtypeStruct((SLICE_ROWS, LANES), f32)
        dma = pltpu.SemaphoreType.DMA
        gathered, stage = pl.pallas_call(
            big_kernel,
            out_shape=(pltpu.VMEM((2, 2, 16, HALF, LANES), bf16), pltpu.VMEM((3, SLICE_ROWS + 2 * MARGIN, LANES), f32)),
            in_specs=[any_spec] * 8,
            out_specs=[vmem_spec] * 2,
            scratch_shapes=[pltpu.VMEM((16, HALF, LANES), f32)] * 2 + [pltpu.VMEM((16, HALF + FRONT, LANES), f32)] * 2 + [pltpu.VMEM((1, HALF, LANES), f32)] * 2 + [pltpu.VMEM((SLICE,), f32)] * 3 + [pltpu.VMEM((3, COVER, LANES), f32)]
            + [dma((2, len(LOADS))), dma((2, len(LOADS))), dma((2,)), dma((2, 4, PIECES)), dma((2, 4)), dma((2, 4, PIECES)), dma((2, 4)), dma((2,)), dma((2,)), dma((3,))],
            compiler_params=pltpu.CompilerParams(collective_id=0, has_side_effects=True, vmem_limit_bytes=BIG_VMEM),
            name='reduce_adam_gather',
        )(*grads, m_shard, v_shard, w_shard)
        placed = pl.pallas_call(
            place_kernel,
            out_shape=[jax.ShapeDtypeStruct((n, LANES), bf16) for n in TENSOR_ROWS] + [flat] * 3 + [jax.ShapeDtypeStruct((1, 2 * SLICE), bf16)],
            in_specs=[vmem_spec] * 2,
            out_specs=[any_spec] * 9,
            scratch_shapes=[pltpu.VMEM((NDEV, GROUP, LANES), bf16), pltpu.VMEM((2, GROUP, LANES), f32), pltpu.VMEM((224, LANES), f32), pltpu.VMEM((24, LANES), f32), pltpu.VMEM((1, 2 * SLICE), bf16)]
            + [dma((2 * NDEV + TILE,)), dma((NDEV,)), dma((3,)), dma((2,))],
            compiler_params=pltpu.CompilerParams(vmem_limit_bytes=PLACE_VMEM),
            name='place',
        )(gathered, stage)
        e, a, f1, f2, b, *state, w_chip = placed
        tensors = (e, untile(a, (16, LANES, 512)), untile(f1, (16, LANES, 512)), f2.reshape(16, 512, LANES), untile(b, (16, 1664), VEC_TILES))
        return tuple(t.reshape(-1)[:SLICE] for t in state) + tensors + (w_chip,)

    return jax.shard_map(local_step, mesh=mesh, in_specs=(P(MESH_AXES),) * TILE, out_specs=(P(MESH_AXES),) * 3 + (P(),) * 5 + (P(MESH_AXES),), check_vma=False)
```

```python
import functools

import jax
import jax.numpy as jnp
from jax import lax
from jax.experimental import pallas as pl
from jax.experimental.pallas import tpu as pltpu
from jax.sharding import PartitionSpec as P

MESH_AXES = ('outer', 'middle', 'inner')
MESH = pl.DeviceIdType.MESH
BETA1, BETA2, EPS, RATE, STEP = 0.9, 0.98, 1e-9, 0.05, 3

NDEV = 32
GROUP = 32
LANES = 128
TILE = 8
BLOCK = 1024
LAST = NDEV - 1
LAST_START = 55696
SPAN = 3597
COLORS = (0, 1)
REST = 1792
ROWS = 1856
HALF = ROWS // 2
SLICE = 230208
SLICE_ROWS = 1800
MARGIN = 64
BIG_VMEM, PLACE_VMEM = 43 << 20, 8 << 20
COVER = ROWS + 8
TENSOR_ROWS = (32768, 8192, 8192, 8192, 208)
STARTS = (0, 32768, 40960, 49152, 57344, 57552)
VEC_TILES = 13
INVERSE = (9329, 25)
PERM_LO, PERM_HI = 32768, 49152
LOADS = (32, 64, 128, 256, 256, 192)
E_SLOTS = 9
E_ROWS = 2048
LATE = 23
AHEAD = 4
FRONT = AHEAD * 32


def bounds(sizes):
    out, at = [], 0
    for n in sizes:
        out.append((at, n))
        at += n
    return out


LOAD = bounds(LOADS)
PIECES = HALF // GROUP
LAGS = ((0, 2, 5, 8, 14, 20, 23, 27, 33), (0, 2, 5, 7, 14, 19, 22, 27, 33))
SEQUENCE = ((4, 1), (6, 0), (5, 0), (3, 0), (0, 0), (5, 1), (0, 1), (2, 1), (6, 1), (2, 0), (1, 0), (7, 1), (4, 0), (3, 1), (1, 1), (8, 0), (8, 1), (7, 0))
STEPS = PIECES + max(map(max, LAGS))
FIRST_ADAM = min(lags[4] for lags in LAGS)
LAST_ADAM = max(lags[4] for lags in LAGS) + PIECES - 1
MOVES = FIRST_ADAM - 6


def start_row(d):
    return LAST_START if d == LAST else 32 * (SPAN * d // 64)


def merge_row(d):
    return 32 * (SPAN * d // 64)


def segments(row, n):
    out = []
    for t in range(5):
        lo, hi = max(row, STARTS[t]), min(row + n, STARTS[t + 1])
        if lo < hi:
            out.append((t, lo - STARTS[t], lo - row, hi - lo))
    return out


def slot_of(color, k, late=False):
    x, y, z0, z1 = k % 2, k // 2 % 2, k // 4 % 2, k // 8
    first, third = (x, y) if color == 0 else (y, x)
    return first * 8 + (third * 4 + z0 * 2 if late else z0 * 4 + third * 2) + z1


def big_kernel(ge, ga, gf1, gf2, gb, m_in, v_in, w_in, gat, stage, acc_a, acc_b, pair_a, pair_b, last_a, last_b, line_m, line_v, line_w, cov, ld_sem, pr_recv, pr_send, rs_recv, rs_send, ag_recv, ag_send, dag_recv, dag_send, state_sem):
    grads = (ge, ga, gf1, gf2, gb)
    acc, pair, final = (acc_a, acc_b), (pair_a, pair_b), (last_a, last_b)
    z, y, inner = lax.axis_index('outer'), lax.axis_index('middle'), lax.axis_index('inner')
    x, c = inner // 2, inner % 2
    z0, z1 = z % 2, z // 2
    dev = (z * 2 + y) * 4 + inner
    to_pair = {'inner': inner + 1 - 2 * c}
    to_x = {'inner': inner + 2 - 4 * x}
    to_y = {'middle': 1 - y}
    to_z0 = {'outer': z + 1 - 2 * z0}
    to_z1 = {'outer': z + 2 - 4 * z1}
    routes = ((to_x, to_z0, to_y, to_z1), (to_y, to_z0, to_x, to_z1))
    bits = ((x, z0, y, z1), (y, z0, x, z1))

    barrier = pltpu.get_barrier_semaphore()
    for to in (to_pair, to_x, to_y, to_z0, to_z1):
        pl.semaphore_signal(barrier, inc=1, device_id=to, device_id_type=MESH)

    def load_one(color, i, tensor, row, slot, at, n, mine):
        src = grads[tensor].at[pl.ds(row, n)]
        if mine:
            pltpu.make_async_copy(src, acc[color].at[slot, pl.ds(at, n)], ld_sem.at[color, i]).start()
        else:
            pltpu.make_async_remote_copy(src, pair[color].at[slot, pl.ds(FRONT + at, n)], pr_send.at[color], pr_recv.at[color, i], device_id=to_pair, device_id_type=MESH).start()

    def load(i, sides=(True, False)):
        at, n = LOAD[i]
        for color in COLORS:
            @pl.loop(0, E_SLOTS)
            def _(k):
                slot = slot_of(color, k, at >= LATE * GROUP)
                for mine in sides:
                    d = 2 * k + (c if mine else 1 - c)
                    row = pl.multiple_of(GROUP * ((SPAN * d) // 64), GROUP) + color * HALF + at
                    load_one(color, i, 0, row, slot, at, n, mine)
            for core in COLORS:
                @pl.when(c == core)
                def _():
                    for k in range(E_SLOTS, NDEV // 2):
                        slot = slot_of(color, k, at >= LATE * GROUP)
                        for mine in sides:
                            d = 2 * k + (core if mine else 1 - core)
                            for tensor, row, off, rows in segments(start_row(d) + color * HALF + at, n):
                                load_one(color, i, tensor, row, slot, at + off, rows, mine)

    load(0, (True,))
    lines = (line_m, line_v, line_w)
    state_in = [pltpu.make_async_copy(src, lines[i], state_sem.at[i]) for i, src in enumerate((m_in, v_in, w_in))]
    for copy in state_in:
        copy.start()
    pl.semaphore_wait(barrier, 5)

    def wait_on(ref, sem):
        pltpu.make_async_copy(ref, ref, sem).wait()

    def rows_at(p):
        return pl.ds(pl.multiple_of(p * GROUP, GROUP), GROUP)

    def rows_at(p):
        return pl.ds(pl.multiple_of(p * GROUP, GROUP), GROUP)

    def add(color, into, slots, first, p, block):
        acc[color][pl.ds(into, slots), rows_at(p), :] += pair[color][pl.ds(first, slots), rows_at(block), :]

    def landing(color, s, p):
        if s == 3:
            return final[color].at[:, rows_at(p)]
        return pair[color].at[pl.ds(16 - (16 >> s), TILE >> s), rows_at(p)]

    def base(color, level):
        return sum((bits[color][i] * (TILE >> i) for i in range(level)), 0 * c)

    def halved(color, level, p):
        one, other = bits[color][level], bits[color][3 - level if level in (1, 2) else level]
        return jnp.where(p >= LATE, other, one)

    def reduce_base(color, level, p):
        return sum((halved(color, i, p) * (TILE >> i) for i in range(level)), 0 * c)

    def reduce_to(color, s, p):
        if s in (0, 3):
            return routes[color][s]
        along_z = p < LATE if s == 1 else p >= LATE
        across_y = jnp.logical_not(along_z) & (color == 0)
        across_x = jnp.logical_not(along_z) & (color == 1)
        return {'outer': jnp.where(along_z, to_z0['outer'], z), 'middle': jnp.where(across_y, 1 - y, y), 'inner': jnp.where(across_x, to_x['inner'], inner)}

    def reduce_send(color, s, p):
        size = TILE >> s
        first = reduce_base(color, s, p) + (1 - halved(color, s, p)) * size
        pltpu.make_async_remote_copy(acc[color].at[pl.ds(first, size), rows_at(p)], landing(color, s, p), rs_send.at[color, s], rs_recv.at[color, s, p], device_id=reduce_to(color, s, p), device_id_type=MESH).start()

    def pair_out(color, slot, size, p):
        block = gat.at[color, c, pl.ds(slot, size), rows_at(p)]
        pltpu.make_async_remote_copy(block, block, dag_send.at[color], dag_recv.at[color], device_id=to_pair, device_id_type=MESH).start()

    def adam_block(g, load_state, store_state):
        g = g * (1.0 / NDEV)
        m = BETA1 * load_state(0) + (1.0 - BETA1) * g
        v = BETA2 * load_state(1) + (1.0 - BETA2) * (g * g)
        m_hat = m / (1.0 - BETA1 ** STEP)
        v_hat = v / (1.0 - BETA2 ** STEP)
        w = load_state(2) - RATE * m_hat / (jnp.sqrt(v_hat) + EPS)
        store_state(0, m)
        store_state(1, v)
        store_state(2, w)
        return w

    cover_start = jnp.where(dev == LAST, LAST_START, GROUP * ((SPAN * dev) // 64))

    def adam(color, p):
        slot, summed = base(color, 4), reduce_base(color, 4, p)
        r = pl.multiple_of(p * GROUP, GROUP)
        f = pl.multiple_of(color * HALF + r, GROUP)
        row = cover_start + f
        permuted = (row >= PERM_LO) & (row < PERM_HI)
        vectors = row + GROUP > STARTS[4]

        def tiles(t, index):
            parts = []
            for q in (2 * t, 2 * t + 1):
                where = index(q)

                def keep(i, value, where=where):
                    cov[i, where, :] = value

                parts.append(adam_block(acc[color][summed, pl.ds(r + TILE * q, TILE), :], lambda i, where=where: cov[i, where, :], keep))
            gat[color, c, slot, pl.ds(r + 16 * t, 16), :] = jnp.concatenate(parts, axis=0).astype(jnp.bfloat16)

        def plain(q):
            return pl.ds(f + TILE * q, TILE)

        def vector_tile(q):
            tile = (row + TILE * q - STARTS[4]) // TILE
            return pl.ds(STARTS[4] - LAST_START + tile // VEC_TILES * VEC_TILES * TILE + tile % VEC_TILES, TILE, stride=VEC_TILES)

        @pl.when(permuted)
        def _():
            for t in COLORS:
                tiles(t, lambda q: pl.ds(f + q, TILE, stride=4))

        @pl.when(jnp.logical_not(permuted | vectors))
        def _():
            for t in COLORS:
                tiles(t, plain)

        @pl.when(vectors)
        def _():
            for t in COLORS:
                inside = row + 16 * t >= STARTS[4]
                pl.when(inside)(functools.partial(tiles, t, vector_tile))
                pl.when(jnp.logical_not(inside))(functools.partial(tiles, t, plain))

    half_rows = jnp.where(dev == LAST, 115, (SPAN * dev) % 64)
    shift = half_rows // 2
    lane = lax.broadcasted_iota(jnp.int32, (GROUP, LANES), 1)

    def moved(first, second):
        return jnp.where(lane < 64, pltpu.roll(first, 64, 1), pltpu.roll(second, 64, 1))

    def state_rows():
        for i, copy in enumerate(state_in):
            copy.wait()
            stage[i, 0:MARGIN, :] = jnp.zeros((MARGIN, LANES), jnp.float32)
            stage[i, MARGIN + SLICE_ROWS - TILE:, :] = jnp.zeros((MARGIN + TILE, LANES), jnp.float32)
            cov[i, ROWS:, :] = jnp.zeros((COVER - ROWS, LANES), jnp.float32)
            for r in range(REST, 1798):
                stage[i, MARGIN + r:MARGIN + r + 1, :] = lines[i][LANES * r:LANES * r + LANES].reshape(1, LANES)
            stage[i, MARGIN + 1798:MARGIN + 1799, 0:64] = lines[i][SLICE - 64:].reshape(1, 64)

    def state_rows_part(t):
        @pl.loop(0, 56)
        def _(k):
            j = t * 56 + k
            for i in range(3):
                stage[i, pl.ds(pl.multiple_of(MARGIN + j * TILE, TILE), TILE), :] = lines[i][pl.ds(pl.multiple_of(j * BLOCK, BLOCK), BLOCK)].reshape(TILE, LANES)

    def state_to_cover(t):
        @pl.loop(0, -(-ROWS // GROUP // MOVES))
        def _(k):
            f = pl.multiple_of(jnp.minimum((t + k * MOVES) * GROUP, ROWS - GROUP), GROUP)
            r = MARGIN + f - shift
            for i in range(3):
                here = stage[i, pl.ds(r, GROUP), :]
                before = stage[i, pl.ds(r - 1, GROUP), :]
                cov[i, pl.ds(f, GROUP), :] = jnp.where(c == 1, moved(before, here), here)

    def cover_to_state(t):
        @pl.loop(0, 15)
        def _(k):
            r = pl.multiple_of((t * 15 + k) * TILE, TILE)
            for i in range(3):
                here = cov[i, pl.ds(r + shift, TILE), :]
                after = cov[i, pl.ds(r + shift + 1, TILE), :]
                both = jnp.where(lane[:TILE] < 64, pltpu.roll(here, 64, 1), pltpu.roll(after, 64, 1))
                stage[i, pl.ds(pl.multiple_of(MARGIN + r, TILE), TILE), :] = jnp.where(c == 1, both, here)

    def state_out():
        for i, dst in enumerate((m_out, v_out, w_out)):
            pltpu.make_async_copy(stage.at[i, pl.ds(MARGIN, SLICE_ROWS)], dst, state_sem.at[i]).start()

    def start_pieces(color, p):
        for i, (first, n) in enumerate(LOAD):
            @pl.when(p == first // GROUP)
            def _():
                wait_on(acc[color].at[:, pl.ds(first, n)], ld_sem.at[color, i])
                wait_on(pair[color].at[:, pl.ds(FRONT + first, n)], pr_recv.at[color, i])
        bit = bits[color][0]
        for slot in ((1 - bit) * TILE, bit * TILE):
            add(color, slot, TILE, slot, p, p + AHEAD)
        reduce_send(color, 0, p)

    def reduce_piece(color, stage_no, p):
        s = stage_no - 1
        wait_on(landing(color, s, p), rs_recv.at[color, s, p])
        first, size, bit = reduce_base(color, stage_no, p), 4 >> s, halved(color, stage_no, p)
        for half in (1 - bit, bit):
            add(color, first + half * size, size, 16 - (16 >> s) + half * size, p, p)
        reduce_send(color, stage_no, p)

    def adam_piece(color, p):
        wait_on(landing(color, 3, p), rs_recv.at[color, 3, p])
        slot = base(color, 4)
        acc[color][reduce_base(color, 4, p), rows_at(p), :] += final[color][0, rows_at(p), :]
        adam(color, p)
        gather_send(color, 0, slot, 1, p)

    def gather_send(color, s, first, size, p):
        block = gat.at[color, c, pl.ds(first, size), rows_at(p)]
        pltpu.make_async_remote_copy(block, block, ag_send.at[color, s], ag_recv.at[color, s, p], device_id=routes[color][3 - s], device_id_type=MESH).start()

    def gather_piece(color, s, p):
        level, size = 4 - s, 1 << s
        arrived = base(color, level - 1) + (1 - bits[color][level - 1]) * size
        wait_on(gat.at[color, c, pl.ds(arrived, size), rows_at(p)], ag_recv.at[color, s, p])
        if s < 3:
            gather_send(color, s + 1, base(color, level - 1), 2 * size, p)
        if s > 1:
            pair_out(color, arrived if s == 3 else base(color, 1), TILE, p)

    load(0, (False,))

    @pl.loop(0, STEPS)
    def _(t):
        for i in range(2, len(LOAD)):
            pl.when(t == LOAD[i - 1][0] // GROUP)(functools.partial(load, i))
        for stage_no, color in SEQUENCE:
            p = t - LAGS[color][stage_no]

            @pl.when((p >= 0) & (p < PIECES))
            def _():
                if stage_no == 0:
                    start_pieces(color, p)
                elif stage_no < 4:
                    reduce_piece(color, stage_no, p)
                elif stage_no == 4:
                    adam_piece(color, p)
                else:
                    gather_piece(color, stage_no - 5, p)

        pl.when(t == 0)(functools.partial(load, 1))

        @pl.when(t == 1)
        def _():
            state_rows()

        @pl.when((t >= 2) & (t < 6))
        def _():
            state_rows_part(t - 2)

        @pl.when((t >= 6) & (t < FIRST_ADAM))
        def _():
            state_to_cover(t - 6)

        @pl.when((t > LAST_ADAM) & (t <= LAST_ADAM + 15))
        def _():
            cover_to_state(t - LAST_ADAM - 1)

    for color in COLORS:
        wait_on(gat.at[color, 1 - c], dag_recv.at[color])
        wait_on(gat.at[color, c], dag_send.at[color])
        wait_on(acc[color], pr_send.at[color])
        for s in range(4):
            wait_on(acc[color].at[pl.ds(0, TILE >> s)], rs_send.at[color, s])
            wait_on(gat.at[color, 0, pl.ds(0, 1 << s)], ag_send.at[color, s])


def place_kernel(gat, stage, e_out, a_out, f1_out, f2_out, b_out, m_out, v_out, w_out, chip_out, merged, loose, vec, tail, block, out_sem, edge_sem, state_sem, chip_sem):
    outs = (e_out, a_out, f1_out, f2_out, b_out)
    chip = (lax.axis_index('outer') * 2 + lax.axis_index('middle')) * 2 + lax.axis_index('inner') // 2
    started = [pltpu.make_async_copy(stage.at[i, pl.ds(MARGIN, SLICE_ROWS)], dst, state_sem.at[i]) for i, dst in enumerate((m_out, v_out, w_out))]

    def rows_from(d, at, n):
        color = at // HALF
        return gat.at[color, d % 2, slot_of(color, d // 2), pl.ds(at - color * HALF, n)]

    row = lax.broadcasted_iota(jnp.int32, (GROUP, LANES), 0)
    lane = lax.broadcasted_iota(jnp.int32, (GROUP, LANES), 1)
    tile_order = (row % TILE) * 4 + row // TILE
    count = 0
    for d in range(NDEV):
        first = merge_row(d)
        last = merge_row(d + 1) if d < LAST else STARTS[-1]
        begin = start_row(d)
        for color in COLORS:
            lo = max(first + (GROUP if d else 0), begin + color * HALF)
            for tensor, at, off, n in segments(lo, min(last, begin + (color + 1) * HALF) - lo):
                started.append(pltpu.make_async_copy(rows_from(d, lo + off - begin, n), outs[tensor].at[pl.ds(at, n)], out_sem.at[count]))
                count += 1
    for copy in started:
        copy.start()
    for d in range(1, NDEV):
        first = merge_row(d)
        flat = tile_order if PERM_LO <= first < PERM_HI else row
        keep = 2 * flat + lane // 64 >= SPAN * d - 2 * first
        new, old = (rows_from(e, first - start_row(e), GROUP)[...].astype(jnp.float32) for e in (d, d - 1))
        merged[d] = jnp.where(keep, new, old).astype(jnp.bfloat16)
        (tensor, at, _, _), = segments(first, GROUP)
        copy = pltpu.make_async_copy(merged.at[d], outs[tensor].at[pl.ds(at, GROUP)], edge_sem.at[d])
        copy.start()
        started.append(copy)

    def rows_of(group):
        d = (64 * group + 63) * INVERSE[0] >> INVERSE[1]
        begin = jnp.where(d == LAST, LAST_START, (SPAN * d >> 6) * GROUP)
        x, y, z0, z1 = ((d >> i) & 1 for i in range(1, 5))
        halves = []
        for h in COLORS:
            at = GROUP * group - begin + 16 * h
            color = (at >= HALF).astype(jnp.int32)
            slot = jnp.where(color == 0, x, y) * TILE + z0 * 4 + jnp.where(color == 0, y, x) * 2 + z1
            halves.append(gat[color, d & 1, slot, pl.ds(pl.multiple_of(at - color * HALF, 16), 16), :])
        return halves

    def put(at, rows):
        block[0:1, pl.ds(pl.multiple_of(at * LANES, BLOCK), BLOCK)] = rows.reshape(1, BLOCK).astype(jnp.bfloat16)
    def put_rows(at, halves):
        for h, half in enumerate(halves):
            rows = half.astype(jnp.float32)
            for q in COLORS:
                put(at + 16 * h + TILE * q, rows[TILE * q:TILE * q + TILE])

    def put_tiles(at, halves, t):
        for h, half in enumerate(halves):
            rows = half.astype(jnp.float32)
            for q in COLORS:
                loose[t, pl.ds(2 * h + q, TILE, stride=4), :] = rows[TILE * q:TILE * q + TILE]
        for q in range(4):
            put(at + TILE * q, loose[t, TILE * q:TILE * q + TILE, :])

    def put_edges(tensors):
        for d in range(1, NDEV):
            (tensor, at, _, _), = segments(merge_row(d), GROUP)
            if tensor not in tensors:
                continue
            layer, owner = divmod(at // GROUP, 16)

            @pl.when(chip == (owner if tensor else at // E_ROWS))
            def _():
                halves = (merged[d, 0:16, :], merged[d, 16:, :])
                if tensor in (1, 2):
                    put_tiles(1536 + 512 * tensor + GROUP * layer, halves, tensor - 1)
                else:
                    put_rows(3072 + GROUP * layer if tensor else at % E_ROWS, halves)

    @pl.loop(0, 64, unroll=4)
    def _(j):
        put_rows(GROUP * j, rows_of(chip * 64 + j))

    put_edges((0,))
    split = E_ROWS * LANES
    sends = [pltpu.make_async_copy(block.at[:, pl.ds(at, n)], chip_out.at[:, pl.ds(at, n)], chip_sem.at[i]) for i, (at, n) in enumerate(((0, split), (split, 2 * SLICE - split)))]
    sends[0].start()

    @pl.loop(0, 16, unroll=2)
    def _(layer):
        for t in (1, 2):
            put_tiles(1536 + 512 * t + GROUP * layer, rows_of(STARTS[t] // GROUP + layer * 16 + chip), t - 1)
        put_rows(3072 + GROUP * layer, rows_of(STARTS[3] // GROUP + layer * 16 + chip))

    put_edges((1, 2, 3))
    at = STARTS[4] - start_row(LAST)
    vec[0:208, :] = rows_from(LAST, at, 208)[...].astype(jnp.float32)
    vec[208:, :] = jnp.zeros((16, LANES), jnp.float32)
    tail[...] = jnp.zeros_like(tail)
    begin = (104 * chip) % LANES
    line = lax.broadcasted_iota(jnp.int32, (TILE, LANES), 1)
    for layer in range(16):
        source = layer // TILE * TILE * VEC_TILES + layer % TILE + (104 * chip) // LANES * TILE
        to = layer * 104 // LANES
        off = layer * 104 % LANES
        turn = (off - begin + LANES) % LANES
        one = pltpu.roll(vec[pl.ds(source, TILE), :], turn, 1)
        two = pltpu.roll(vec[pl.ds(source + TILE, TILE), :], turn, 1)
        t = (line - off + LANES) % LANES
        got = jnp.where(begin + t < LANES, one, two)
        here = (t < 104) & (line >= off)
        tail[to:to + 1, :] = jnp.where(here, got, tail[pl.ds(to, TILE), :])[0:1]
        if off + 104 > LANES:
            there = (t < 104) & (line < off)
            tail[to + 1:to + 2, :] = jnp.where(there, got, tail[pl.ds(to + 1, TILE), :])[0:1]
    put(3584, tail[0:TILE, :])
    block[0:1, 3592 * LANES:] = tail[TILE:16, :].reshape(1, BLOCK)[:, 0:640].astype(jnp.bfloat16)
    sends[1].start()
    for copy in started + sends:
        copy.wait()


def tile_rows(tensor, tiles=4):
    return tensor.reshape(-1, TILE, tiles, LANES).transpose(0, 2, 1, 3).reshape(-1, LANES)


def untile(rows, shape, tiles=4):
    return rows.reshape(-1, tiles, TILE, LANES).transpose(0, 2, 1, 3).reshape(shape)


def solution(mesh):
    def local_step(g_embed, g_attn, g_ffn_in, g_ffn_out, g_vec, m_shard, v_shard, w_shard):
        grads = (g_embed[0], tile_rows(g_attn[0]), tile_rows(g_ffn_in[0]), g_ffn_out[0].reshape(-1, LANES), tile_rows(g_vec[0], VEC_TILES))
        any_spec, vmem_spec = pl.BlockSpec(memory_space=pl.ANY), pl.BlockSpec(memory_space=pltpu.VMEM)
        f32, bf16 = jnp.float32, jnp.bfloat16
        flat = jax.ShapeDtypeStruct((SLICE_ROWS, LANES), f32)
        dma = pltpu.SemaphoreType.DMA
        gathered, stage = pl.pallas_call(
            big_kernel,
            out_shape=(pltpu.VMEM((2, 2, 16, HALF, LANES), bf16), pltpu.VMEM((3, SLICE_ROWS + 2 * MARGIN, LANES), f32)),
            in_specs=[any_spec] * 8,
            out_specs=[vmem_spec] * 2,
            scratch_shapes=[pltpu.VMEM((16, HALF, LANES), f32)] * 2 + [pltpu.VMEM((16, HALF + FRONT, LANES), f32)] * 2 + [pltpu.VMEM((1, HALF, LANES), f32)] * 2 + [pltpu.VMEM((SLICE,), f32)] * 3 + [pltpu.VMEM((3, COVER, LANES), f32)]
            + [dma((2, len(LOADS))), dma((2, len(LOADS))), dma((2,)), dma((2, 4, PIECES)), dma((2, 4)), dma((2, 4, PIECES)), dma((2, 4)), dma((2,)), dma((2,)), dma((3,))],
            compiler_params=pltpu.CompilerParams(collective_id=0, has_side_effects=True, vmem_limit_bytes=BIG_VMEM),
            name='reduce_adam_gather',
        )(*grads, m_shard, v_shard, w_shard)
        placed = pl.pallas_call(
            place_kernel,
            out_shape=[jax.ShapeDtypeStruct((n, LANES), bf16) for n in TENSOR_ROWS] + [flat] * 3 + [jax.ShapeDtypeStruct((1, 2 * SLICE), bf16)],
            in_specs=[vmem_spec] * 2,
            out_specs=[any_spec] * 9,
            scratch_shapes=[pltpu.VMEM((NDEV, GROUP, LANES), bf16), pltpu.VMEM((2, GROUP, LANES), f32), pltpu.VMEM((224, LANES), f32), pltpu.VMEM((24, LANES), f32), pltpu.VMEM((1, 2 * SLICE), bf16)]
            + [dma((2 * NDEV + TILE,)), dma((NDEV,)), dma((3,)), dma((2,))],
            compiler_params=pltpu.CompilerParams(vmem_limit_bytes=PLACE_VMEM),
            name='place',
        )(gathered, stage)
        e, a, f1, f2, b, *state, w_chip = placed
        tensors = (e, untile(a, (16, LANES, 512)), untile(f1, (16, LANES, 512)), f2.reshape(16, 512, LANES), untile(b, (16, 1664), VEC_TILES))
        return tuple(t.reshape(-1)[:SLICE] for t in state) + tensors + (w_chip,)

    return jax.shard_map(local_step, mesh=mesh, in_specs=(P(MESH_AXES),) * TILE, out_specs=(P(MESH_AXES),) * 3 + (P(),) * 5 + (P(MESH_AXES),), check_vma=False)
```
